32 devices in a mesh: grp: 4 (over y, x), seq: 2 (over core), mdl: 4 (over z).
Axes of the slice: x: 2, y: 2, z: 4, core: 2. Of those that a mesh axis runs over, the one named last changes fastest.
Arguments:
- layer_input: bfloat16 [1024, 8192], P('seq', 'grp'), may hold values from -64 to 64
- attn_weight: bfloat16 [8192, 8, 1280], P(('grp', 'seq'), 'mdl'), may hold values from -0.0625 to 0.0625
- rate_weight: bfloat16 [8192, 64], P('grp', 'mdl'), may hold values from -0.15625 to 0.15625
- rate_bias: float32 [64], P(('mdl', 'grp')), may hold values from -8 to -3
- decay_rate: float32 [64], P(('mdl', 'grp')), may hold values from 1e-05 to 0.1
- skip_gain: float32 [64], P(('mdl', 'grp')), may hold values from 0.5 to 1.5
Outputs:
- teacher_heads: bfloat16 [1024, 8192], P('seq', ('mdl', 'grp'))
- student_heads: bfloat16 [1024, 8192], P('seq', ('mdl', 'grp'))
The draws below stay inside these ranges and needn't reach their ends.
All inputs are finite; a program needn't handle non-finite values.
Results may differ from the reference program's by a relative error of at most 0.03.
Values may be sent and summed in bfloat16 or wider, within the bound.
No kernel may reach another device: no remote copies, remote signals or barrier semaphores. Data moves between devices by JAX's collectives and lax.ppermute only.
A program may use at most 192 MiB of HBM per device.

```python
import math
import jax
import jax.numpy as jnp
from jax import lax

D = 8192
HEADS = 64
KV_HEADS = 8
HEAD_DIM = 128
STRETCH = 256
TOKENS = 1024


def draw_layer_input(key, part):
    drawn = jax.random.normal(jax.random.fold_in(key, 105), (TOKENS, D), jnp.float32)
    return jnp.clip(drawn, -64.0, 64.0).astype(jnp.bfloat16)


def draw_decay_rate(key, part):
    unit = jax.random.uniform(jax.random.fold_in(key, 201), (HEADS,), jnp.float32)
    lower = math.log(0.0005)
    upper = math.log(0.1)
    return jnp.exp(lower + (upper - lower) * unit)


def levels(stream_key, extent, split, smallest, high):
    loudness, own = 1.0, jax.random.fold_in(stream_key, 6)
    for axis_at, shards_of in split:
        heights = jnp.exp(jax.random.uniform(jax.random.fold_in(own, axis_at), (shards_of,), jnp.float32, smallest / len(split), high / len(split)))
        loudness = loudness * jnp.repeat(heights, extent[axis_at] // shards_of).reshape([-1 if axis == axis_at else 1 for axis in range(len(extent))])
    return loudness


def bell_draw(own_key, dims, width, reach, split=(), kind=jnp.bfloat16):
    result = jax.random.normal(own_key, dims, jnp.float32) * width
    if len(split) > 0:
        result = levels(own_key, dims, split, -0.22, 0.18) * result
    return jnp.clip(result, min=-reach, max=reach).astype(kind)


def setup_inputs(seed: int = 0) -> dict:
    key_list = jax.random.split(jax.random.key(seed), 7)
    return {
        "layer_input": draw_layer_input(jax.random.fold_in(key_list[6], 71), 0),
        "attn_weight": bell_draw(key_list[1], (D, KV_HEADS, (HEADS // KV_HEADS + 2) * HEAD_DIM), D ** -0.5, 0.0625, ((0, 8), (1, 4))),
        "rate_weight": bell_draw(key_list[2], (D, HEADS), (D // 6) ** -0.5, 0.15625, ((0, 4), (1, 4))),
        "rate_bias": jnp.clip(-8.0 + 5.0 * jax.random.uniform(key_list[3], (HEADS,), jnp.float32) ** levels(key_list[3], (HEADS,), ((0, 16),), -0.2, 0.2), -8.0, -3.0),
        "decay_rate": draw_decay_rate(jax.random.fold_in(key_list[6], 71), 0),
        "skip_gain": jnp.clip(0.5 + 1.0 * jax.random.uniform(key_list[5], (HEADS,), jnp.float32) ** levels(key_list[5], (HEADS,), ((0, 16),), -0.2, 0.2), 0.5, 1.5),
    }


ROPE_BASE = 500000.0


def rope_angles(positions):
    half = HEAD_DIM // 2
    freq = ROPE_BASE ** (-2.0 * jnp.arange(half, dtype=jnp.float32) / HEAD_DIM)
    angle = positions.astype(jnp.float32)[:, None] * freq[None, :]
    return jnp.cos(angle), jnp.sin(angle)


def rotate(vectors, cosine, sine):
    half = vectors.shape[-1] // 2
    first = vectors[..., :half]
    second = vectors[..., half:]
    cosine = cosine[:, None, :]
    sine = sine[:, None, :]
    return jnp.concatenate([first * cosine - second * sine, second * cosine + first * sine], axis=-1)


def attend_head(query, keys, values, scale):
    block = math.gcd(512, TOKENS)
    pieces = []
    for first in range(0, TOKENS, block):
        last = first + block
        scores = jnp.dot(query[first:last], keys[:last].T, preferred_element_type=jnp.float32) * scale
        rows = jnp.arange(first, last, dtype=jnp.int32)[:, None]
        cols = jnp.arange(last, dtype=jnp.int32)[None, :]
        causal = cols <= rows
        masked = jnp.where(causal, scores, -1e30)
        top = jnp.max(masked, axis=1, keepdims=True)
        weights = jnp.where(causal, jnp.exp(masked - top), 0.0)
        total = jnp.sum(weights, axis=1, keepdims=True)
        numer = jnp.dot(weights.astype(jnp.bfloat16), values[:last], preferred_element_type=jnp.float32)
        pieces.append((numer / total).astype(jnp.bfloat16))
    return jnp.concatenate(pieces, axis=0)


def student_scan(cterm, bterm, values, raw, rate_bias, decay_rate, skip_gain, scale):
    group = HEADS // KV_HEADS
    step = jax.nn.softplus(raw + rate_bias[None, :])
    log_decay = -decay_rate[None, :] * step
    b_all = jnp.repeat(bterm, group, axis=1)
    x_all = jnp.repeat(values, group, axis=1)
    count = TOKENS // STRETCH

    def stretched(array):
        return array.reshape((count, STRETCH) + array.shape[1:])

    causal = (jnp.arange(STRETCH, dtype=jnp.int32)[:, None] >= jnp.arange(STRETCH, dtype=jnp.int32)[None, :])[None]

    def advance(state, parts):
        cpart, bpart, xpart, decay, rate = parts
        cfull = cpart.astype(jnp.float32)
        bfull = bpart.astype(jnp.float32)
        xfull = xpart.astype(jnp.float32)
        cum = jnp.cumsum(decay, axis=0)
        gram = jnp.einsum('thn,shn->hts', cfull, bfull, precision=lax.Precision.HIGHEST) * scale
        diff = cum.T[:, :, None] - cum.T[:, None, :]
        mix = jnp.where(causal, jnp.exp(jnp.where(causal, diff, -1e4)) * rate.T[:, None, :] * gram, 0.0)
        mix = mix.astype(jnp.bfloat16).astype(jnp.float32)
        intra = jnp.einsum('hts,shp->thp', mix, xfull, precision=lax.Precision.HIGHEST)
        carried = jnp.einsum('thn,hnp->thp', cfull, state, precision=lax.Precision.HIGHEST) * scale * jnp.exp(cum)[:, :, None]
        weighted = ((jnp.exp(cum[-1][None, :] - cum) * rate)[:, :, None] * bfull).astype(jnp.bfloat16).astype(jnp.float32)
        contribution = jnp.einsum('shn,shp->hnp', weighted, xfull, precision=lax.Precision.HIGHEST)
        state = jnp.exp(cum[-1])[:, None, None] * state + contribution
        output = (intra + carried + skip_gain[None, :, None] * xfull).astype(jnp.bfloat16)
        return state, output

    start = jnp.zeros((HEADS, HEAD_DIM, HEAD_DIM), jnp.float32)
    _, outputs = lax.scan(advance, start, (stretched(cterm), stretched(b_all), stretched(x_all), stretched(log_decay), stretched(step)))
    return outputs.reshape(TOKENS, HEADS * HEAD_DIM)


def reference(layer_input, attn_weight, rate_weight, rate_bias, decay_rate, skip_gain):
    group = HEADS // KV_HEADS
    scale = HEAD_DIM ** -0.5
    merged = jnp.dot(layer_input, attn_weight.reshape(D, KV_HEADS * (group + 2) * HEAD_DIM), preferred_element_type=jnp.float32)
    merged = merged.reshape(TOKENS, KV_HEADS, group + 2, HEAD_DIM)
    query = merged[:, :, :group].reshape(TOKENS, HEADS, HEAD_DIM)
    keys = merged[:, :, group]
    values = merged[:, :, group + 1].astype(jnp.bfloat16)
    raw = jnp.dot(layer_input, rate_weight, preferred_element_type=jnp.float32)
    cosine, sine = rope_angles(jnp.arange(TOKENS, dtype=jnp.int32))
    rot_query = rotate(query, cosine, sine).astype(jnp.bfloat16)
    rot_keys = rotate(keys, cosine, sine).astype(jnp.bfloat16)

    def one_head(index):
        kv_index = index // group
        return attend_head(rot_query[:, index], rot_keys[:, kv_index], values[:, kv_index], scale)

    heads = lax.map(one_head, jnp.arange(HEADS, dtype=jnp.int32))
    teacher_heads = jnp.transpose(heads, (1, 0, 2)).reshape(TOKENS, HEADS * HEAD_DIM)
    student_heads = student_scan(query.astype(jnp.bfloat16), keys.astype(jnp.bfloat16), values, raw, rate_bias, decay_rate, skip_gain, scale)
    return teacher_heads, student_heads
```

```python
import functools

import jax
import jax.numpy as jnp
from jax import lax
from jax.experimental import pallas as pl
from jax.experimental.pallas import tpu as pltpu
from jax.sharding import PartitionSpec as P

HEADS = 64
KV_HEADS = 8
HEAD_DIM = 128
STRETCH = 256


ROPE_BASE = 500000.0
FAR_BELOW = -1e30


def rope_angles(positions):
    half = HEAD_DIM // 2
    freq = ROPE_BASE ** (-2.0 * jnp.arange(half, dtype=jnp.float32) / HEAD_DIM)
    angle = positions.astype(jnp.float32)[:, None] * freq[None, :]
    return (jnp.cos(angle), jnp.sin(angle))


def rotate(vectors, cosine, sine):
    half = vectors.shape[-1] // 2
    first = vectors[..., :half]
    second = vectors[..., half:]
    cosine = cosine[:, None, :]
    sine = sine[:, None, :]
    return jnp.concatenate(
        [first * cosine - second * sine, second * cosine + first * sine], axis=-1
    )


def state_product(cterm, state):
    high = state.astype(jnp.bfloat16)
    low = (state - high.astype(jnp.float32)).astype(jnp.bfloat16)
    upper = jnp.einsum("thn,hnp->thp", cterm, high, preferred_element_type=jnp.float32)
    return upper + jnp.einsum("thn,hnp->thp", cterm, low, preferred_element_type=jnp.float32)


def key_absorber(queries, own_first, scale, carry, piece):
    top, total, accum = carry
    keys, values = piece
    scores = jnp.einsum("thd,nd->thn", queries, keys, preferred_element_type=jnp.float32) * scale
    query_pos = own_first + jnp.arange(queries.shape[0], dtype=jnp.int32)
    key_pos = jnp.arange(keys.shape[0], dtype=jnp.int32)
    causal = (key_pos[None, :] <= query_pos[:, None])[:, None, :]
    masked = jnp.where(causal, scores, FAR_BELOW)
    new_top = jnp.maximum(top, jnp.max(masked, axis=2))
    weights = jnp.where(causal, jnp.exp(masked - new_top[:, :, None]), 0.0)
    total = jnp.sum(weights, axis=2)
    accum = jnp.einsum(
        "thn,nd->thd", weights.astype(jnp.bfloat16), values, preferred_element_type=jnp.float32
    )
    return (new_top, total, accum)


def body(layer_input, attn_weight, rate_weight, rate_bias, decay_rate, skip_gain):
    tok = layer_input.shape[0]
    kv_local = attn_weight.shape[1]
    heads_local = rate_bias.shape[0]
    group = HEADS // KV_HEADS
    scale = HEAD_DIM ** (-0.5)
    merged = jnp.einsum(
        "td,dkc->tkc",
        layer_input,
        lax.all_gather(attn_weight, "seq", axis=0, tiled=True),
        preferred_element_type=jnp.float32,
    )
    rate_part = jnp.dot(layer_input, rate_weight, preferred_element_type=jnp.float32)
    grp_index = lax.axis_index("grp")
    summed, rate_whole = (
        lax.psum(merged.astype(jnp.bfloat16), "grp").astype(jnp.float32),
        lax.psum(rate_part.astype(jnp.bfloat16), "grp").astype(jnp.float32),
    )
    query_whole = summed[:, :, : group * HEAD_DIM].reshape(tok, kv_local * group * HEAD_DIM)
    query_flat = lax.dynamic_slice_in_dim(
        query_whole, grp_index * heads_local * HEAD_DIM, heads_local * HEAD_DIM, 1
    )
    raw = lax.dynamic_slice_in_dim(rate_whole, grp_index * heads_local, heads_local, 1)
    pairs = summed[:, :, group * HEAD_DIM :]
    kv_index = grp_index * heads_local // group
    pair = lax.dynamic_index_in_dim(pairs, kv_index, 1, keepdims=False)
    keys = pair[:, :HEAD_DIM]
    values = pair[:, HEAD_DIM:].astype(jnp.bfloat16)
    query = query_flat.reshape(tok, heads_local, HEAD_DIM)
    own_first = lax.axis_index("seq") * tok
    cosine, sine = rope_angles(own_first + jnp.arange(tok, dtype=jnp.int32))
    rot_query = rotate(query, cosine, sine).astype(jnp.bfloat16)
    rot_keys = rotate(keys[:, None, :], cosine, sine)[:, 0].astype(jnp.bfloat16)
    start_carry = (
        jnp.full((tok, heads_local), FAR_BELOW, jnp.float32),
        jnp.zeros((tok, heads_local), jnp.float32),
        jnp.zeros((tok, heads_local, HEAD_DIM), jnp.float32),
    )
    top, total, accum = key_absorber(
        rot_query,
        own_first,
        scale,
        start_carry,
        (
            lax.all_gather(rot_keys, "seq", axis=0, tiled=True),
            lax.all_gather(values, "seq", axis=0, tiled=True),
        ),
    )
    teacher = (accum / total[:, :, None]).astype(jnp.bfloat16).reshape(tok, heads_local * HEAD_DIM)
    step = jax.nn.softplus(raw + rate_bias[None, :])
    log_decay = -decay_rate[None, :] * step
    c_all = query.astype(jnp.bfloat16)
    b_all = keys.astype(jnp.bfloat16)
    causal = (
        jnp.arange(STRETCH, dtype=jnp.int32)[:, None]
        >= jnp.arange(STRETCH, dtype=jnp.int32)[None, :]
    )[None]
    state = jnp.zeros((heads_local, HEAD_DIM, HEAD_DIM), jnp.float32)
    before = jnp.zeros((heads_local,), jnp.float32)
    partials = []
    offsets = []
    for index in range(tok // STRETCH):
        first = index * STRETCH
        cpart = c_all[first : first + STRETCH]
        bpart = b_all[first : first + STRETCH]
        xpart = values[first : first + STRETCH]
        decay = log_decay[first : first + STRETCH]
        rate = step[first : first + STRETCH]
        cum = jnp.cumsum(decay, axis=0)
        gram = jnp.einsum("thn,sn->hts", cpart, bpart, preferred_element_type=jnp.float32) * scale
        diff = cum.T[:, :, None] - cum.T[:, None, :]
        mix = jnp.where(
            causal, jnp.exp(jnp.where(causal, diff, -10000.0)) * rate.T[:, None, :] * gram, 0.0
        ).astype(jnp.bfloat16)
        intra = jnp.einsum("hts,sp->thp", mix, xpart, preferred_element_type=jnp.float32)
        carried = state_product(cpart, state) * scale * jnp.exp(cum)[:, :, None]
        weighted = (
            (jnp.exp(cum[-1][None, :] - cum) * rate)[:, :, None]
            * bpart.astype(jnp.float32)[:, None, :]
        ).astype(jnp.bfloat16)
        contribution = jnp.einsum(
            "shn,sp->hnp", weighted, xpart, preferred_element_type=jnp.float32
        )
        state = jnp.exp(cum[-1])[:, None, None] * state + contribution
        partials.append(intra + carried)
        offsets.append(cum + before[None, :])
        before = before + cum[-1]
    totals, states = (
        lax.all_gather(before[None, :].astype(jnp.bfloat16), "seq", axis=0, tiled=True).astype(
            jnp.float32
        ),
        lax.all_gather(state[None].astype(jnp.bfloat16), "seq", axis=0, tiled=True).astype(
            jnp.float32
        ),
    )
    position = lax.axis_index("seq")
    order = jnp.arange(totals.shape[0], dtype=jnp.int32)
    between = ((order[:, None] < order[None, :]) & (order[None, :] < position)).astype(jnp.float32)
    span = jnp.dot(between, totals, precision=lax.Precision.HIGHEST)
    reach_back = jnp.where(order[:, None] < position, jnp.exp(span), 0.0)
    incoming = jnp.einsum("dh,dhnp->hnp", reach_back, states, precision=lax.Precision.HIGHEST)
    inside = jnp.concatenate(partials, axis=0)
    reach = jnp.exp(jnp.concatenate(offsets, axis=0))
    arriving = state_product(c_all, incoming) * scale * reach[:, :, None]
    skipped = skip_gain[None, :, None] * values.astype(jnp.float32)[:, None, :]
    student = (
        (inside + arriving + skipped).astype(jnp.bfloat16).reshape(tok, heads_local * HEAD_DIM)
    )
    return (teacher, student)


LANES = 128
VMEM_GRANT = 24 * 1024 * 1024
F32 = jnp.float32
BF16 = jnp.bfloat16


def cost(flops, moved):
    return pl.CostEstimate(flops=flops, bytes_accessed=moved, transcendentals=0)


def project_kernel(ids, x_ref, w0, w1, w2, w3, out_ref):
    weights = jnp.concatenate([w0[0], w1[0], w2[0], w3[0]], axis=1)
    out_ref[...] = jnp.dot(x_ref[...], weights, preferred_element_type=F32).astype(BF16)


def project_add_kernel(ids, x_ref, w0, w1, w2, w3, r_ref, send_ref, keep_ref):
    half = keep_ref.shape[1]
    sent = jnp.concatenate([w0[0], w1[0]], axis=1)
    kept = jnp.concatenate([w2[0], w3[0]], axis=1)
    first = jnp.dot(x_ref[...], sent, preferred_element_type=F32)
    send_ref[...] = (first + r_ref[:, :half].astype(F32)).astype(BF16)
    second = jnp.dot(x_ref[...], kept, preferred_element_type=F32)
    keep_ref[...] = second + r_ref[:, half:].astype(F32)


def weight_spec(rows, place):
    def index(step, ids):
        kv, col = place(ids[0], ids[1])
        return (kv, 0, col)

    return pl.BlockSpec((1, rows, LANES), index)


def project(ids, x, x_block, weights, places):
    tok, rows = x.shape[0], weights.shape[1]
    wide = len(places) * LANES
    return pl.pallas_call(
        project_kernel,
        grid_spec=pltpu.PrefetchScalarGridSpec(
            num_scalar_prefetch=1,
            grid=(1,),
            in_specs=[pl.BlockSpec((tok, rows), x_block)]
            + [weight_spec(rows, place) for place in places],
            out_specs=pl.BlockSpec((tok, wide), lambda step, ids: (0, 0)),
        ),
        out_shape=jax.ShapeDtypeStruct((tok, wide), BF16),
        compiler_params=pltpu.CompilerParams(vmem_limit_bytes=VMEM_GRANT),
        cost_estimate=cost(2 * tok * rows * wide, 2 * rows * (tok + wide)),
    )(ids, x, *([weights] * len(places)))


def project_add(ids, x, x_block, weights, places, received):
    tok, rows = x.shape[0], weights.shape[1]
    wide = len(places) * LANES
    half = wide // 2
    return pl.pallas_call(
        project_add_kernel,
        grid_spec=pltpu.PrefetchScalarGridSpec(
            num_scalar_prefetch=1,
            grid=(1,),
            in_specs=[pl.BlockSpec((tok, rows), x_block)]
            + [weight_spec(rows, place) for place in places]
            + [pl.BlockSpec((tok, wide), lambda step, ids: (0, 0))],
            out_specs=[
                pl.BlockSpec((tok, half), lambda step, ids: (0, 0)),
                pl.BlockSpec((tok, half), lambda step, ids: (0, 0)),
            ],
        ),
        out_shape=[
            jax.ShapeDtypeStruct((tok, half), BF16),
            jax.ShapeDtypeStruct((tok, half), F32),
        ],
        compiler_params=pltpu.CompilerParams(vmem_limit_bytes=VMEM_GRANT),
        cost_estimate=cost(2 * tok * rows * wide, 2 * rows * (tok + wide)),
    )(ids, x, *([weights] * len(places)), received)


def turn(vectors, cosine, sine):
    return vectors * cosine + pltpu.roll(vectors, HEAD_DIM // 2, 1) * sine


def keys_kernel(keep_ref, u_ref, z_ref, cos_ref, sin_ref, rotv_ref, bterm_ref):
    pair = keep_ref[...] + u_ref[...].astype(F32) + z_ref[...].astype(F32)
    keys = pair[:, :HEAD_DIM]
    rotv_ref[:, :HEAD_DIM] = turn(keys, cos_ref[...], sin_ref[...]).astype(BF16)
    rotv_ref[:, HEAD_DIM:] = pair[:, HEAD_DIM:].astype(BF16)
    bterm_ref[...] = keys.astype(BF16)


def whole(shape):
    return pl.BlockSpec(shape, lambda: (0,) * len(shape))


def keys_call(keep, u, z, cosine, sine):
    tok = keep.shape[0]
    shapes = [(tok, 2 * HEAD_DIM), (tok, HEAD_DIM)]
    return pl.pallas_call(
        keys_kernel,
        in_specs=[whole(a.shape) for a in (keep, u, z, cosine, sine)],
        out_specs=[whole(s) for s in shapes],
        out_shape=[jax.ShapeDtypeStruct(s, BF16) for s in shapes],
        compiler_params=pltpu.CompilerParams(vmem_limit_bytes=VMEM_GRANT),
        cost_estimate=cost(10**8, 10**6),
    )(keep, u, z, cosine, sine)


def decays_of(raw, bias, rate):
    step = jax.nn.softplus(raw + bias)
    return step, -rate * step


def running(decay):
    count = decay.shape[1]
    rows = lax.broadcasted_iota(jnp.int32, (count, count), 0)
    cols = lax.broadcasted_iota(jnp.int32, (count, count), 1)
    below = (cols <= rows).astype(F32)
    dims = (((1,), (1,)), ((), ()))
    across = lax.dot_general(
        decay, below, dims, precision=lax.Precision.HIGHEST, preferred_element_type=F32
    )
    down = lax.dot_general(
        below, decay, dims, precision=lax.Precision.HIGHEST, preferred_element_type=F32
    )
    return across, down


def states_kernel(
    stretch, raw_ref, bias_ref, rate_ref, rotv_ref, bterm_ref,
    across_ref, down_ref, step_ref, first_ref, last_ref,
):
    heads = raw_ref.shape[0]
    tok = raw_ref.shape[1]
    step, decay = decays_of(raw_ref[...], bias_ref[...], rate_ref[...])
    step_ref[...] = step
    states = [jnp.zeros((HEAD_DIM, HEAD_DIM), F32)] * heads
    for index in range(tok // stretch):
        span = slice(index * stretch, (index + 1) * stretch)
        across, down = running(decay[:, span])
        across_ref[:, span] = across
        down_ref[span, :] = down
        keys = bterm_ref[span, :].astype(F32)
        values = rotv_ref[span, HEAD_DIM:]
        ends = jnp.exp(across[:, stretch - 1 :])
        tail = jnp.exp(across[:, stretch - 1 :] - across) * step[:, span]
        eye = (
            lax.broadcasted_iota(jnp.int32, (heads, heads), 0)
            == lax.broadcasted_iota(jnp.int32, (heads, heads), 1)
        ).astype(F32)
        tail = lax.dot_general(
            tail, eye, (((0,), (0,)), ((), ())),
            precision=lax.Precision.HIGHEST, preferred_element_type=F32,
        )
        for head in range(heads):
            weighted = (keys * tail[:, head : head + 1]).astype(BF16)
            fresh = lax.dot_general(
                weighted, values, (((0,), (0,)), ((), ())), preferred_element_type=F32
            )
            states[head] = ends[head : head + 1, :] * states[head] + fresh
            if index == 0:
                first_ref[head] = states[head]
    for head in range(heads):
        last_ref[head] = states[head].astype(BF16)


def states_call(raw, bias, rate, rotv, bterm):
    heads, tok = raw.shape
    square = (heads, HEAD_DIM, HEAD_DIM)
    shapes = [((heads, tok), F32), ((tok, heads), F32), ((heads, tok), F32), (square, F32), (square, BF16)]
    return pl.pallas_call(
        functools.partial(states_kernel, STRETCH),
        in_specs=[whole(a.shape) for a in (raw, bias, rate, rotv, bterm)],
        out_specs=[whole(s) for s, _ in shapes],
        out_shape=[jax.ShapeDtypeStruct(s, d) for s, d in shapes],
        compiler_params=pltpu.CompilerParams(vmem_limit_bytes=VMEM_GRANT),
        cost_estimate=cost(10**9, 10**6),
    )(raw, bias, rate, rotv, bterm)


def heads_kernel(stretch, numbers, ids, *refs):
    pieces = refs[: 3 * len(numbers)]
    (cos_ref, sin_ref, rotv_ref, bterm_ref, prev_ref, across_ref, down_ref, step_ref,
     first_ref, arrived_ref, skip_ref) = refs[3 * len(numbers) : 3 * len(numbers) + 11]
    outs = refs[-2 * len(numbers) :]
    tok = rotv_ref.shape[0]
    scale = HEAD_DIM ** (-0.5)
    power = scale * 1.4426950408889634
    later = (ids[2] > 0).astype(F32)
    blocked = (1.0 - later) * FAR_BELOW
    rows = lax.broadcasted_iota(jnp.int32, (stretch, stretch), 0)
    cols = lax.broadcasted_iota(jnp.int32, (stretch, stretch), 1)
    causal = cols <= rows
    last = (((1,), (1,)), ((), ()))
    ones = jnp.ones((tok, HEAD_DIM), BF16)
    own_keys = rotv_ref[:, :HEAD_DIM]
    prev_keys = prev_ref[:, :HEAD_DIM]
    own_values = jnp.concatenate([rotv_ref[:, HEAD_DIM:], ones], axis=1)
    prev_values = jnp.concatenate([prev_ref[:, HEAD_DIM:], ones], axis=1)
    for at, head in enumerate(numbers):
        keep_ref, u_ref, z_ref = pieces[3 * at : 3 * at + 3]
        teacher_ref, student_ref = outs[2 * at : 2 * at + 2]
        query = keep_ref[...] + u_ref[...].astype(F32) + z_ref[...].astype(F32)
        turned = turn(query, cos_ref[...], sin_ref[...]).astype(BF16)
        cterm = query.astype(BF16)
        state = arrived_ref[head].astype(F32) * later
        skip = skip_ref[0, head]
        for index in range(tok // stretch):
            span = slice(index * stretch, (index + 1) * stretch)
            queries = turned[span]
            far = lax.dot_general(queries, prev_keys, last, preferred_element_type=F32) + blocked
            near = lax.dot_general(
                queries, own_keys[: (index + 1) * stretch], last, preferred_element_type=F32
            )
            diagonal = jnp.where(causal, near[:, index * stretch :], FAR_BELOW)
            near = diagonal if index == 0 else jnp.concatenate([near[:, : index * stretch], diagonal], axis=1)
            top = jnp.maximum(jnp.max(far, axis=1, keepdims=True), jnp.max(near, axis=1, keepdims=True))
            far = jnp.exp2((far - top) * power).astype(BF16)
            near = jnp.exp2((near - top) * power).astype(BF16)
            mixed = jnp.dot(far, prev_values, preferred_element_type=F32) + jnp.dot(
                near, own_values[: (index + 1) * stretch], preferred_element_type=F32
            )
            teacher_ref[span, :] = (mixed[:, :HEAD_DIM] / mixed[:, HEAD_DIM:]).astype(BF16)
            values = rotv_ref[span, HEAD_DIM:]
            down = down_ref[span, head : head + 1]
            across = across_ref[head : head + 1, span]
            gram = lax.dot_general(
                cterm[span], bterm_ref[span, :], last, preferred_element_type=F32
            ) * (step_ref[head : head + 1, span] * scale)
            mix = jnp.where(causal, jnp.exp(jnp.where(causal, down - across, -1e4)) * gram, 0.0)
            inner = jnp.dot(mix.astype(BF16), values, preferred_element_type=F32)
            high = state.astype(BF16)
            low = (state - high.astype(F32)).astype(BF16)
            carried = jnp.dot(cterm[span], high, preferred_element_type=F32) + jnp.dot(
                cterm[span], low, preferred_element_type=F32
            )
            carried = carried * (jnp.exp(down) * scale)
            student_ref[span, :] = (inner + carried + skip * values.astype(F32)).astype(BF16)
            if index == 0:
                ends = jnp.exp(across[:, stretch - 1 :])
                state = ends * state + first_ref[head]


def heads_call(ids, numbers, pieces, shared):
    tok = shared[2].shape[0]
    wide = lambda a, col: pl.BlockSpec((tok, LANES), lambda step, ids, col=col: (0, col))
    flat = lambda a: pl.BlockSpec(a.shape, lambda step, ids, n=a.ndim: (0,) * n)
    specs, args = [], []
    for keep, u, z in pieces:
        specs += [wide(keep, 1), wide(u, 1), wide(z, 0)]
        args += [keep, u, z]
    specs += [flat(a) for a in shared[:-1]] + [pl.BlockSpec(memory_space=pltpu.SMEM)]
    count = 2 * len(numbers)
    return pl.pallas_call(
        functools.partial(heads_kernel, STRETCH, numbers),
        grid_spec=pltpu.PrefetchScalarGridSpec(
            num_scalar_prefetch=1,
            grid=(1,),
            in_specs=specs,
            out_specs=[pl.BlockSpec((tok, LANES), lambda step, ids: (0, 0))] * count,
        ),
        out_shape=[jax.ShapeDtypeStruct((tok, LANES), BF16)] * count,
        compiler_params=pltpu.CompilerParams(vmem_limit_bytes=VMEM_GRANT),
        cost_estimate=cost(2 * 10**9, 3 * 10**6),
    )(ids, *args, *shared)


def pair_body(layer_input, attn_weight, rate_weight, rate_bias, decay_rate, skip_gain):
    tok, share = layer_input.shape
    rows = attn_weight.shape[0]
    heads = rate_bias.shape[0]
    group = HEADS // KV_HEADS
    grp = lax.axis_index("grp")
    seq = lax.axis_index("seq")
    high, low = grp // 2, grp % 2
    ids = jnp.stack([high, low, seq]).astype(jnp.int32)
    count = lax.axis_size("grp")
    swap_high = [(g, g ^ 2) for g in range(count)]
    swap_low = [(g, g ^ 1) for g in range(count)]
    swap_seq = [(0, 1), (1, 0)]
    onward = [(0, 1)]
    over_high = lambda a: lax.ppermute(a, "grp", swap_high)
    over_low = lambda a: lax.ppermute(a, "grp", swap_low)
    over_seq = lambda a: lax.ppermute(a, "seq", swap_seq)

    other = over_seq(lax.dynamic_slice_in_dim(layer_input, (1 - seq) * rows, rows, 1))
    weights = jnp.transpose(attn_weight, (1, 0, 2))
    other_block = lambda step, ids: (0, 0)
    own_block = lambda step, ids: (0, ids[2])

    raw = jnp.einsum("dh,td->ht", rate_weight, layer_input, preferred_element_type=F32)
    raw = lax.dynamic_slice_in_dim(raw, high * 2 * heads, 2 * heads, 0) + over_high(
        lax.dynamic_slice_in_dim(raw, (1 - high) * 2 * heads, 2 * heads, 0)
    )
    raw = lax.dynamic_slice_in_dim(raw, low * heads, heads, 0) + over_low(
        lax.dynamic_slice_in_dim(raw, (1 - low) * heads, heads, 0)
    )

    cosine, sine = rope_angles(seq * tok + jnp.arange(tok, dtype=jnp.int32))
    cosine = jnp.concatenate([cosine, cosine], axis=1)
    sine = jnp.concatenate([-sine, sine], axis=1)

    def pair_places(col):
        return [
            lambda h, l: (1 - h, col), lambda h, l: (1 - h, col + 1),
            lambda h, l: (h, col), lambda h, l: (h, col + 1),
        ]

    def high_places(j):
        return [
            lambda h, l: (1 - h, (1 - l) * heads + j), lambda h, l: (1 - h, l * heads + j),
            lambda h, l: (h, (1 - l) * heads + j), lambda h, l: (h, l * heads + j),
        ]

    def low_places(j):
        return [
            lambda h, l: (1 - h, (1 - l) * heads + j), lambda h, l: (h, (1 - l) * heads + j),
            lambda h, l: (1 - h, l * heads + j), lambda h, l: (h, l * heads + j),
        ]

    half = heads // 2
    plan = [("kv", None, pair_places(group), over_high, over_low)]
    for j in range(half):
        plan.append(("q", j, high_places(j), over_high, over_low))
        plan.append(("q", half + j, low_places(half + j), over_low, over_high))
    crossed = [
        over_seq(project(ids, other, other_block, weights, places))
        for _, _, places, _, _ in plan
    ]
    pieces = {}
    for (kind, j, places, first, second), received in zip(plan, crossed):
        send, keep = project_add(ids, layer_input, own_block, weights, places, received)
        u = first(send)
        if kind == "kv":
            z = second((keep + u.astype(F32)).astype(BF16))
            rotv, bterm = keys_call(keep, u, z, cosine, sine)
            prev = lax.ppermute(rotv, "seq", onward)
            across, down, step, first_state, last_state = states_call(
                raw, rate_bias[:, None], decay_rate[:, None], rotv, bterm
            )
            arrived = lax.ppermute(last_state, "seq", onward)
        else:
            z = second((keep[:, :LANES] + u[:, :LANES].astype(F32)).astype(BF16))
            pieces[j] = (keep, u, z)
    shared = (
        cosine, sine, rotv, bterm, prev, across, down, step, first_state, arrived, skip_gain[None, :],
    )
    teacher, student = [None] * heads, [None] * heads
    for j in range(half):
        numbers = (j, half + j)
        outs = heads_call(ids, numbers, [pieces[n] for n in numbers], shared)
        for at, n in enumerate(numbers):
            teacher[n], student[n] = outs[2 * at], outs[2 * at + 1]
    return jnp.concatenate(teacher, axis=1), jnp.concatenate(student, axis=1)


def solution(mesh):
    placed = (
        P("seq", "grp"),
        P(("grp", "seq"), "mdl", None),
        P("grp", "mdl"),
        P(("mdl", "grp")),
        P(("mdl", "grp")),
        P(("mdl", "grp")),
    )
    chips = mesh.shape["grp"] * mesh.shape["mdl"]
    paired = (
        mesh.shape["seq"] == 2
        and mesh.shape["grp"] == 4
        and KV_HEADS == 2 * mesh.shape["mdl"]
        and HEADS // chips == 4
    )
    return jax.shard_map(
        pair_body if paired else body,
        mesh=mesh,
        in_specs=placed,
        out_specs=(P("seq", ("mdl", "grp")), P("seq", ("mdl", "grp"))),
        check_vma=False,
    )
```

```python
import functools
import math

import jax
import jax.numpy as jnp
from jax import lax
from jax.experimental import pallas as pl
from jax.experimental.pallas import tpu as pltpu
from jax.sharding import PartitionSpec as P


HEADS = 64
KV_HEADS = 8
HEAD_DIM = 128
STRETCH = 256


ROPE_BASE = 500000.0
FAR_BELOW = -1e30


def rope_angles(positions):
    half = HEAD_DIM // 2
    freq = ROPE_BASE ** (-2.0 * jnp.arange(half, dtype=jnp.float32) / HEAD_DIM)
    angle = positions.astype(jnp.float32)[:, None] * freq[None, :]
    return (jnp.cos(angle), jnp.sin(angle))


def rotate(vectors, cosine, sine):
    half = vectors.shape[-1] // 2
    first = vectors[..., :half]
    second = vectors[..., half:]
    cosine = cosine[:, None, :]
    sine = sine[:, None, :]
    return jnp.concatenate(
        [first * cosine - second * sine, second * cosine + first * sine], axis=-1
    )


def state_product(cterm, state):
    high = state.astype(jnp.bfloat16)
    low = (state - high.astype(jnp.float32)).astype(jnp.bfloat16)
    upper = jnp.einsum("thn,hnp->thp", cterm, high, preferred_element_type=jnp.float32)
    return upper + jnp.einsum("thn,hnp->thp", cterm, low, preferred_element_type=jnp.float32)


def key_absorber(queries, own_first, scale, carry, piece):
    top, total, accum = carry
    keys, values = piece
    scores = jnp.einsum("thd,nd->thn", queries, keys, preferred_element_type=jnp.float32) * scale
    query_pos = own_first + jnp.arange(queries.shape[0], dtype=jnp.int32)
    key_pos = jnp.arange(keys.shape[0], dtype=jnp.int32)
    causal = (key_pos[None, :] <= query_pos[:, None])[:, None, :]
    masked = jnp.where(causal, scores, FAR_BELOW)
    new_top = jnp.maximum(top, jnp.max(masked, axis=2))
    weights = jnp.where(causal, jnp.exp(masked - new_top[:, :, None]), 0.0)
    total = jnp.sum(weights, axis=2)
    accum = jnp.einsum(
        "thn,nd->thd", weights.astype(jnp.bfloat16), values, preferred_element_type=jnp.float32
    )
    return (new_top, total, accum)


def body(layer_input, attn_weight, rate_weight, rate_bias, decay_rate, skip_gain):
    tok = layer_input.shape[0]
    kv_local = attn_weight.shape[1]
    heads_local = rate_bias.shape[0]
    group = HEADS // KV_HEADS
    scale = HEAD_DIM ** (-0.5)
    merged = jnp.einsum(
        "td,dkc->tkc",
        layer_input,
        lax.all_gather(attn_weight, "seq", axis=0, tiled=True),
        preferred_element_type=jnp.float32,
    )
    rate_part = jnp.dot(layer_input, rate_weight, preferred_element_type=jnp.float32)
    grp_index = lax.axis_index("grp")
    summed, rate_whole = (
        lax.psum(merged.astype(jnp.bfloat16), "grp").astype(jnp.float32),
        lax.psum(rate_part.astype(jnp.bfloat16), "grp").astype(jnp.float32),
    )
    query_whole = summed[:, :, : group * HEAD_DIM].reshape(tok, kv_local * group * HEAD_DIM)
    query_flat = lax.dynamic_slice_in_dim(
        query_whole, grp_index * heads_local * HEAD_DIM, heads_local * HEAD_DIM, 1
    )
    raw = lax.dynamic_slice_in_dim(rate_whole, grp_index * heads_local, heads_local, 1)
    pairs = summed[:, :, group * HEAD_DIM :]
    kv_index = grp_index * heads_local // group
    pair = lax.dynamic_index_in_dim(pairs, kv_index, 1, keepdims=False)
    keys = pair[:, :HEAD_DIM]
    values = pair[:, HEAD_DIM:].astype(jnp.bfloat16)
    query = query_flat.reshape(tok, heads_local, HEAD_DIM)
    own_first = lax.axis_index("seq") * tok
    cosine, sine = rope_angles(own_first + jnp.arange(tok, dtype=jnp.int32))
    rot_query = rotate(query, cosine, sine).astype(jnp.bfloat16)
    rot_keys = rotate(keys[:, None, :], cosine, sine)[:, 0].astype(jnp.bfloat16)
    start_carry = (
        jnp.full((tok, heads_local), FAR_BELOW, jnp.float32),
        jnp.zeros((tok, heads_local), jnp.float32),
        jnp.zeros((tok, heads_local, HEAD_DIM), jnp.float32),
    )
    _, total, accum = key_absorber(
        rot_query,
        own_first,
        scale,
        start_carry,
        (
            lax.all_gather(rot_keys, "seq", axis=0, tiled=True),
            lax.all_gather(values, "seq", axis=0, tiled=True),
        ),
    )
    teacher = (accum / total[:, :, None]).astype(jnp.bfloat16).reshape(tok, heads_local * HEAD_DIM)
    step = jax.nn.softplus(raw + rate_bias[None, :])
    log_decay = -decay_rate[None, :] * step
    c_all = query.astype(jnp.bfloat16)
    b_all = keys.astype(jnp.bfloat16)
    causal = (
        jnp.arange(STRETCH, dtype=jnp.int32)[:, None]
        >= jnp.arange(STRETCH, dtype=jnp.int32)[None, :]
    )[None]
    state = jnp.zeros((heads_local, HEAD_DIM, HEAD_DIM), jnp.float32)
    before = jnp.zeros((heads_local,), jnp.float32)
    partials = []
    offsets = []
    for index in range(tok // STRETCH):
        first = index * STRETCH
        cpart = c_all[first : first + STRETCH]
        bpart = b_all[first : first + STRETCH]
        xpart = values[first : first + STRETCH]
        decay = log_decay[first : first + STRETCH]
        rate = step[first : first + STRETCH]
        cum = jnp.cumsum(decay, axis=0)
        gram = jnp.einsum("thn,sn->hts", cpart, bpart, preferred_element_type=jnp.float32) * scale
        diff = cum.T[:, :, None] - cum.T[:, None, :]
        mix = jnp.where(
            causal, jnp.exp(jnp.where(causal, diff, -10000.0)) * rate.T[:, None, :] * gram, 0.0
        ).astype(jnp.bfloat16)
        intra = jnp.einsum("hts,sp->thp", mix, xpart, preferred_element_type=jnp.float32)
        carried = state_product(cpart, state) * scale * jnp.exp(cum)[:, :, None]
        weighted = (
            (jnp.exp(cum[-1][None, :] - cum) * rate)[:, :, None]
            * bpart.astype(jnp.float32)[:, None, :]
        ).astype(jnp.bfloat16)
        contribution = jnp.einsum(
            "shn,sp->hnp", weighted, xpart, preferred_element_type=jnp.float32
        )
        state = jnp.exp(cum[-1])[:, None, None] * state + contribution
        partials.append(intra + carried)
        offsets.append(cum + before[None, :])
        before = before + cum[-1]
    totals, states = (
        lax.all_gather(before[None, :].astype(jnp.bfloat16), "seq", axis=0, tiled=True).astype(
            jnp.float32
        ),
        lax.all_gather(state[None].astype(jnp.bfloat16), "seq", axis=0, tiled=True).astype(
            jnp.float32
        ),
    )
    position = lax.axis_index("seq")
    order = jnp.arange(totals.shape[0], dtype=jnp.int32)
    between = ((order[:, None] < order[None, :]) & (order[None, :] < position)).astype(jnp.float32)
    span = jnp.dot(between, totals, precision=lax.Precision.HIGHEST)
    reach_back = jnp.where(order[:, None] < position, jnp.exp(span), 0.0)
    incoming = jnp.einsum("dh,dhnp->hnp", reach_back, states, precision=lax.Precision.HIGHEST)
    inside = jnp.concatenate(partials, axis=0)
    reach = jnp.exp(jnp.concatenate(offsets, axis=0))
    arriving = state_product(c_all, incoming) * scale * reach[:, :, None]
    skipped = skip_gain[None, :, None] * values.astype(jnp.float32)[:, None, :]
    student = (
        (inside + arriving + skipped).astype(jnp.bfloat16).reshape(tok, heads_local * HEAD_DIM)
    )
    return (teacher, student)


LANES = 128
EXTRA = 16
VMEM_GRANT = 24 * 1024 * 1024
F32 = jnp.float32
BF16 = jnp.bfloat16
LAST = (((1,), (1,)), ((), ()))


def cost(flops, moved):
    return pl.CostEstimate(flops=flops, bytes_accessed=moved, transcendentals=0)


def joined(refs):
    return jnp.concatenate([ref[(0,) * (len(ref.shape) - 2)] for ref in refs], axis=1)


def project_kernel(ids, x_ref, w0, w1, w2, w3, out_ref):
    out_ref[...] = jnp.dot(
        x_ref[...], joined((w0, w1, w2, w3)), preferred_element_type=F32
    ).astype(BF16)


def add_halves(x_ref, w0, w1, w2, w3, r_ref, send_ref, keep_ref):
    tok, half = keep_ref.shape
    first = jnp.dot(x_ref[...], joined((w0, w1)), preferred_element_type=F32)
    send_ref[:tok, :] = (first + r_ref[:, :half].astype(F32)).astype(BF16)
    second = jnp.dot(x_ref[...], joined((w2, w3)), preferred_element_type=F32)
    keep_ref[...] = second + r_ref[:, half:].astype(F32)


def project_add_kernel(ids, *refs):
    add_halves(*refs)


def folded(rates):
    half = rates.shape[1] // 2
    return jnp.concatenate([rates[:, :half], rates[:, half:]], axis=0)


def unfolded(rows):
    half = rows.shape[0] // 2
    return jnp.concatenate([rows[:half], rows[half:]], axis=1)


def project_pair_kernel(ids, raw_ref, *refs):
    add_halves(*refs)
    send_ref, tok = refs[-2], refs[-1].shape[0]
    away = EXTRA // 2
    rates = jnp.where(ids[0] == 0, raw_ref[away:, :], raw_ref[:away, :])
    send_ref[tok:, :] = folded(rates).astype(BF16)


def own_rates(ids, raw_ref, u_ref):
    tok = raw_ref.shape[1]
    own = EXTRA // 2
    rates = jnp.where(ids[0] == 0, raw_ref[:own, :], raw_ref[own:, :])
    return rates + unfolded(u_ref[tok:, :].astype(F32))


def pair_middle_kernel(ids, raw_ref, keep_ref, u_ref, send_ref):
    tok = keep_ref.shape[0]
    send_ref[:tok, :] = (keep_ref[...] + u_ref[:tok, :].astype(F32)).astype(BF16)
    send_ref[tok:, :] = folded(own_rates(ids, raw_ref, u_ref)).astype(BF16)


def middle_kernel(ids, keep_ref, u_ref, send_ref):
    send_ref[...] = (keep_ref[...] + u_ref[...].astype(F32)).astype(BF16)


def prepare_kernel(ids, x_ref, rates_ref, raw_ref, cos_ref, sin_ref):
    raw_ref[...] = lax.dot_general(
        rates_ref[...], x_ref[...], LAST, preferred_element_type=F32
    )
    tok, wide = cos_ref.shape
    half = wide // 2
    row = lax.broadcasted_iota(jnp.int32, (tok, wide), 0) + ids[2] * tok
    lane = lax.broadcasted_iota(jnp.int32, (1, wide), 1)
    slot = jnp.where(lane < half, lane, lane - half).astype(F32)
    freq = jnp.exp(slot * (-2.0 / wide * math.log(ROPE_BASE)))
    angle = row.astype(F32) * freq
    cos_ref[...] = jnp.cos(angle)
    sine = jnp.sin(angle)
    sin_ref[...] = jnp.where(lane < half, -sine, sine)


def weight_spec(weights, place):
    ndim = weights.ndim
    block = (1,) * (ndim - 2) + (weights.shape[-2], LANES)
    return pl.BlockSpec(block, lambda step, ids: place(ids[0], ids[1]))


def flat(shape):
    return pl.BlockSpec(shape, lambda step, ids, n=len(shape): (0,) * n)


def call(kernel, ids, specs, args, shapes, flops, aliases={}, out_specs=None):
    return pl.pallas_call(
        kernel,
        grid_spec=pltpu.PrefetchScalarGridSpec(
            num_scalar_prefetch=1,
            grid=(1,),
            in_specs=specs,
            out_specs=out_specs or [flat(s) for s, _ in shapes],
        ),
        out_shape=[jax.ShapeDtypeStruct(s, d) for s, d in shapes],
        input_output_aliases=aliases,
        compiler_params=pltpu.CompilerParams(vmem_limit_bytes=VMEM_GRANT),
        cost_estimate=cost(flops, 3 * 10**6),
    )(ids, *args)


def project(ids, x, x_block, weights, places):
    tok, rows = x.shape[0], weights.shape[-2]
    wide = len(places) * LANES
    specs = [pl.BlockSpec((tok, rows), x_block)]
    specs += [weight_spec(weights, place) for place in places]
    args = [x] + [weights] * len(places)
    return call(project_kernel, ids, specs, args, [((tok, wide), BF16)], 2 * tok * rows * wide)[0]


def project_add(ids, x, x_block, weights, places, received, raw=None):
    tok, rows = x.shape[0], weights.shape[-2]
    wide = len(places) * LANES
    half = wide // 2
    specs = [pl.BlockSpec((tok, rows), x_block)]
    specs += [weight_spec(weights, place) for place in places] + [flat(received.shape)]
    args = [x] + [weights] * len(places) + [received]
    tall, kernel = tok, project_add_kernel
    if raw is not None:
        specs, args = [flat(raw.shape)] + specs, [raw] + args
        tall, kernel = tok + EXTRA, project_pair_kernel
    shapes = [((tall, half), BF16), ((tok, half), F32)]
    return call(kernel, ids, specs, args, shapes, 2 * tok * rows * wide)


def turn(vectors, cosine, sine):
    return vectors * cosine + pltpu.roll(vectors, HEAD_DIM // 2, 1) * sine


def split_sum(rows, mask):
    high = rows.astype(BF16)
    rest = rows - high.astype(F32)
    middle = rest.astype(BF16)
    low = (rest - middle.astype(F32)).astype(BF16)
    count = rows.shape[0]
    parts = jnp.concatenate([high.astype(F32), middle.astype(F32), low.astype(F32)], axis=0)
    sums = lax.dot_general(parts.astype(BF16), mask, LAST, preferred_element_type=F32)
    return sums[:count] + (sums[count : 2 * count] + sums[2 * count :])


def context_kernel(
    stretch, ids, raw_ref, keep_ref, u_ref, z_ref, cos_ref, sin_ref, bias_ref, rate_ref,
    carry_ref, bterm_ref, across_ref, down_ref, step_ref, first_ref,
):
    tok = keep_ref.shape[0]
    heads = bias_ref.shape[0]
    spans = tok // stretch
    pair = keep_ref[...] + u_ref[:tok, :].astype(F32) + z_ref[:tok, :].astype(F32)
    keys = pair[:, :HEAD_DIM]
    values = pair[:, HEAD_DIM:].astype(BF16)
    bterm = keys.astype(BF16)
    carry_ref[:tok, :HEAD_DIM] = turn(keys, cos_ref[...], sin_ref[...]).astype(BF16)
    carry_ref[:tok, HEAD_DIM:] = values
    bterm_ref[...] = bterm
    both = own_rates(ids, raw_ref, u_ref) + unfolded(z_ref[tok:, :].astype(F32))
    raw = jnp.where(ids[1] == 0, both[:heads], both[heads:])
    step = jax.nn.softplus(raw + bias_ref[...])
    decay = -rate_ref[...] * step
    rows = lax.broadcasted_iota(jnp.int32, (stretch, stretch), 0)
    cols = lax.broadcasted_iota(jnp.int32, (stretch, stretch), 1)
    below = (cols <= rows).astype(F32).astype(BF16)
    fold = lambda a: jnp.concatenate([a[:, i * stretch : (i + 1) * stretch] for i in range(spans)], axis=0)
    across = split_sum(fold(decay), below)
    steps = fold(step)
    tails = jnp.exp(across[:, stretch - 1 :] - across) * steps
    across_ref[...] = across
    step_ref[...] = steps
    count = heads * spans
    filler = jnp.zeros((LANES - 2 * count, stretch), F32)
    down = jnp.transpose(jnp.concatenate([across, tails, filler], axis=0))
    down_ref[...] = down
    states = [None] * heads
    for index in range(spans):
        span = slice(index * stretch, (index + 1) * stretch)
        part = bterm[span].astype(F32)
        weighted = jnp.concatenate(
            [
                (part * down[:, count + index * heads + h : count + index * heads + h + 1]).astype(BF16)
                for h in range(heads)
            ],
            axis=1,
        )
        fresh = lax.dot_general(
            weighted, values[span], (((0,), (0,)), ((), ())), preferred_element_type=F32
        )
        for h in range(heads):
            new = fresh[h * HEAD_DIM : (h + 1) * HEAD_DIM]
            if index > 0:
                at = index * heads + h
                new = new + jnp.exp(across[at : at + 1, stretch - 1 :]) * states[h]
            else:
                first_ref[h] = new
            states[h] = new
    for h in range(heads):
        row, col = tok + (h // 2) * HEAD_DIM, (h % 2) * HEAD_DIM
        carry_ref[row : row + HEAD_DIM, col : col + HEAD_DIM] = states[h].astype(BF16)


def heads_kernel(stretch, numbers, ids, *refs):
    refs = list(refs)
    pieces = refs[: 3 * len(numbers)]
    (cos_ref, sin_ref, carry_ref, bterm_ref, came_ref, across_ref, down_ref, step_ref,
     first_ref, skip_ref) = refs[3 * len(numbers) : 3 * len(numbers) + 10]
    teacher_ref, student_ref = refs[-2:]
    tok = bterm_ref.shape[0]
    heads = first_ref.shape[0]
    scale = HEAD_DIM ** (-0.5)
    power = scale * 1.4426950408889634
    later = (ids[2] > 0).astype(F32)
    blocked = (1.0 - later) * FAR_BELOW
    rows = lax.broadcasted_iota(jnp.int32, (stretch, stretch), 0)
    cols = lax.broadcasted_iota(jnp.int32, (stretch, stretch), 1)
    causal = cols <= rows
    ones = jnp.ones((tok, HEAD_DIM), BF16)
    own_keys = carry_ref[:tok, :HEAD_DIM]
    prev_keys = came_ref[:tok, :HEAD_DIM]
    own_values = jnp.concatenate([carry_ref[:tok, HEAD_DIM:], ones], axis=1)
    prev_values = jnp.concatenate([came_ref[:tok, HEAD_DIM:], ones], axis=1)
    for at, head in enumerate(numbers):
        keep_ref, u_ref, z_ref = pieces[3 * at : 3 * at + 3]
        place = slice(at * HEAD_DIM, (at + 1) * HEAD_DIM)
        query = keep_ref[...] + u_ref[...].astype(F32) + z_ref[...].astype(F32)
        turned = turn(query, cos_ref[...], sin_ref[...]).astype(BF16)
        cterm = query.astype(BF16)
        row, col = tok + (head // 2) * HEAD_DIM, (head % 2) * HEAD_DIM
        state = came_ref[row : row + HEAD_DIM, col : col + HEAD_DIM].astype(F32) * later
        skip = skip_ref[0, head]
        for index in range(tok // stretch):
            span = slice(index * stretch, (index + 1) * stretch)
            reach = (index + 1) * stretch
            queries = turned[span]
            far = lax.dot_general(queries, prev_keys, LAST, preferred_element_type=F32) + blocked
            near = lax.dot_general(queries, own_keys[:reach], LAST, preferred_element_type=F32)
            diagonal = jnp.where(causal, near[:, index * stretch :], FAR_BELOW)
            if index > 0:
                near = jnp.concatenate([near[:, : index * stretch], diagonal], axis=1)
            else:
                near = diagonal
            top = jnp.maximum(
                jnp.max(far, axis=1, keepdims=True), jnp.max(near, axis=1, keepdims=True)
            )
            far = jnp.exp2((far - top) * power).astype(BF16)
            near = jnp.exp2((near - top) * power).astype(BF16)
            mixed = jnp.dot(far, prev_values, preferred_element_type=F32) + jnp.dot(
                near, own_values[:reach], preferred_element_type=F32
            )
            teacher_ref[span, place] = (mixed[:, :HEAD_DIM] / mixed[:, HEAD_DIM:]).astype(BF16)
            values = carry_ref[span, HEAD_DIM:]
            which = index * heads + head
            down = down_ref[:, which : which + 1]
            across = across_ref[which : which + 1, :]
            gram = lax.dot_general(
                cterm[span], bterm_ref[span, :], LAST, preferred_element_type=F32
            ) * (step_ref[which : which + 1, :] * scale)
            mix = jnp.where(causal, jnp.exp(jnp.where(causal, down - across, -1e4)) * gram, 0.0)
            inner = jnp.dot(mix.astype(BF16), values, preferred_element_type=F32)
            high = state.astype(BF16)
            low = (state - high.astype(F32)).astype(BF16)
            carried = jnp.dot(
                cterm[span], jnp.concatenate([high, low], axis=1), preferred_element_type=F32
            )
            carried = (carried[:, :HEAD_DIM] + carried[:, HEAD_DIM:]) * (jnp.exp(down) * scale)
            student_ref[span, place] = (inner + carried + skip * values.astype(F32)).astype(BF16)
            if index == 0:
                state = jnp.exp(across[:, stretch - 1 :]) * state + first_ref[head]


def heads_call(ids, group_at, numbers, pieces, shared, total, before):
    tok = pieces[0][0].shape[0]
    column = lambda col: pl.BlockSpec((tok, LANES), lambda step, ids, col=col: (0, col))
    specs, args = [], []
    for keep, u, z in pieces:
        specs += [column(1), column(1), column(0)]
        args += [keep, u, z]
    specs += [flat(a.shape) for a in shared[:-1]] + [pl.BlockSpec(memory_space=pltpu.SMEM)]
    args += list(shared)
    aliases = {}
    if before is not None:
        aliases = {1 + len(args): 0, 2 + len(args): 1}
        specs += [pl.BlockSpec(memory_space=pl.ANY)] * 2
        args += list(before)
    wide = len(numbers) * LANES
    block = pl.BlockSpec((tok, wide), lambda step, ids: (0, group_at))
    return call(
        functools.partial(heads_kernel, STRETCH, numbers),
        ids, specs, args, [((tok, total), BF16)] * 2, 2 * 10**9, aliases, [block] * 2,
    )


def pair_body(*args):
    return pair_steps(*args)


def pair_steps(layer_input, attn_weight, rate_weight, rate_bias, decay_rate, skip_gain):
    tok, _ = layer_input.shape
    heads = rate_bias.shape[0]
    group = HEADS // KV_HEADS
    grp = lax.axis_index("grp")
    seq = lax.axis_index("seq")
    ids = jnp.stack([grp // 2, grp % 2, seq]).astype(jnp.int32)
    count = lax.axis_size("grp")
    swap_high = [(g, g ^ 2) for g in range(count)]
    swap_low = [(g, g ^ 1) for g in range(count)]
    over_high = lambda a: lax.ppermute(a, "grp", swap_high)
    over_low = lambda a: lax.ppermute(a, "grp", swap_low)
    over_seq = lambda a: lax.ppermute(a, "seq", [(0, 1), (1, 0)])
    own_block = lambda step, ids: (0, ids[2])

    other = over_seq(layer_input)
    queries = group * HEAD_DIM
    pair_weights = jnp.transpose(attn_weight[:, :, queries:], (1, 0, 2))
    head_weights = jnp.transpose(attn_weight[:, :, :queries], (1, 0, 2))
    args = [layer_input, rate_weight.T]
    shapes = [((EXTRA, tok), F32), ((tok, HEAD_DIM), F32), ((tok, HEAD_DIM), F32)]
    raw, cosine, sine = call(
        prepare_kernel, ids, [flat(a.shape) for a in args], args, shapes, 10**9
    )

    pair_places = [
        lambda h, l: (1 - h, 0, 0), lambda h, l: (1 - h, 0, 1),
        lambda h, l: (h, 0, 0), lambda h, l: (h, 0, 1),
    ]

    def high_places(j):
        return [
            lambda h, l: (1 - h, 0, (1 - l) * heads + j), lambda h, l: (1 - h, 0, l * heads + j),
            lambda h, l: (h, 0, (1 - l) * heads + j), lambda h, l: (h, 0, l * heads + j),
        ]

    def low_places(j):
        return [
            lambda h, l: (1 - h, 0, (1 - l) * heads + j), lambda h, l: (h, 0, (1 - l) * heads + j),
            lambda h, l: (1 - h, 0, l * heads + j), lambda h, l: (h, 0, l * heads + j),
        ]

    other, pair_weights, head_weights = lax.optimization_barrier((other, pair_weights, head_weights))
    plan = [(None, pair_weights, pair_places, over_high, over_low)]
    for pair in range(heads // 2):
        plan.append((2 * pair + 1, head_weights, low_places(2 * pair + 1), over_low, over_high))
        plan.append((2 * pair, head_weights, high_places(2 * pair), over_high, over_low))
    ahead = [ids]

    def queued(make):
        ready, _ = lax.optimization_barrier((ids, ahead[0]))
        outs = make(ready)
        ahead[0] = outs[0]
        return outs

    crossed, parts, arrived, pieces, kept = {}, {}, {}, {}, {}

    def cross(at):
        _, weights, places, _, _ = plan[at]
        out = queued(lambda ready: [project(ready, other, own_block, weights, places)])[0]
        crossed[at] = over_seq(out)

    def mine(at):
        j, weights, places, first, _ = plan[at]
        send, kept[at] = queued(
            lambda ready: project_add(
                ready, layer_input, own_block, weights, places, crossed[at],
                raw if j is None else None,
            )
        )
        parts[at] = first(send)

    def middle(at):
        j, _, _, _, second = plan[at]
        keep, u = kept[at], parts[at]
        if j is None:
            args = [raw, keep, u]
            shapes = [((tok + EXTRA, 2 * HEAD_DIM), BF16)]
            send = queued(
                lambda ready: call(
                    pair_middle_kernel, ready, [flat(a.shape) for a in args], args, shapes, 10**7
                )
            )[0]
        else:
            specs = [pl.BlockSpec((tok, LANES), lambda step, ids: (0, 0))] * 2
            send = queued(
                lambda ready: call(
                    middle_kernel, ready, specs, [keep, u], [((tok, LANES), BF16)], 10**7
                )
            )[0]
        arrived[at] = second(send)
        if j is not None:
            pieces[j] = (keep, u, arrived[at])

    def context():
        args = [
            raw, kept[0], parts[0], arrived[0], cosine, sine, rate_bias[:, None], decay_rate[:, None],
        ]
        spans = tok // STRETCH
        shapes = [
            ((tok + heads // 2 * HEAD_DIM, 2 * HEAD_DIM), BF16), ((tok, HEAD_DIM), BF16),
            ((heads * spans, STRETCH), F32), ((STRETCH, LANES), F32), ((heads * spans, STRETCH), F32),
            ((heads, HEAD_DIM, HEAD_DIM), F32),
        ]
        carry, *rest = queued(
            lambda ready: call(
                functools.partial(context_kernel, STRETCH), ready,
                [flat(a.shape) for a in args], args, shapes, 10**9,
            )
        )
        came = over_seq(carry)
        bterm, across, down, step, first_state = rest
        return (
            cosine, sine, carry, bterm, came, across, down, step, first_state, skip_gain[None, :],
        )

    def tail(pair, shared, before):
        numbers = (2 * pair, 2 * pair + 1)
        return queued(
            lambda ready: heads_call(
                ready, pair, numbers, [pieces[n] for n in numbers], shared,
                heads * HEAD_DIM, before,
            )
        )

    cross(0)
    cross(1)
    mine(0)
    mine(1)
    cross(2)
    cross(3)
    mine(2)
    cross(4)
    middle(0)
    mine(3)
    mine(4)
    middle(1)
    middle(2)
    shared = context()
    middle(3)
    outs = tail(0, shared, None)
    middle(4)
    outs = tail(1, shared, outs)
    return outs[0], outs[1]


def solution(mesh):
    placed = (
        P("seq", "grp"),
        P(("grp", "seq"), "mdl", None),
        P("grp", "mdl"),
        P(("mdl", "grp")),
        P(("mdl", "grp")),
        P(("mdl", "grp")),
    )
    chips = mesh.shape["grp"] * mesh.shape["mdl"]
    paired = (
        mesh.shape["seq"] == 2
        and mesh.shape["grp"] == 4
        and KV_HEADS == 2 * mesh.shape["mdl"]
        and HEADS // chips == 4
    )
    return jax.shard_map(
        pair_body if paired else body,
        mesh=mesh,
        in_specs=placed,
        out_specs=(P("seq", ("mdl", "grp")), P("seq", ("mdl", "grp"))),
        check_vma=False,
    )
```

```python
import functools
import math

import jax
import jax.numpy as jnp
from jax import lax
from jax.experimental import pallas as pl
from jax.experimental.pallas import tpu as pltpu
from jax.sharding import PartitionSpec as P


HEADS = 64
KV_HEADS = 8
HEAD_DIM = 128
STRETCH = 256


ROPE_BASE = 500000.0
FAR_BELOW = -1e30


def rope_angles(positions):
    half = HEAD_DIM // 2
    freq = ROPE_BASE ** (-2.0 * jnp.arange(half, dtype=jnp.float32) / HEAD_DIM)
    angle = positions.astype(jnp.float32)[:, None] * freq[None, :]
    return (jnp.cos(angle), jnp.sin(angle))


def rotate(vectors, cosine, sine):
    half = vectors.shape[-1] // 2
    first = vectors[..., :half]
    second = vectors[..., half:]
    cosine = cosine[:, None, :]
    sine = sine[:, None, :]
    return jnp.concatenate(
        [first * cosine - second * sine, second * cosine + first * sine], axis=-1
    )


def state_product(cterm, state):
    high = state.astype(jnp.bfloat16)
    low = (state - high.astype(jnp.float32)).astype(jnp.bfloat16)
    upper = jnp.einsum("thn,hnp->thp", cterm, high, preferred_element_type=jnp.float32)
    return upper + jnp.einsum("thn,hnp->thp", cterm, low, preferred_element_type=jnp.float32)


def key_absorber(queries, own_first, scale, carry, piece):
    top, total, accum = carry
    keys, values = piece
    scores = jnp.einsum("thd,nd->thn", queries, keys, preferred_element_type=jnp.float32) * scale
    query_pos = own_first + jnp.arange(queries.shape[0], dtype=jnp.int32)
    key_pos = jnp.arange(keys.shape[0], dtype=jnp.int32)
    causal = (key_pos[None, :] <= query_pos[:, None])[:, None, :]
    masked = jnp.where(causal, scores, FAR_BELOW)
    new_top = jnp.maximum(top, jnp.max(masked, axis=2))
    weights = jnp.where(causal, jnp.exp(masked - new_top[:, :, None]), 0.0)
    total = jnp.sum(weights, axis=2)
    accum = jnp.einsum(
        "thn,nd->thd", weights.astype(jnp.bfloat16), values, preferred_element_type=jnp.float32
    )
    return (new_top, total, accum)


def body(layer_input, attn_weight, rate_weight, rate_bias, decay_rate, skip_gain):
    tok = layer_input.shape[0]
    kv_local = attn_weight.shape[1]
    heads_local = rate_bias.shape[0]
    group = HEADS // KV_HEADS
    scale = HEAD_DIM ** (-0.5)
    merged = jnp.einsum(
        "td,dkc->tkc",
        layer_input,
        lax.all_gather(attn_weight, "seq", axis=0, tiled=True),
        preferred_element_type=jnp.float32,
    )
    rate_part = jnp.dot(layer_input, rate_weight, preferred_element_type=jnp.float32)
    grp_index = lax.axis_index("grp")
    summed, rate_whole = (
        lax.psum(merged.astype(jnp.bfloat16), "grp").astype(jnp.float32),
        lax.psum(rate_part.astype(jnp.bfloat16), "grp").astype(jnp.float32),
    )
    query_whole = summed[:, :, : group * HEAD_DIM].reshape(tok, kv_local * group * HEAD_DIM)
    query_flat = lax.dynamic_slice_in_dim(
        query_whole, grp_index * heads_local * HEAD_DIM, heads_local * HEAD_DIM, 1
    )
    raw = lax.dynamic_slice_in_dim(rate_whole, grp_index * heads_local, heads_local, 1)
    pairs = summed[:, :, group * HEAD_DIM :]
    kv_index = grp_index * heads_local // group
    pair = lax.dynamic_index_in_dim(pairs, kv_index, 1, keepdims=False)
    keys = pair[:, :HEAD_DIM]
    values = pair[:, HEAD_DIM:].astype(jnp.bfloat16)
    query = query_flat.reshape(tok, heads_local, HEAD_DIM)
    own_first = lax.axis_index("seq") * tok
    cosine, sine = rope_angles(own_first + jnp.arange(tok, dtype=jnp.int32))
    rot_query = rotate(query, cosine, sine).astype(jnp.bfloat16)
    rot_keys = rotate(keys[:, None, :], cosine, sine)[:, 0].astype(jnp.bfloat16)
    start_carry = (
        jnp.full((tok, heads_local), FAR_BELOW, jnp.float32),
        jnp.zeros((tok, heads_local), jnp.float32),
        jnp.zeros((tok, heads_local, HEAD_DIM), jnp.float32),
    )
    _, total, accum = key_absorber(
        rot_query,
        own_first,
        scale,
        start_carry,
        (
            lax.all_gather(rot_keys, "seq", axis=0, tiled=True),
            lax.all_gather(values, "seq", axis=0, tiled=True),
        ),
    )
    teacher = (accum / total[:, :, None]).astype(jnp.bfloat16).reshape(tok, heads_local * HEAD_DIM)
    step = jax.nn.softplus(raw + rate_bias[None, :])
    log_decay = -decay_rate[None, :] * step
    c_all = query.astype(jnp.bfloat16)
    b_all = keys.astype(jnp.bfloat16)
    causal = (
        jnp.arange(STRETCH, dtype=jnp.int32)[:, None]
        >= jnp.arange(STRETCH, dtype=jnp.int32)[None, :]
    )[None]
    state = jnp.zeros((heads_local, HEAD_DIM, HEAD_DIM), jnp.float32)
    before = jnp.zeros((heads_local,), jnp.float32)
    partials = []
    offsets = []
    for index in range(tok // STRETCH):
        first = index * STRETCH
        cpart = c_all[first : first + STRETCH]
        bpart = b_all[first : first + STRETCH]
        xpart = values[first : first + STRETCH]
        decay = log_decay[first : first + STRETCH]
        rate = step[first : first + STRETCH]
        cum = jnp.cumsum(decay, axis=0)
        gram = jnp.einsum("thn,sn->hts", cpart, bpart, preferred_element_type=jnp.float32) * scale
        diff = cum.T[:, :, None] - cum.T[:, None, :]
        mix = jnp.where(
            causal, jnp.exp(jnp.where(causal, diff, -10000.0)) * rate.T[:, None, :] * gram, 0.0
        ).astype(jnp.bfloat16)
        intra = jnp.einsum("hts,sp->thp", mix, xpart, preferred_element_type=jnp.float32)
        carried = state_product(cpart, state) * scale * jnp.exp(cum)[:, :, None]
        weighted = (
            (jnp.exp(cum[-1][None, :] - cum) * rate)[:, :, None]
            * bpart.astype(jnp.float32)[:, None, :]
        ).astype(jnp.bfloat16)
        contribution = jnp.einsum(
            "shn,sp->hnp", weighted, xpart, preferred_element_type=jnp.float32
        )
        state = jnp.exp(cum[-1])[:, None, None] * state + contribution
        partials.append(intra + carried)
        offsets.append(cum + before[None, :])
        before = before + cum[-1]
    totals, states = (
        lax.all_gather(before[None, :].astype(jnp.bfloat16), "seq", axis=0, tiled=True).astype(
            jnp.float32
        ),
        lax.all_gather(state[None].astype(jnp.bfloat16), "seq", axis=0, tiled=True).astype(
            jnp.float32
        ),
    )
    position = lax.axis_index("seq")
    order = jnp.arange(totals.shape[0], dtype=jnp.int32)
    between = ((order[:, None] < order[None, :]) & (order[None, :] < position)).astype(jnp.float32)
    span = jnp.dot(between, totals, precision=lax.Precision.HIGHEST)
    reach_back = jnp.where(order[:, None] < position, jnp.exp(span), 0.0)
    incoming = jnp.einsum("dh,dhnp->hnp", reach_back, states, precision=lax.Precision.HIGHEST)
    inside = jnp.concatenate(partials, axis=0)
    reach = jnp.exp(jnp.concatenate(offsets, axis=0))
    arriving = state_product(c_all, incoming) * scale * reach[:, :, None]
    skipped = skip_gain[None, :, None] * values.astype(jnp.float32)[:, None, :]
    student = (
        (inside + arriving + skipped).astype(jnp.bfloat16).reshape(tok, heads_local * HEAD_DIM)
    )
    return (teacher, student)


LANES = 128
EXTRA = 16
GRANTS = tuple(mib * 1024 * 1024 for mib in (6, 12, 16, 24))
F32 = jnp.float32
BF16 = jnp.bfloat16
LAST = (((1,), (1,)), ((), ()))


def cost(flops, moved):
    return pl.CostEstimate(flops=flops, bytes_accessed=moved, transcendentals=0)


def joined(refs):
    return jnp.concatenate([ref[(0,) * (len(ref.shape) - 2)] for ref in refs], axis=1)


def project_kernel(ids, x_ref, w0, w1, w2, w3, out_ref):
    out_ref[...] = jnp.dot(
        x_ref[...], joined((w0, w1, w2, w3)), preferred_element_type=F32
    ).astype(BF16)


def add_halves(x_ref, w0, w1, w2, w3, r_ref, send_ref, keep_ref):
    tok, half = keep_ref.shape
    first = jnp.dot(x_ref[...], joined((w0, w1)), preferred_element_type=F32)
    send_ref[:tok, :] = (first + r_ref[:, :half].astype(F32)).astype(BF16)
    second = jnp.dot(x_ref[...], joined((w2, w3)), preferred_element_type=F32)
    keep_ref[...] = second + r_ref[:, half:].astype(F32)


def project_add_kernel(ids, *refs):
    add_halves(*refs)


def folded(rates):
    half = rates.shape[1] // 2
    return jnp.concatenate([rates[:, :half], rates[:, half:]], axis=0)


def unfolded(rows):
    half = rows.shape[0] // 2
    return jnp.concatenate([rows[:half], rows[half:]], axis=1)


def project_pair_kernel(ids, raw_ref, *refs):
    add_halves(*refs)
    send_ref, tok = refs[-2], refs[-1].shape[0]
    away = EXTRA // 2
    rates = jnp.where(ids[0] == 0, raw_ref[away:, :], raw_ref[:away, :])
    send_ref[tok:, :] = folded(rates).astype(BF16)


def own_rates(ids, raw_ref, u_ref):
    tok = raw_ref.shape[1]
    own = EXTRA // 2
    rates = jnp.where(ids[0] == 0, raw_ref[:own, :], raw_ref[own:, :])
    return rates + unfolded(u_ref[tok:, :].astype(F32))


def pair_middle_kernel(ids, raw_ref, keep_ref, u_ref, send_ref):
    tok = keep_ref.shape[0]
    send_ref[:tok, :] = (keep_ref[...] + u_ref[:tok, :].astype(F32)).astype(BF16)
    send_ref[tok:, :] = folded(own_rates(ids, raw_ref, u_ref)).astype(BF16)


def middle_kernel(ids, keep_ref, u_ref, send_ref):
    send_ref[...] = (keep_ref[...] + u_ref[...].astype(F32)).astype(BF16)


def prepare_kernel(ids, x_ref, rates_ref, raw_ref, cos_ref, sin_ref):
    raw_ref[...] = lax.dot_general(
        rates_ref[...], x_ref[...], LAST, preferred_element_type=F32
    )
    tok, wide = cos_ref.shape
    half = wide // 2
    row = lax.broadcasted_iota(jnp.int32, (tok, wide), 0) + ids[2] * tok
    lane = lax.broadcasted_iota(jnp.int32, (1, wide), 1)
    slot = jnp.where(lane < half, lane, lane - half).astype(F32)
    freq = jnp.exp(slot * (-2.0 / wide * math.log(ROPE_BASE)))
    angle = row.astype(F32) * freq
    cos_ref[...] = jnp.cos(angle)
    sine = jnp.sin(angle)
    sin_ref[...] = jnp.where(lane < half, -sine, sine)


def weight_spec(weights, place):
    ndim = weights.ndim
    block = (1,) * (ndim - 2) + (weights.shape[-2], LANES)
    return pl.BlockSpec(block, lambda step, ids: place(ids[0], ids[1]))


def flat(shape):
    return pl.BlockSpec(shape, lambda step, ids, n=len(shape): (0,) * n)


def call(kernel, ids, specs, args, shapes, flops, aliases={}, out_specs=None, grant=GRANTS[1]):
    return pl.pallas_call(
        kernel,
        grid_spec=pltpu.PrefetchScalarGridSpec(
            num_scalar_prefetch=1,
            grid=(1,),
            in_specs=specs,
            out_specs=out_specs or [flat(s) for s, _ in shapes],
        ),
        out_shape=[jax.ShapeDtypeStruct(s, d) for s, d in shapes],
        input_output_aliases=aliases,
        compiler_params=pltpu.CompilerParams(vmem_limit_bytes=grant),
        cost_estimate=cost(flops, 3 * 10**6),
    )(ids, *args)


def project(ids, x, x_block, weights, places):
    tok, rows = x.shape[0], weights.shape[-2]
    wide = len(places) * LANES
    specs = [pl.BlockSpec((tok, rows), x_block)]
    specs += [weight_spec(weights, place) for place in places]
    args = [x] + [weights] * len(places)
    return call(project_kernel, ids, specs, args, [((tok, wide), BF16)], 2 * tok * rows * wide)[0]


def project_add(ids, x, x_block, weights, places, received, raw=None):
    tok, rows = x.shape[0], weights.shape[-2]
    wide = len(places) * LANES
    half = wide // 2
    specs = [pl.BlockSpec((tok, rows), x_block)]
    specs += [weight_spec(weights, place) for place in places] + [flat(received.shape)]
    args = [x] + [weights] * len(places) + [received]
    tall, kernel = tok, project_add_kernel
    if raw is not None:
        specs, args = [flat(raw.shape)] + specs, [raw] + args
        tall, kernel = tok + EXTRA, project_pair_kernel
    shapes = [((tall, half), BF16), ((tok, half), F32)]
    return call(kernel, ids, specs, args, shapes, 2 * tok * rows * wide)


def turn(vectors, cosine, sine):
    return vectors * cosine + pltpu.roll(vectors, HEAD_DIM // 2, 1) * sine


def split_sum(rows, mask):
    high = rows.astype(BF16)
    rest = rows - high.astype(F32)
    middle = rest.astype(BF16)
    low = (rest - middle.astype(F32)).astype(BF16)
    count = rows.shape[0]
    parts = jnp.concatenate([high.astype(F32), middle.astype(F32), low.astype(F32)], axis=0)
    sums = lax.dot_general(parts.astype(BF16), mask, LAST, preferred_element_type=F32)
    return sums[:count] + (sums[count : 2 * count] + sums[2 * count :])


def context_kernel(
    stretch, ids, raw_ref, keep_ref, u_ref, z_ref, cos_ref, sin_ref, bias_ref, rate_ref,
    carry_ref, bterm_ref, across_ref, down_ref, step_ref, first_ref,
):
    tok = keep_ref.shape[0]
    heads = bias_ref.shape[0]
    spans = tok // stretch
    pair = keep_ref[...] + u_ref[:tok, :].astype(F32) + z_ref[:tok, :].astype(F32)
    keys = pair[:, :HEAD_DIM]
    values = pair[:, HEAD_DIM:].astype(BF16)
    bterm = keys.astype(BF16)
    carry_ref[:tok, :HEAD_DIM] = turn(keys, cos_ref[...], sin_ref[...]).astype(BF16)
    carry_ref[:tok, HEAD_DIM:] = values
    bterm_ref[...] = bterm
    both = own_rates(ids, raw_ref, u_ref) + unfolded(z_ref[tok:, :].astype(F32))
    raw = jnp.where(ids[1] == 0, both[:heads], both[heads:])
    which = lax.broadcasted_iota(jnp.int32, (heads, 1), 0)
    bias = jnp.full((heads, 1), bias_ref[0], F32)
    rate = jnp.full((heads, 1), rate_ref[0], F32)
    for h in range(1, heads):
        bias = jnp.where(which == h, bias_ref[h], bias)
        rate = jnp.where(which == h, rate_ref[h], rate)
    step = jax.nn.softplus(raw + bias)
    decay = -rate * step
    rows = lax.broadcasted_iota(jnp.int32, (stretch, stretch), 0)
    cols = lax.broadcasted_iota(jnp.int32, (stretch, stretch), 1)
    below = (cols <= rows).astype(F32).astype(BF16)
    fold = lambda a: jnp.concatenate([a[:, i * stretch : (i + 1) * stretch] for i in range(spans)], axis=0)
    across = split_sum(fold(decay), below)
    steps = fold(step)
    tails = jnp.exp(across[:, stretch - 1 :] - across) * steps
    across_ref[...] = across
    step_ref[...] = steps
    count = heads * spans
    filler = jnp.zeros((LANES - 2 * count, stretch), F32)
    down = jnp.transpose(jnp.concatenate([across, tails, filler], axis=0))
    down_ref[...] = down
    states = [None] * heads
    for index in range(spans):
        span = slice(index * stretch, (index + 1) * stretch)
        part = bterm[span].astype(F32)
        weighted = jnp.concatenate(
            [
                (part * down[:, count + index * heads + h : count + index * heads + h + 1]).astype(BF16)
                for h in range(heads)
            ],
            axis=1,
        )
        fresh = lax.dot_general(
            weighted, values[span], (((0,), (0,)), ((), ())), preferred_element_type=F32
        )
        for h in range(heads):
            new = fresh[h * HEAD_DIM : (h + 1) * HEAD_DIM]
            if index > 0:
                at = index * heads + h
                new = new + jnp.exp(across[at : at + 1, stretch - 1 :]) * states[h]
            else:
                first_ref[h] = new
            states[h] = new
    for h in range(heads):
        row, col = tok + (h // 2) * HEAD_DIM, (h % 2) * HEAD_DIM
        carry_ref[row : row + HEAD_DIM, col : col + HEAD_DIM] = states[h].astype(BF16)


def heads_kernel(stretch, numbers, ids, *refs):
    refs = list(refs)
    pieces = refs[: 3 * len(numbers)]
    (cos_ref, sin_ref, carry_ref, bterm_ref, came_ref, across_ref, down_ref, step_ref,
     first_ref, skip_ref) = refs[3 * len(numbers) : 3 * len(numbers) + 10]
    teacher_ref, student_ref = refs[-2:]
    tok = bterm_ref.shape[0]
    heads = first_ref.shape[0]
    scale = HEAD_DIM ** (-0.5)
    power = scale * 1.4426950408889634
    later = (ids[2] > 0).astype(F32)
    blocked = (1.0 - later) * FAR_BELOW
    rows = lax.broadcasted_iota(jnp.int32, (stretch, stretch), 0)
    cols = lax.broadcasted_iota(jnp.int32, (stretch, stretch), 1)
    causal = cols <= rows
    ones = jnp.ones((tok, HEAD_DIM), BF16)
    own_keys = carry_ref[:tok, :HEAD_DIM]
    prev_keys = came_ref[:tok, :HEAD_DIM]
    own_values = jnp.concatenate([carry_ref[:tok, HEAD_DIM:], ones], axis=1)
    prev_values = jnp.concatenate([came_ref[:tok, HEAD_DIM:], ones], axis=1)
    for at, head in enumerate(numbers):
        keep_ref, u_ref, z_ref = pieces[3 * at : 3 * at + 3]
        place = slice(at * HEAD_DIM, (at + 1) * HEAD_DIM)
        query = keep_ref[...] + u_ref[...].astype(F32) + z_ref[...].astype(F32)
        turned = turn(query, cos_ref[...], sin_ref[...]).astype(BF16)
        cterm = query.astype(BF16)
        row, col = tok + (head // 2) * HEAD_DIM, (head % 2) * HEAD_DIM
        state = came_ref[row : row + HEAD_DIM, col : col + HEAD_DIM].astype(F32) * later
        skip = skip_ref[head]
        for index in range(tok // stretch):
            span = slice(index * stretch, (index + 1) * stretch)
            reach = (index + 1) * stretch
            queries = turned[span]
            far = lax.dot_general(queries, prev_keys, LAST, preferred_element_type=F32) + blocked
            near = lax.dot_general(queries, own_keys[:reach], LAST, preferred_element_type=F32)
            diagonal = jnp.where(causal, near[:, index * stretch :], FAR_BELOW)
            if index > 0:
                near = jnp.concatenate([near[:, : index * stretch], diagonal], axis=1)
            else:
                near = diagonal
            top = jnp.maximum(
                jnp.max(far, axis=1, keepdims=True), jnp.max(near, axis=1, keepdims=True)
            )
            far = jnp.exp2((far - top) * power).astype(BF16)
            near = jnp.exp2((near - top) * power).astype(BF16)
            mixed = jnp.dot(far, prev_values, preferred_element_type=F32) + jnp.dot(
                near, own_values[:reach], preferred_element_type=F32
            )
            teacher_ref[span, place] = (mixed[:, :HEAD_DIM] / mixed[:, HEAD_DIM:]).astype(BF16)
            values = carry_ref[span, HEAD_DIM:]
            which = index * heads + head
            down = down_ref[:, which : which + 1]
            across = across_ref[which : which + 1, :]
            gram = lax.dot_general(
                cterm[span], bterm_ref[span, :], LAST, preferred_element_type=F32
            ) * (step_ref[which : which + 1, :] * scale)
            mix = jnp.where(causal, jnp.exp(jnp.where(causal, down - across, -1e4)) * gram, 0.0)
            inner = jnp.dot(mix.astype(BF16), values, preferred_element_type=F32)
            high = state.astype(BF16)
            low = (state - high.astype(F32)).astype(BF16)
            carried = jnp.dot(
                cterm[span], jnp.concatenate([high, low], axis=1), preferred_element_type=F32
            )
            carried = (carried[:, :HEAD_DIM] + carried[:, HEAD_DIM:]) * (jnp.exp(down) * scale)
            student_ref[span, place] = (inner + carried + skip * values.astype(F32)).astype(BF16)
            if index == 0:
                state = jnp.exp(across[:, stretch - 1 :]) * state + first_ref[head]


def heads_call(ids, group_at, numbers, pieces, shared, total, before):
    tok = pieces[0][0].shape[0]
    column = lambda col: pl.BlockSpec((tok, LANES), lambda step, ids, col=col: (0, col))
    specs, args = [], []
    for keep, u, z in pieces:
        specs += [column(1), column(1), column(0)]
        args += [keep, u, z]
    specs += [flat(a.shape) for a in shared[:-1]] + [pl.BlockSpec(memory_space=pltpu.SMEM)]
    args += list(shared)
    aliases = {}
    if before is not None:
        aliases = {1 + len(args): 0, 2 + len(args): 1}
        specs += [pl.BlockSpec(memory_space=pl.ANY)] * 2
        args += list(before)
    wide = len(numbers) * LANES
    block = pl.BlockSpec((tok, wide), lambda step, ids: (0, group_at))
    return call(
        functools.partial(heads_kernel, STRETCH, numbers),
        ids, specs, args, [((tok, total), BF16)] * 2, 2 * 10**9, aliases, [block] * 2,
        GRANTS[3],
    )


def pair_body(*args):
    return pair_steps(*args)


def pair_steps(layer_input, attn_weight, rate_weight, rate_bias, decay_rate, skip_gain):
    tok, _ = layer_input.shape
    heads = rate_bias.shape[0]
    group = HEADS // KV_HEADS
    grp = lax.axis_index("grp")
    seq = lax.axis_index("seq")
    ids = jnp.stack([grp // 2, grp % 2, seq]).astype(jnp.int32)
    count = lax.axis_size("grp")
    swap_high = [(g, g ^ 2) for g in range(count)]
    swap_low = [(g, g ^ 1) for g in range(count)]
    over_high = lambda a: lax.ppermute(a, "grp", swap_high)
    over_low = lambda a: lax.ppermute(a, "grp", swap_low)
    over_seq = lambda a: lax.ppermute(a, "seq", [(0, 1), (1, 0)])
    own_block = lambda step, ids: (0, ids[2])

    other = over_seq(layer_input)
    weights_all = jnp.transpose(attn_weight, (1, 0, 2))
    args = [layer_input, rate_weight.T]
    shapes = [((EXTRA, tok), F32), ((tok, HEAD_DIM), F32), ((tok, HEAD_DIM), F32)]
    raw, cosine, sine = call(
        prepare_kernel, ids, [flat(a.shape) for a in args], args, shapes, 10**9
    )

    pair_places = [
        lambda h, l: (1 - h, 0, group), lambda h, l: (1 - h, 0, group + 1),
        lambda h, l: (h, 0, group), lambda h, l: (h, 0, group + 1),
    ]

    def high_places(j):
        return [
            lambda h, l: (1 - h, 0, (1 - l) * heads + j), lambda h, l: (1 - h, 0, l * heads + j),
            lambda h, l: (h, 0, (1 - l) * heads + j), lambda h, l: (h, 0, l * heads + j),
        ]

    def low_places(j):
        return [
            lambda h, l: (1 - h, 0, (1 - l) * heads + j), lambda h, l: (h, 0, (1 - l) * heads + j),
            lambda h, l: (1 - h, 0, l * heads + j), lambda h, l: (h, 0, l * heads + j),
        ]

    other, weights_all = lax.optimization_barrier((other, weights_all))
    plan = [(None, weights_all, pair_places, over_high, over_low)]
    for pair in range(heads // 2):
        plan.append((2 * pair + 1, weights_all, low_places(2 * pair + 1), over_low, over_high))
        plan.append((2 * pair, weights_all, high_places(2 * pair), over_high, over_low))
    ahead = [ids]

    def queued(make):
        ready, _ = lax.optimization_barrier((ids, ahead[0]))
        outs = make(ready)
        ahead[0] = outs[0]
        return outs

    crossed, parts, arrived, pieces, kept = {}, {}, {}, {}, {}

    def cross(at):
        _, weights, places, _, _ = plan[at]
        out = queued(lambda ready: [project(ready, other, own_block, weights, places)])[0]
        crossed[at] = over_seq(out)

    def mine(at):
        j, weights, places, first, _ = plan[at]
        send, kept[at] = queued(
            lambda ready: project_add(
                ready, layer_input, own_block, weights, places, crossed[at],
                raw if j is None else None,
            )
        )
        parts[at] = first(send)

    def middle(at):
        j, _, _, _, second = plan[at]
        keep, u = kept[at], parts[at]
        if j is None:
            args = [raw, keep, u]
            shapes = [((tok + EXTRA, 2 * HEAD_DIM), BF16)]
            send = queued(
                lambda ready: call(
                    pair_middle_kernel, ready, [flat(a.shape) for a in args], args, shapes, 10**7
                )
            )[0]
        else:
            specs = [pl.BlockSpec((tok, LANES), lambda step, ids: (0, 0))] * 2
            send = queued(
                lambda ready: call(
                    middle_kernel, ready, specs, [keep, u], [((tok, LANES), BF16)], 10**7, grant=GRANTS[0]
                )
            )[0]
        arrived[at] = second(send)
        if j is not None:
            pieces[j] = (keep, u, arrived[at])

    def context():
        args = [
            raw, kept[0], parts[0], arrived[0], cosine, sine, rate_bias, decay_rate,
        ]
        scalars = pl.BlockSpec(memory_space=pltpu.SMEM)
        specs = [flat(a.shape) for a in args[:-2]] + [scalars] * 2
        spans = tok // STRETCH
        shapes = [
            ((tok + heads // 2 * HEAD_DIM, 2 * HEAD_DIM), BF16), ((tok, HEAD_DIM), BF16),
            ((heads * spans, STRETCH), F32), ((STRETCH, LANES), F32), ((heads * spans, STRETCH), F32),
            ((heads, HEAD_DIM, HEAD_DIM), F32),
        ]
        carry, *rest = queued(
            lambda ready: call(
                functools.partial(context_kernel, STRETCH), ready,
                specs, args, shapes, 10**9, grant=GRANTS[2],
            )
        )
        came = over_seq(carry)
        bterm, across, down, step, first_state = rest
        return (
            cosine, sine, carry, bterm, came, across, down, step, first_state, skip_gain,
        )

    def tail(pair, shared, before):
        numbers = (2 * pair, 2 * pair + 1)
        return queued(
            lambda ready: heads_call(
                ready, pair, numbers, [pieces[n] for n in numbers], shared,
                heads * HEAD_DIM, before,
            )
        )

    cross(0)
    cross(1)
    mine(0)
    mine(1)
    cross(2)
    cross(3)
    mine(2)
    cross(4)
    middle(0)
    mine(3)
    mine(4)
    middle(1)
    middle(2)
    shared = context()
    middle(3)
    outs = tail(0, shared, None)
    middle(4)
    outs = tail(1, shared, outs)
    return outs[0], outs[1]


def solution(mesh):
    placed = (
        P("seq", "grp"),
        P(("grp", "seq"), "mdl", None),
        P("grp", "mdl"),
        P(("mdl", "grp")),
        P(("mdl", "grp")),
        P(("mdl", "grp")),
    )
    chips = mesh.shape["grp"] * mesh.shape["mdl"]
    paired = (
        mesh.shape["seq"] == 2
        and mesh.shape["grp"] == 4
        and KV_HEADS == 2 * mesh.shape["mdl"]
        and HEADS // chips == 4
    )
    return jax.shard_map(
        pair_body if paired else body,
        mesh=mesh,
        in_specs=placed,
        out_specs=(P("seq", ("mdl", "grp")), P("seq", ("mdl", "grp"))),
        check_vma=False,
    )
```

```python
import functools
import math

import jax
import jax.numpy as jnp
from jax import lax
from jax.experimental import pallas as pl
from jax.experimental.pallas import tpu as pltpu
from jax.sharding import PartitionSpec as P


HEADS = 64
KV_HEADS = 8
HEAD_DIM = 128
STRETCH = 256


ROPE_BASE = 500000.0
FAR_BELOW = -1e30


def rope_angles(positions):
    half = HEAD_DIM // 2
    freq = ROPE_BASE ** (-2.0 * jnp.arange(half, dtype=jnp.float32) / HEAD_DIM)
    angle = positions.astype(jnp.float32)[:, None] * freq[None, :]
    return (jnp.cos(angle), jnp.sin(angle))


def rotate(vectors, cosine, sine):
    half = vectors.shape[-1] // 2
    first = vectors[..., :half]
    second = vectors[..., half:]
    cosine = cosine[:, None, :]
    sine = sine[:, None, :]
    return jnp.concatenate(
        [first * cosine - second * sine, second * cosine + first * sine], axis=-1
    )


def state_product(cterm, state):
    high = state.astype(jnp.bfloat16)
    low = (state - high.astype(jnp.float32)).astype(jnp.bfloat16)
    upper = jnp.einsum("thn,hnp->thp", cterm, high, preferred_element_type=jnp.float32)
    return upper + jnp.einsum("thn,hnp->thp", cterm, low, preferred_element_type=jnp.float32)


def key_absorber(queries, own_first, scale, carry, piece):
    top, total, accum = carry
    keys, values = piece
    scores = jnp.einsum("thd,nd->thn", queries, keys, preferred_element_type=jnp.float32) * scale
    query_pos = own_first + jnp.arange(queries.shape[0], dtype=jnp.int32)
    key_pos = jnp.arange(keys.shape[0], dtype=jnp.int32)
    causal = (key_pos[None, :] <= query_pos[:, None])[:, None, :]
    masked = jnp.where(causal, scores, FAR_BELOW)
    new_top = jnp.maximum(top, jnp.max(masked, axis=2))
    weights = jnp.where(causal, jnp.exp(masked - new_top[:, :, None]), 0.0)
    total = jnp.sum(weights, axis=2)
    accum = jnp.einsum(
        "thn,nd->thd", weights.astype(jnp.bfloat16), values, preferred_element_type=jnp.float32
    )
    return (new_top, total, accum)


def body(layer_input, attn_weight, rate_weight, rate_bias, decay_rate, skip_gain):
    tok = layer_input.shape[0]
    kv_local = attn_weight.shape[1]
    heads_local = rate_bias.shape[0]
    group = HEADS // KV_HEADS
    scale = HEAD_DIM ** (-0.5)
    merged = jnp.einsum(
        "td,dkc->tkc",
        layer_input,
        lax.all_gather(attn_weight, "seq", axis=0, tiled=True),
        preferred_element_type=jnp.float32,
    )
    rate_part = jnp.dot(layer_input, rate_weight, preferred_element_type=jnp.float32)
    grp_index = lax.axis_index("grp")
    summed, rate_whole = (
        lax.psum(merged.astype(jnp.bfloat16), "grp").astype(jnp.float32),
        lax.psum(rate_part.astype(jnp.bfloat16), "grp").astype(jnp.float32),
    )
    query_whole = summed[:, :, : group * HEAD_DIM].reshape(tok, kv_local * group * HEAD_DIM)
    query_flat = lax.dynamic_slice_in_dim(
        query_whole, grp_index * heads_local * HEAD_DIM, heads_local * HEAD_DIM, 1
    )
    raw = lax.dynamic_slice_in_dim(rate_whole, grp_index * heads_local, heads_local, 1)
    pairs = summed[:, :, group * HEAD_DIM :]
    kv_index = grp_index * heads_local // group
    pair = lax.dynamic_index_in_dim(pairs, kv_index, 1, keepdims=False)
    keys = pair[:, :HEAD_DIM]
    values = pair[:, HEAD_DIM:].astype(jnp.bfloat16)
    query = query_flat.reshape(tok, heads_local, HEAD_DIM)
    own_first = lax.axis_index("seq") * tok
    cosine, sine = rope_angles(own_first + jnp.arange(tok, dtype=jnp.int32))
    rot_query = rotate(query, cosine, sine).astype(jnp.bfloat16)
    rot_keys = rotate(keys[:, None, :], cosine, sine)[:, 0].astype(jnp.bfloat16)
    start_carry = (
        jnp.full((tok, heads_local), FAR_BELOW, jnp.float32),
        jnp.zeros((tok, heads_local), jnp.float32),
        jnp.zeros((tok, heads_local, HEAD_DIM), jnp.float32),
    )
    _, total, accum = key_absorber(
        rot_query,
        own_first,
        scale,
        start_carry,
        (
            lax.all_gather(rot_keys, "seq", axis=0, tiled=True),
            lax.all_gather(values, "seq", axis=0, tiled=True),
        ),
    )
    teacher = (accum / total[:, :, None]).astype(jnp.bfloat16).reshape(tok, heads_local * HEAD_DIM)
    step = jax.nn.softplus(raw + rate_bias[None, :])
    log_decay = -decay_rate[None, :] * step
    c_all = query.astype(jnp.bfloat16)
    b_all = keys.astype(jnp.bfloat16)
    causal = (
        jnp.arange(STRETCH, dtype=jnp.int32)[:, None]
        >= jnp.arange(STRETCH, dtype=jnp.int32)[None, :]
    )[None]
    state = jnp.zeros((heads_local, HEAD_DIM, HEAD_DIM), jnp.float32)
    before = jnp.zeros((heads_local,), jnp.float32)
    partials = []
    offsets = []
    for index in range(tok // STRETCH):
        first = index * STRETCH
        cpart = c_all[first : first + STRETCH]
        bpart = b_all[first : first + STRETCH]
        xpart = values[first : first + STRETCH]
        decay = log_decay[first : first + STRETCH]
        rate = step[first : first + STRETCH]
        cum = jnp.cumsum(decay, axis=0)
        gram = jnp.einsum("thn,sn->hts", cpart, bpart, preferred_element_type=jnp.float32) * scale
        diff = cum.T[:, :, None] - cum.T[:, None, :]
        mix = jnp.where(
            causal, jnp.exp(jnp.where(causal, diff, -10000.0)) * rate.T[:, None, :] * gram, 0.0
        ).astype(jnp.bfloat16)
        intra = jnp.einsum("hts,sp->thp", mix, xpart, preferred_element_type=jnp.float32)
        carried = state_product(cpart, state) * scale * jnp.exp(cum)[:, :, None]
        weighted = (
            (jnp.exp(cum[-1][None, :] - cum) * rate)[:, :, None]
            * bpart.astype(jnp.float32)[:, None, :]
        ).astype(jnp.bfloat16)
        contribution = jnp.einsum(
            "shn,sp->hnp", weighted, xpart, preferred_element_type=jnp.float32
        )
        state = jnp.exp(cum[-1])[:, None, None] * state + contribution
        partials.append(intra + carried)
        offsets.append(cum + before[None, :])
        before = before + cum[-1]
    totals, states = (
        lax.all_gather(before[None, :].astype(jnp.bfloat16), "seq", axis=0, tiled=True).astype(
            jnp.float32
        ),
        lax.all_gather(state[None].astype(jnp.bfloat16), "seq", axis=0, tiled=True).astype(
            jnp.float32
        ),
    )
    position = lax.axis_index("seq")
    order = jnp.arange(totals.shape[0], dtype=jnp.int32)
    between = ((order[:, None] < order[None, :]) & (order[None, :] < position)).astype(jnp.float32)
    span = jnp.dot(between, totals, precision=lax.Precision.HIGHEST)
    reach_back = jnp.where(order[:, None] < position, jnp.exp(span), 0.0)
    incoming = jnp.einsum("dh,dhnp->hnp", reach_back, states, precision=lax.Precision.HIGHEST)
    inside = jnp.concatenate(partials, axis=0)
    reach = jnp.exp(jnp.concatenate(offsets, axis=0))
    arriving = state_product(c_all, incoming) * scale * reach[:, :, None]
    skipped = skip_gain[None, :, None] * values.astype(jnp.float32)[:, None, :]
    student = (
        (inside + arriving + skipped).astype(jnp.bfloat16).reshape(tok, heads_local * HEAD_DIM)
    )
    return (teacher, student)


LANES = 128
EXTRA = 16
GRANTS = tuple(mib * 1024 * 1024 for mib in (6, 12, 16, 24))
F32 = jnp.float32
BF16 = jnp.bfloat16
LAST = (((1,), (1,)), ((), ()))


def cost(flops, moved):
    return pl.CostEstimate(flops=flops, bytes_accessed=moved, transcendentals=0)


def place_of():
    grp = lax.axis_index("grp")
    return grp // 2, grp % 2, lax.axis_index("seq")


def gathered(w_ref, blocks):
    return jnp.concatenate(
        [w_ref[kv, :, pl.ds(pl.multiple_of(col * LANES, LANES), LANES)] for kv, col in blocks], axis=1
    )


def own_columns(x_ref, rows):
    first = pl.multiple_of(lax.axis_index("seq") * rows, LANES)
    return x_ref[:, pl.ds(first, rows)]


def project_kernel(places, order, x_ref, w_ref, out_ref):
    high, low, _ = place_of()
    weights = gathered(w_ref, places(high, low))
    out_ref[...] = jnp.dot(
        own_columns(x_ref, w_ref.shape[1]), weights, preferred_element_type=F32
    ).astype(BF16)


def project_add_kernel(places, order, x_ref, w_ref, r_ref, send_ref, keep_ref):
    high, low, _ = place_of()
    blocks = places(high, low)
    tok, half = keep_ref.shape
    tokens = own_columns(x_ref, w_ref.shape[1])
    first = jnp.dot(tokens, gathered(w_ref, blocks[:2]), preferred_element_type=F32)
    send_ref[:tok, :] = (first + r_ref[:, :half].astype(F32)).astype(BF16)
    second = jnp.dot(tokens, gathered(w_ref, blocks[2:]), preferred_element_type=F32)
    keep_ref[...] = second + r_ref[:, half:].astype(F32)


def folded(rates):
    half = rates.shape[1] // 2
    return jnp.concatenate([rates[:, :half], rates[:, half:]], axis=0)


def unfolded(rows):
    half = rows.shape[0] // 2
    return jnp.concatenate([rows[:half], rows[half:]], axis=1)


def project_pair_kernel(places, order, raw_ref, *refs):
    project_add_kernel(places, order, *refs)
    send_ref, tok = refs[-2], refs[-1].shape[0]
    away = EXTRA // 2
    rates = jnp.where(place_of()[0] == 0, raw_ref[away:, :], raw_ref[:away, :])
    send_ref[tok:, :] = folded(rates).astype(BF16)


def own_rates(raw_ref, u_ref):
    tok = raw_ref.shape[1]
    own = EXTRA // 2
    rates = jnp.where(place_of()[0] == 0, raw_ref[:own, :], raw_ref[own:, :])
    return rates + unfolded(u_ref[tok:, :].astype(F32))


def pair_middle_kernel(order, raw_ref, keep_ref, u_ref, send_ref):
    tok = keep_ref.shape[0]
    send_ref[:tok, :] = (keep_ref[...] + u_ref[:tok, :].astype(F32)).astype(BF16)
    send_ref[tok:, :] = folded(own_rates(raw_ref, u_ref)).astype(BF16)


def middle_kernel(order, keep_ref, u_ref, send_ref):
    send_ref[...] = (keep_ref[:, :LANES] + u_ref[:, :LANES].astype(F32)).astype(BF16)


def prepare_kernel(order, x_ref, rates_ref, raw_ref, cos_ref, sin_ref):
    raw_ref[...] = lax.dot_general(
        rates_ref[...], x_ref[...], LAST, preferred_element_type=F32
    )
    tok, wide = cos_ref.shape
    half = wide // 2
    fine = EXTRA
    lane = lax.broadcasted_iota(jnp.int32, (1, wide), 1)
    slot = jnp.where(lane < half, lane, lane - half).astype(F32)
    freq = jnp.exp(slot * (-2.0 / wide * math.log(ROPE_BASE)))
    start = lax.axis_index("seq") * tok
    coarse = lax.broadcasted_iota(jnp.int32, (tok // fine, wide), 0) * fine + start
    coarse = coarse.astype(F32) * freq
    small = lax.broadcasted_iota(jnp.int32, (fine, wide), 0).astype(F32) * freq
    cos_big, sin_big = jnp.cos(coarse), jnp.sin(coarse)
    cos_small, sin_small = jnp.cos(small), jnp.sin(small)
    sign = jnp.where(lane < half, -1.0, 1.0)
    for at in range(tok // fine):
        c, d = cos_big[at : at + 1, :], sin_big[at : at + 1, :]
        span = slice(at * fine, (at + 1) * fine)
        cos_ref[span, :] = c * cos_small - d * sin_small
        sin_ref[span, :] = (d * cos_small + c * sin_small) * sign


VMEM = pl.BlockSpec(memory_space=pltpu.VMEM)
SMEM = pl.BlockSpec(memory_space=pltpu.SMEM)
ANY = pl.BlockSpec(memory_space=pl.ANY)


def call(kernel, order, args, shapes, flops, in_specs=None, **rest):
    return pl.pallas_call(
        kernel,
        in_specs=[ANY] + (in_specs or [VMEM] * len(args)),
        out_specs=rest.pop("out_specs", [VMEM] * len(shapes)),
        out_shape=[jax.ShapeDtypeStruct(s, d) for s, d in shapes],
        compiler_params=pltpu.CompilerParams(vmem_limit_bytes=rest.pop("grant", GRANTS[1])),
        cost_estimate=cost(flops, 3 * 10**6),
        **rest,
    )(order, *args)


def project(order, x, weights, places):
    tok, rows = x.shape[0], weights.shape[1]
    wide = 4 * LANES
    return call(
        functools.partial(project_kernel, places), order, [x, weights],
        [((tok, wide), BF16)], 2 * tok * rows * wide,
    )


def project_add(order, x, weights, places, received, raw):
    tok, rows = x.shape[0], weights.shape[1]
    wide = 4 * LANES
    args, tall, kernel = [x, weights, received], tok, project_add_kernel
    if raw is not None:
        args, tall, kernel = [raw] + args, tok + EXTRA, project_pair_kernel
    shapes = [((tall, wide // 2), BF16), ((tok, wide // 2), F32)]
    return call(functools.partial(kernel, places), order, args, shapes, 2 * tok * rows * wide)


def turn(vectors, cosine, sine):
    return vectors * cosine + pltpu.roll(vectors, HEAD_DIM // 2, 1) * sine


def split_sum(rows, mask):
    high = rows.astype(BF16)
    rest = rows - high.astype(F32)
    middle = rest.astype(BF16)
    low = (rest - middle.astype(F32)).astype(BF16)
    count = rows.shape[0]
    parts = jnp.concatenate([high.astype(F32), middle.astype(F32), low.astype(F32)], axis=0)
    sums = lax.dot_general(parts.astype(BF16), mask, LAST, preferred_element_type=F32)
    return sums[:count] + (sums[count : 2 * count] + sums[2 * count :])


def context_kernel(
    stretch, order, raw_ref, keep_ref, u_ref, z_ref, cos_ref, sin_ref, bias_ref, rate_ref,
    carry_ref, bterm_ref, across_ref, down_ref, step_ref, first_ref,
):
    tok = keep_ref.shape[0]
    heads = bias_ref.shape[0]
    spans = tok // stretch
    pair = keep_ref[...] + u_ref[:tok, :].astype(F32) + z_ref[:tok, :].astype(F32)
    keys = pair[:, :HEAD_DIM]
    values = pair[:, HEAD_DIM:].astype(BF16)
    bterm = keys.astype(BF16)
    carry_ref[:tok, :HEAD_DIM] = turn(keys, cos_ref[...], sin_ref[...]).astype(BF16)
    carry_ref[:tok, HEAD_DIM:] = values
    bterm_ref[...] = bterm
    both = own_rates(raw_ref, u_ref) + unfolded(z_ref[tok:, :].astype(F32))
    raw = jnp.where(place_of()[1] == 0, both[:heads], both[heads:])
    which = lax.broadcasted_iota(jnp.int32, (heads, 1), 0)
    bias = jnp.full((heads, 1), bias_ref[0], F32)
    rate = jnp.full((heads, 1), rate_ref[0], F32)
    for h in range(1, heads):
        bias = jnp.where(which == h, bias_ref[h], bias)
        rate = jnp.where(which == h, rate_ref[h], rate)
    step = jax.nn.softplus(raw + bias)
    decay = -rate * step
    rows = lax.broadcasted_iota(jnp.int32, (stretch, stretch), 0)
    cols = lax.broadcasted_iota(jnp.int32, (stretch, stretch), 1)
    below = (cols <= rows).astype(F32).astype(BF16)
    fold = lambda a: jnp.concatenate([a[:, i * stretch : (i + 1) * stretch] for i in range(spans)], axis=0)
    across = split_sum(fold(decay), below)
    steps = fold(step)
    tails = jnp.exp(across[:, stretch - 1 :] - across) * steps
    across_ref[...] = across
    step_ref[...] = steps
    count = heads * spans
    filler = jnp.zeros((LANES - 2 * count, stretch), F32)
    down = jnp.transpose(jnp.concatenate([across, tails, filler], axis=0))
    down_ref[...] = down
    states = [None] * heads
    for index in range(spans):
        span = slice(index * stretch, (index + 1) * stretch)
        part = bterm[span].astype(F32)
        weighted = jnp.concatenate(
            [
                (part * down[:, count + index * heads + h : count + index * heads + h + 1]).astype(BF16)
                for h in range(heads)
            ],
            axis=1,
        )
        fresh = lax.dot_general(
            weighted, values[span], (((0,), (0,)), ((), ())), preferred_element_type=F32
        )
        for h in range(heads):
            new = fresh[h * HEAD_DIM : (h + 1) * HEAD_DIM]
            if index > 0:
                at = index * heads + h
                new = new + jnp.exp(across[at : at + 1, stretch - 1 :]) * states[h]
            else:
                first_ref[h] = new
            states[h] = new
    for h in range(heads):
        row, col = tok + (h // 2) * HEAD_DIM, (h % 2) * HEAD_DIM
        carry_ref[row : row + HEAD_DIM, col : col + HEAD_DIM] = states[h].astype(BF16)


def head_kernel(
    stretch, head, order, keep_ref, u_ref, z_ref, cos_ref, sin_ref, carry_ref, bterm_ref, came_ref,
    across_ref, down_ref, step_ref, first_ref, skip_ref, *rest,
):
    teacher_out, student_out, teacher_ref, student_ref, sems = rest[-5:]
    tok = bterm_ref.shape[0]
    heads = first_ref.shape[0]
    scale = HEAD_DIM ** (-0.5)
    power = scale * 1.4426950408889634
    later = (lax.axis_index("seq") > 0).astype(F32)
    blocked = (1.0 - later) * FAR_BELOW
    rows = lax.broadcasted_iota(jnp.int32, (stretch, stretch), 0)
    cols = lax.broadcasted_iota(jnp.int32, (stretch, stretch), 1)
    causal = cols <= rows
    ones = jnp.ones((tok, HEAD_DIM), BF16)
    own_keys = carry_ref[:tok, :HEAD_DIM]
    prev_keys = came_ref[:tok, :HEAD_DIM]
    own_values = jnp.concatenate([carry_ref[:tok, HEAD_DIM:], ones], axis=1)
    prev_values = jnp.concatenate([came_ref[:tok, HEAD_DIM:], ones], axis=1)
    query = keep_ref[:, LANES:] + u_ref[:, LANES:].astype(F32) + z_ref[...].astype(F32)
    turned = turn(query, cos_ref[...], sin_ref[...]).astype(BF16)
    cterm = query.astype(BF16)
    row, col = tok + (head // 2) * HEAD_DIM, (head % 2) * HEAD_DIM
    state = came_ref[row : row + HEAD_DIM, col : col + HEAD_DIM].astype(F32) * later
    place = slice(head * HEAD_DIM, (head + 1) * HEAD_DIM)
    copies = []
    skip = skip_ref[head]
    for index in range(tok // stretch):
        span = slice(index * stretch, (index + 1) * stretch)
        reach = (index + 1) * stretch
        queries = turned[span]
        far = lax.dot_general(queries, prev_keys, LAST, preferred_element_type=F32) + blocked
        near = lax.dot_general(queries, own_keys[:reach], LAST, preferred_element_type=F32)
        diagonal = jnp.where(causal, near[:, index * stretch :], FAR_BELOW)
        if index > 0:
            near = jnp.concatenate([near[:, : index * stretch], diagonal], axis=1)
        else:
            near = diagonal
        top = jnp.maximum(
            jnp.max(far, axis=1, keepdims=True), jnp.max(near, axis=1, keepdims=True)
        )
        far = jnp.exp2((far - top) * power).astype(BF16)
        near = jnp.exp2((near - top) * power).astype(BF16)
        mixed = jnp.dot(far, prev_values, preferred_element_type=F32) + jnp.dot(
            near, own_values[:reach], preferred_element_type=F32
        )
        teacher_ref[span, :] = (mixed[:, :HEAD_DIM] / mixed[:, HEAD_DIM:]).astype(BF16)
        values = carry_ref[span, HEAD_DIM:]
        which = index * heads + head
        down = down_ref[:, which : which + 1]
        across = across_ref[which : which + 1, :]
        gram = lax.dot_general(
            cterm[span], bterm_ref[span, :], LAST, preferred_element_type=F32
        ) * (step_ref[which : which + 1, :] * scale)
        mix = jnp.where(causal, jnp.exp(jnp.where(causal, down - across, -1e4)) * gram, 0.0)
        inner = jnp.dot(mix.astype(BF16), values, preferred_element_type=F32)
        high = state.astype(BF16)
        low = (state - high.astype(F32)).astype(BF16)
        carried = jnp.dot(
            cterm[span], jnp.concatenate([high, low], axis=1), preferred_element_type=F32
        )
        carried = (carried[:, :HEAD_DIM] + carried[:, HEAD_DIM:]) * (jnp.exp(down) * scale)
        student_ref[span, :] = (inner + carried + skip * values.astype(F32)).astype(BF16)
        if index == 0:
            state = jnp.exp(across[:, stretch - 1 :]) * state + first_ref[head]
        for kind, (held, out) in enumerate(((teacher_ref, teacher_out), (student_ref, student_out))):
            copy = pltpu.make_async_copy(held.at[span, :], out.at[span, place], sems.at[kind, index])
            copy.start()
            copies.append(copy)
    for copy in copies:
        copy.wait()


def head_call(order, head, piece, shared, total, before):
    tok = piece[0].shape[0]
    args = list(piece) + list(shared)
    specs = [VMEM] * (len(args) - 1) + [SMEM]
    aliases = {}
    if before is not None:
        aliases = {1 + len(args): 0, 2 + len(args): 1}
        args, specs = args + list(before), specs + [ANY] * 2
    held = pltpu.VMEM((tok, HEAD_DIM), BF16)
    return call(
        functools.partial(head_kernel, STRETCH, head), order, args, [((tok, total), BF16)] * 2, 10**9,
        specs, out_specs=[ANY] * 2, input_output_aliases=aliases, grant=GRANTS[3],
        scratch_shapes=[held, held, pltpu.SemaphoreType.DMA((2, tok // STRETCH))],
    )


def pair_body(*args):
    return pair_steps(*args)


def pair_steps(layer_input, attn_weight, rate_weight, rate_bias, decay_rate, skip_gain):
    tok, _ = layer_input.shape
    heads = rate_bias.shape[0]
    group = HEADS // KV_HEADS
    ids = skip_gain[:1]
    count = lax.axis_size("grp")
    swap_high = [(g, g ^ 2) for g in range(count)]
    swap_low = [(g, g ^ 1) for g in range(count)]
    over_high = lambda a: lax.ppermute(a, "grp", swap_high)
    over_low = lambda a: lax.ppermute(a, "grp", swap_low)
    over_seq = lambda a: lax.ppermute(a, "seq", [(0, 1), (1, 0)])

    other = over_seq(layer_input)
    weights_all = jnp.transpose(attn_weight, (1, 0, 2))
    shapes = [((EXTRA, tok), F32), ((tok, HEAD_DIM), F32), ((tok, HEAD_DIM), F32)]

    def pair_places(h, l):
        return [(1 - h, group), (1 - h, group + 1), (h, group), (h, group + 1)]

    def high_places(j):
        return lambda h, l: [
            (1 - h, (1 - l) * heads + j), (1 - h, l * heads + j),
            (h, (1 - l) * heads + j), (h, l * heads + j),
        ]

    def low_places(j):
        return lambda h, l: [
            (1 - h, (1 - l) * heads + j), (h, (1 - l) * heads + j),
            (1 - h, l * heads + j), (h, l * heads + j),
        ]

    other, weights_all = lax.optimization_barrier((other, weights_all))
    plan = [(None, weights_all, pair_places, over_high, over_low)]
    for pair in range(heads // 2):
        plan.append((2 * pair + 1, weights_all, low_places(2 * pair + 1), over_low, over_high))
        plan.append((2 * pair, weights_all, high_places(2 * pair), over_high, over_low))
    ahead = [ids]

    def queued(make):
        ready, _ = lax.optimization_barrier((ids, ahead[0]))
        outs = make(ready)
        ahead[0] = outs[0]
        return outs

    crossed, parts, arrived, pieces, kept = {}, {}, {}, {}, {}

    def cross(at):
        _, weights, places, _, _ = plan[at]
        out = queued(lambda ready: project(ready, other, weights, places))[0]
        crossed[at] = over_seq(out)

    def mine(at):
        j, weights, places, first, _ = plan[at]
        send, kept[at] = queued(
            lambda ready: project_add(
                ready, layer_input, weights, places, crossed[at],
                raw if j is None else None,
            )
        )
        parts[at] = first(send)

    def middle(at):
        j, _, _, _, second = plan[at]
        keep, u = kept[at], parts[at]
        if j is None:
            shapes = [((tok + EXTRA, 2 * HEAD_DIM), BF16)]
            send = queued(lambda ready: call(pair_middle_kernel, ready, [raw, keep, u], shapes, 10**7))[0]
        else:
            shapes = [((tok, LANES), BF16)]
            send = queued(lambda ready: call(middle_kernel, ready, [keep, u], shapes, 10**7))[0]
        arrived[at] = second(send)
        if j is not None:
            pieces[j] = (keep, u, arrived[at])

    def context():
        args = [
            raw, kept[0], parts[0], arrived[0], cosine, sine, rate_bias, decay_rate,
        ]
        specs = [VMEM] * (len(args) - 2) + [SMEM] * 2
        spans = tok // STRETCH
        shapes = [
            ((tok + heads // 2 * HEAD_DIM, 2 * HEAD_DIM), BF16), ((tok, HEAD_DIM), BF16),
            ((heads * spans, STRETCH), F32), ((STRETCH, LANES), F32), ((heads * spans, STRETCH), F32),
            ((heads, HEAD_DIM, HEAD_DIM), F32),
        ]
        carry, *rest = queued(
            lambda ready: call(
                functools.partial(context_kernel, STRETCH), ready, args, shapes, 10**9, specs,
                grant=GRANTS[2],
            )
        )
        came = over_seq(carry)
        bterm, across, down, step, first_state = rest
        return (
            cosine, sine, carry, bterm, came, across, down, step, first_state, skip_gain,
        )

    def tail(j, shared, before):
        return queued(
            lambda ready: head_call(ready, j, pieces[j], shared, heads * HEAD_DIM, before)
        )

    def prepare():
        return queued(
            lambda ready: call(prepare_kernel, ready, [layer_input, rate_weight.T], shapes, 10**9)
        )

    cross(0)
    cross(1)
    raw, cosine, sine = prepare()
    mine(0)
    mine(1)
    cross(2)
    cross(3)
    mine(2)
    cross(4)
    middle(0)
    mine(3)
    mine(4)
    middle(1)
    middle(2)
    shared = context()
    outs = tail(1, shared, None)
    middle(3)
    outs = tail(0, shared, outs)
    middle(4)
    outs = tail(3, shared, outs)
    outs = tail(2, shared, outs)
    return outs[0], outs[1]


def solution(mesh):
    placed = (
        P("seq", "grp"),
        P(("grp", "seq"), "mdl", None),
        P("grp", "mdl"),
        P(("mdl", "grp")),
        P(("mdl", "grp")),
        P(("mdl", "grp")),
    )
    chips = mesh.shape["grp"] * mesh.shape["mdl"]
    paired = (
        mesh.shape["seq"] == 2
        and mesh.shape["grp"] == 4
        and KV_HEADS == 2 * mesh.shape["mdl"]
        and HEADS // chips == 4
    )
    return jax.shard_map(
        pair_body if paired else body,
        mesh=mesh,
        in_specs=placed,
        out_specs=(P("seq", ("mdl", "grp")), P("seq", ("mdl", "grp"))),
        check_vma=False,
    )
```

```python
import functools
import math

import jax
import jax.numpy as jnp
from jax import lax
from jax.experimental import pallas as pl
from jax.experimental.pallas import tpu as pltpu
from jax.sharding import PartitionSpec as P


HEADS = 64
KV_HEADS = 8
HEAD_DIM = 128
STRETCH = 256


ROPE_BASE = 500000.0
FAR_BELOW = -1e30


def rope_angles(positions):
    half = HEAD_DIM // 2
    freq = ROPE_BASE ** (-2.0 * jnp.arange(half, dtype=jnp.float32) / HEAD_DIM)
    angle = positions.astype(jnp.float32)[:, None] * freq[None, :]
    return (jnp.cos(angle), jnp.sin(angle))


def rotate(vectors, cosine, sine):
    half = vectors.shape[-1] // 2
    first = vectors[..., :half]
    second = vectors[..., half:]
    cosine = cosine[:, None, :]
    sine = sine[:, None, :]
    return jnp.concatenate(
        [first * cosine - second * sine, second * cosine + first * sine], axis=-1
    )


def state_product(cterm, state):
    high = state.astype(jnp.bfloat16)
    low = (state - high.astype(jnp.float32)).astype(jnp.bfloat16)
    upper = jnp.einsum("thn,hnp->thp", cterm, high, preferred_element_type=jnp.float32)
    return upper + jnp.einsum("thn,hnp->thp", cterm, low, preferred_element_type=jnp.float32)


def key_absorber(queries, own_first, scale, carry, piece):
    top, total, accum = carry
    keys, values = piece
    scores = jnp.einsum("thd,nd->thn", queries, keys, preferred_element_type=jnp.float32) * scale
    query_pos = own_first + jnp.arange(queries.shape[0], dtype=jnp.int32)
    key_pos = jnp.arange(keys.shape[0], dtype=jnp.int32)
    causal = (key_pos[None, :] <= query_pos[:, None])[:, None, :]
    masked = jnp.where(causal, scores, FAR_BELOW)
    new_top = jnp.maximum(top, jnp.max(masked, axis=2))
    weights = jnp.where(causal, jnp.exp(masked - new_top[:, :, None]), 0.0)
    total = jnp.sum(weights, axis=2)
    accum = jnp.einsum(
        "thn,nd->thd", weights.astype(jnp.bfloat16), values, preferred_element_type=jnp.float32
    )
    return (new_top, total, accum)


def body(layer_input, attn_weight, rate_weight, rate_bias, decay_rate, skip_gain):
    tok = layer_input.shape[0]
    kv_local = attn_weight.shape[1]
    heads_local = rate_bias.shape[0]
    group = HEADS // KV_HEADS
    scale = HEAD_DIM ** (-0.5)
    merged = jnp.einsum(
        "td,dkc->tkc",
        layer_input,
        lax.all_gather(attn_weight, "seq", axis=0, tiled=True),
        preferred_element_type=jnp.float32,
    )
    rate_part = jnp.dot(layer_input, rate_weight, preferred_element_type=jnp.float32)
    grp_index = lax.axis_index("grp")
    summed, rate_whole = (
        lax.psum(merged.astype(jnp.bfloat16), "grp").astype(jnp.float32),
        lax.psum(rate_part.astype(jnp.bfloat16), "grp").astype(jnp.float32),
    )
    query_whole = summed[:, :, : group * HEAD_DIM].reshape(tok, kv_local * group * HEAD_DIM)
    query_flat = lax.dynamic_slice_in_dim(
        query_whole, grp_index * heads_local * HEAD_DIM, heads_local * HEAD_DIM, 1
    )
    raw = lax.dynamic_slice_in_dim(rate_whole, grp_index * heads_local, heads_local, 1)
    pairs = summed[:, :, group * HEAD_DIM :]
    kv_index = grp_index * heads_local // group
    pair = lax.dynamic_index_in_dim(pairs, kv_index, 1, keepdims=False)
    keys = pair[:, :HEAD_DIM]
    values = pair[:, HEAD_DIM:].astype(jnp.bfloat16)
    query = query_flat.reshape(tok, heads_local, HEAD_DIM)
    own_first = lax.axis_index("seq") * tok
    cosine, sine = rope_angles(own_first + jnp.arange(tok, dtype=jnp.int32))
    rot_query = rotate(query, cosine, sine).astype(jnp.bfloat16)
    rot_keys = rotate(keys[:, None, :], cosine, sine)[:, 0].astype(jnp.bfloat16)
    start_carry = (
        jnp.full((tok, heads_local), FAR_BELOW, jnp.float32),
        jnp.zeros((tok, heads_local), jnp.float32),
        jnp.zeros((tok, heads_local, HEAD_DIM), jnp.float32),
    )
    _, total, accum = key_absorber(
        rot_query,
        own_first,
        scale,
        start_carry,
        (
            lax.all_gather(rot_keys, "seq", axis=0, tiled=True),
            lax.all_gather(values, "seq", axis=0, tiled=True),
        ),
    )
    teacher = (accum / total[:, :, None]).astype(jnp.bfloat16).reshape(tok, heads_local * HEAD_DIM)
    step = jax.nn.softplus(raw + rate_bias[None, :])
    log_decay = -decay_rate[None, :] * step
    c_all = query.astype(jnp.bfloat16)
    b_all = keys.astype(jnp.bfloat16)
    causal = (
        jnp.arange(STRETCH, dtype=jnp.int32)[:, None]
        >= jnp.arange(STRETCH, dtype=jnp.int32)[None, :]
    )[None]
    state = jnp.zeros((heads_local, HEAD_DIM, HEAD_DIM), jnp.float32)
    before = jnp.zeros((heads_local,), jnp.float32)
    partials = []
    offsets = []
    for index in range(tok // STRETCH):
        first = index * STRETCH
        cpart = c_all[first : first + STRETCH]
        bpart = b_all[first : first + STRETCH]
        xpart = values[first : first + STRETCH]
        decay = log_decay[first : first + STRETCH]
        rate = step[first : first + STRETCH]
        cum = jnp.cumsum(decay, axis=0)
        gram = jnp.einsum("thn,sn->hts", cpart, bpart, preferred_element_type=jnp.float32) * scale
        diff = cum.T[:, :, None] - cum.T[:, None, :]
        mix = jnp.where(
            causal, jnp.exp(jnp.where(causal, diff, -10000.0)) * rate.T[:, None, :] * gram, 0.0
        ).astype(jnp.bfloat16)
        intra = jnp.einsum("hts,sp->thp", mix, xpart, preferred_element_type=jnp.float32)
        carried = state_product(cpart, state) * scale * jnp.exp(cum)[:, :, None]
        weighted = (
            (jnp.exp(cum[-1][None, :] - cum) * rate)[:, :, None]
            * bpart.astype(jnp.float32)[:, None, :]
        ).astype(jnp.bfloat16)
        contribution = jnp.einsum(
            "shn,sp->hnp", weighted, xpart, preferred_element_type=jnp.float32
        )
        state = jnp.exp(cum[-1])[:, None, None] * state + contribution
        partials.append(intra + carried)
        offsets.append(cum + before[None, :])
        before = before + cum[-1]
    totals, states = (
        lax.all_gather(before[None, :].astype(jnp.bfloat16), "seq", axis=0, tiled=True).astype(
            jnp.float32
        ),
        lax.all_gather(state[None].astype(jnp.bfloat16), "seq", axis=0, tiled=True).astype(
            jnp.float32
        ),
    )
    position = lax.axis_index("seq")
    order = jnp.arange(totals.shape[0], dtype=jnp.int32)
    between = ((order[:, None] < order[None, :]) & (order[None, :] < position)).astype(jnp.float32)
    span = jnp.dot(between, totals, precision=lax.Precision.HIGHEST)
    reach_back = jnp.where(order[:, None] < position, jnp.exp(span), 0.0)
    incoming = jnp.einsum("dh,dhnp->hnp", reach_back, states, precision=lax.Precision.HIGHEST)
    inside = jnp.concatenate(partials, axis=0)
    reach = jnp.exp(jnp.concatenate(offsets, axis=0))
    arriving = state_product(c_all, incoming) * scale * reach[:, :, None]
    skipped = skip_gain[None, :, None] * values.astype(jnp.float32)[:, None, :]
    student = (
        (inside + arriving + skipped).astype(jnp.bfloat16).reshape(tok, heads_local * HEAD_DIM)
    )
    return (teacher, student)


LANES = 128
EXTRA = 16
GRANTS = tuple(mib * 1024 * 1024 for mib in (6, 12, 16, 24))
F32 = jnp.float32
BF16 = jnp.bfloat16
LAST = (((1,), (1,)), ((), ()))


def cost(flops, moved):
    return pl.CostEstimate(flops=flops, bytes_accessed=moved, transcendentals=0)


def place_of():
    grp = lax.axis_index("grp")
    return grp // 2, grp % 2, lax.axis_index("seq")


def gathered(w_ref, blocks):
    return jnp.concatenate(
        [w_ref[kv, :, pl.ds(pl.multiple_of(col * LANES, LANES), LANES)] for kv, col in blocks], axis=1
    )


def own_columns(x_ref, rows):
    first = pl.multiple_of(lax.axis_index("seq") * rows, LANES)
    return x_ref[:, pl.ds(first, rows)]


def project_kernel(places, order, x_ref, w_ref, out_ref):
    high, low, _ = place_of()
    weights = gathered(w_ref, places(high, low))
    out_ref[...] = jnp.dot(
        own_columns(x_ref, w_ref.shape[1]), weights, preferred_element_type=F32
    ).astype(BF16)


def project_add_kernel(places, order, x_ref, w_ref, r_ref, send_ref, keep_ref):
    high, low, _ = place_of()
    blocks = places(high, low)
    tok, half = keep_ref.shape
    tokens = own_columns(x_ref, w_ref.shape[1])
    first = jnp.dot(tokens, gathered(w_ref, blocks[:2]), preferred_element_type=F32)
    send_ref[:tok, :] = (first + r_ref[:, :half].astype(F32)).astype(BF16)
    second = jnp.dot(tokens, gathered(w_ref, blocks[2:]), preferred_element_type=F32)
    keep_ref[...] = second + r_ref[:, half:].astype(F32)


def folded(rates):
    half = rates.shape[1] // 2
    return jnp.concatenate([rates[:, :half], rates[:, half:]], axis=0)


def unfolded(rows):
    half = rows.shape[0] // 2
    return jnp.concatenate([rows[:half], rows[half:]], axis=1)


def project_pair_kernel(places, order, raw_ref, *refs):
    project_add_kernel(places, order, *refs)
    send_ref, tok = refs[-2], refs[-1].shape[0]
    away = EXTRA // 2
    rates = jnp.where(place_of()[0] == 0, raw_ref[away:, :], raw_ref[:away, :])
    send_ref[tok:, :] = folded(rates).astype(BF16)


def own_rates(raw_ref, u_ref):
    tok = raw_ref.shape[1]
    own = EXTRA // 2
    rates = jnp.where(place_of()[0] == 0, raw_ref[:own, :], raw_ref[own:, :])
    return rates + unfolded(u_ref[tok:, :].astype(F32))


def pair_middle_kernel(order, raw_ref, keep_ref, u_ref, send_ref):
    tok = keep_ref.shape[0]
    send_ref[:tok, :] = (keep_ref[...] + u_ref[:tok, :].astype(F32)).astype(BF16)
    send_ref[tok:, :] = folded(own_rates(raw_ref, u_ref)).astype(BF16)


def middle_kernel(order, keep_ref, u_ref, send_ref):
    send_ref[...] = (keep_ref[:, :LANES] + u_ref[:, :LANES].astype(F32)).astype(BF16)


def prepare_kernel(order, x_ref, rates_ref, raw_ref, cos_ref, sin_ref):
    raw_ref[...] = lax.dot_general(
        rates_ref[...], x_ref[...], LAST, preferred_element_type=F32
    )
    tok, wide = cos_ref.shape
    half = wide // 2
    fine = EXTRA
    lane = lax.broadcasted_iota(jnp.int32, (1, wide), 1)
    slot = jnp.where(lane < half, lane, lane - half).astype(F32)
    freq = jnp.exp(slot * (-2.0 / wide * math.log(ROPE_BASE)))
    start = lax.axis_index("seq") * tok
    coarse = lax.broadcasted_iota(jnp.int32, (tok // fine, wide), 0) * fine + start
    coarse = coarse.astype(F32) * freq
    small = lax.broadcasted_iota(jnp.int32, (fine, wide), 0).astype(F32) * freq
    cos_big, sin_big = jnp.cos(coarse), jnp.sin(coarse)
    cos_small, sin_small = jnp.cos(small), jnp.sin(small)
    sign = jnp.where(lane < half, -1.0, 1.0)
    for at in range(tok // fine):
        c, d = cos_big[at : at + 1, :], sin_big[at : at + 1, :]
        span = slice(at * fine, (at + 1) * fine)
        cos_ref[span, :] = c * cos_small - d * sin_small
        sin_ref[span, :] = (d * cos_small + c * sin_small) * sign


VMEM = pl.BlockSpec(memory_space=pltpu.VMEM)
SMEM = pl.BlockSpec(memory_space=pltpu.SMEM)
ANY = pl.BlockSpec(memory_space=pl.ANY)


def call(kernel, order, args, shapes, flops, in_specs=None, **rest):
    return pl.pallas_call(
        kernel,
        in_specs=[ANY] + (in_specs or [VMEM] * len(args)),
        out_specs=rest.pop("out_specs", [VMEM] * len(shapes)),
        out_shape=[jax.ShapeDtypeStruct(s, d) for s, d in shapes],
        compiler_params=pltpu.CompilerParams(vmem_limit_bytes=rest.pop("grant", GRANTS[1])),
        cost_estimate=cost(flops, 3 * 10**6),
        **rest,
    )(order, *args)


def project(order, x, weights, places):
    tok, rows = x.shape[0], weights.shape[1]
    wide = 4 * LANES
    return call(
        functools.partial(project_kernel, places), order, [x, weights],
        [((tok, wide), BF16)], 2 * tok * rows * wide,
    )


def project_add(order, x, weights, places, received, raw):
    tok, rows = x.shape[0], weights.shape[1]
    wide = 4 * LANES
    args, tall, kernel = [x, weights, received], tok, project_add_kernel
    if raw is not None:
        args, tall, kernel = [raw] + args, tok + EXTRA, project_pair_kernel
    shapes = [((tall, wide // 2), BF16), ((tok, wide // 2), F32)]
    return call(functools.partial(kernel, places), order, args, shapes, 2 * tok * rows * wide)


def turn(vectors, cosine, sine):
    return vectors * cosine + pltpu.roll(vectors, HEAD_DIM // 2, 1) * sine


def split_sum(rows, mask):
    high = rows.astype(BF16)
    rest = rows - high.astype(F32)
    middle = rest.astype(BF16)
    low = (rest - middle.astype(F32)).astype(BF16)
    count = rows.shape[0]
    parts = jnp.concatenate([high.astype(F32), middle.astype(F32), low.astype(F32)], axis=0)
    sums = lax.dot_general(parts.astype(BF16), mask, LAST, preferred_element_type=F32)
    return sums[:count] + (sums[count : 2 * count] + sums[2 * count :])


def upright(row):
    count = row.shape[1]
    down = lax.broadcasted_iota(jnp.int32, (count, count), 0)
    along = lax.broadcasted_iota(jnp.int32, (count, count), 1)
    return jnp.sum(jnp.where(down == along, row, 0.0), axis=1, keepdims=True)


def context_kernel(
    stretch, order, raw_ref, keep_ref, u_ref, z_ref, cos_ref, sin_ref, bias_ref, rate_ref,
    carry_ref, bterm_ref, across_ref, down_ref, step_ref, first_ref,
):
    tok = keep_ref.shape[0]
    heads = bias_ref.shape[1]
    spans = tok // stretch
    pair = keep_ref[...] + u_ref[:tok, :].astype(F32) + z_ref[:tok, :].astype(F32)
    keys = pair[:, :HEAD_DIM]
    values = pair[:, HEAD_DIM:].astype(BF16)
    bterm = keys.astype(BF16)
    carry_ref[:tok, :HEAD_DIM] = turn(keys, cos_ref[...], sin_ref[...]).astype(BF16)
    carry_ref[:tok, HEAD_DIM:] = values
    bterm_ref[...] = bterm
    both = own_rates(raw_ref, u_ref) + unfolded(z_ref[tok:, :].astype(F32))
    raw = jnp.where(place_of()[1] == 0, both[:heads], both[heads:])
    bias, rate = upright(bias_ref[...]), upright(rate_ref[...])
    step = jax.nn.softplus(raw + bias)
    decay = -rate * step
    rows = lax.broadcasted_iota(jnp.int32, (stretch, stretch), 0)
    cols = lax.broadcasted_iota(jnp.int32, (stretch, stretch), 1)
    below = (cols <= rows).astype(F32).astype(BF16)
    fold = lambda a: jnp.concatenate([a[:, i * stretch : (i + 1) * stretch] for i in range(spans)], axis=0)
    across = split_sum(fold(decay), below)
    steps = fold(step)
    tails = jnp.exp(across[:, stretch - 1 :] - across) * steps
    across_ref[...] = across
    step_ref[...] = steps
    count = heads * spans
    filler = jnp.zeros((LANES - 2 * count, stretch), F32)
    down = jnp.transpose(jnp.concatenate([across, tails, filler], axis=0))
    down_ref[...] = down
    states = [None] * heads
    for index in range(spans):
        span = slice(index * stretch, (index + 1) * stretch)
        part = bterm[span].astype(F32)
        weighted = jnp.concatenate(
            [
                (part * down[:, count + index * heads + h : count + index * heads + h + 1]).astype(BF16)
                for h in range(heads)
            ],
            axis=1,
        )
        fresh = lax.dot_general(
            weighted, values[span], (((0,), (0,)), ((), ())), preferred_element_type=F32
        )
        for h in range(heads):
            new = fresh[h * HEAD_DIM : (h + 1) * HEAD_DIM]
            if index > 0:
                at = index * heads + h
                new = new + jnp.exp(across[at : at + 1, stretch - 1 :]) * states[h]
            else:
                first_ref[h] = new
            states[h] = new
    for h in range(heads):
        row, col = tok + (h // 2) * HEAD_DIM, (h % 2) * HEAD_DIM
        carry_ref[row : row + HEAD_DIM, col : col + HEAD_DIM] = states[h].astype(BF16)


def head_kernel(
    stretch, head, order, keep_ref, u_ref, z_ref, cos_ref, sin_ref, carry_ref, bterm_ref, came_ref,
    across_ref, down_ref, step_ref, first_ref, skip_ref, *rest,
):
    if len(rest) == 2:
        teacher_ref, student_ref = rest
    else:
        teacher_out, student_out, teacher_ref, student_ref, sems = rest[-5:]
        before, copies = rest[:-5], []
        for at, held in enumerate(before):
            number, kind = at // 2, at % 2
            number = number + (number >= head)
            out = (teacher_out, student_out)[kind]
            place = slice(number * HEAD_DIM, (number + 1) * HEAD_DIM)
            copies.append(pltpu.make_async_copy(held, out.at[:, place], sems.at[at]))
            copies[-1].start()
    tok = bterm_ref.shape[0]
    heads = first_ref.shape[0]
    scale = HEAD_DIM ** (-0.5)
    power = scale * 1.4426950408889634
    later = (lax.axis_index("seq") > 0).astype(F32)
    blocked = (1.0 - later) * FAR_BELOW
    rows = lax.broadcasted_iota(jnp.int32, (stretch, stretch), 0)
    cols = lax.broadcasted_iota(jnp.int32, (stretch, stretch), 1)
    causal = cols <= rows
    ones = jnp.ones((tok, HEAD_DIM), BF16)
    own_keys = carry_ref[:tok, :HEAD_DIM]
    prev_keys = came_ref[:tok, :HEAD_DIM]
    own_values = jnp.concatenate([carry_ref[:tok, HEAD_DIM:], ones], axis=1)
    prev_values = jnp.concatenate([came_ref[:tok, HEAD_DIM:], ones], axis=1)
    query = keep_ref[:, LANES:] + u_ref[:, LANES:].astype(F32) + z_ref[...].astype(F32)
    turned = turn(query, cos_ref[...], sin_ref[...]).astype(BF16)
    cterm = query.astype(BF16)
    row, col = tok + (head // 2) * HEAD_DIM, (head % 2) * HEAD_DIM
    state = came_ref[row : row + HEAD_DIM, col : col + HEAD_DIM].astype(F32) * later
    skip = skip_ref[:, head : head + 1]
    for index in range(tok // stretch):
        span = slice(index * stretch, (index + 1) * stretch)
        reach = (index + 1) * stretch
        queries = turned[span]
        far = lax.dot_general(queries, prev_keys, LAST, preferred_element_type=F32) + blocked
        near = lax.dot_general(queries, own_keys[:reach], LAST, preferred_element_type=F32)
        diagonal = jnp.where(causal, near[:, index * stretch :], FAR_BELOW)
        if index > 0:
            near = jnp.concatenate([near[:, : index * stretch], diagonal], axis=1)
        else:
            near = diagonal
        top = jnp.maximum(
            jnp.max(far, axis=1, keepdims=True), jnp.max(near, axis=1, keepdims=True)
        )
        far = jnp.exp2((far - top) * power).astype(BF16)
        near = jnp.exp2((near - top) * power).astype(BF16)
        mixed = jnp.dot(far, prev_values, preferred_element_type=F32) + jnp.dot(
            near, own_values[:reach], preferred_element_type=F32
        )
        teacher_ref[span, :] = (mixed[:, :HEAD_DIM] / mixed[:, HEAD_DIM:]).astype(BF16)
        values = carry_ref[span, HEAD_DIM:]
        which = index * heads + head
        down = down_ref[:, which : which + 1]
        across = across_ref[which : which + 1, :]
        gram = lax.dot_general(
            cterm[span], bterm_ref[span, :], LAST, preferred_element_type=F32
        ) * (step_ref[which : which + 1, :] * scale)
        mix = jnp.where(causal, jnp.exp(jnp.where(causal, down - across, -1e4)) * gram, 0.0)
        inner = jnp.dot(mix.astype(BF16), values, preferred_element_type=F32)
        high = state.astype(BF16)
        low = (state - high.astype(F32)).astype(BF16)
        carried = jnp.dot(
            cterm[span], jnp.concatenate([high, low], axis=1), preferred_element_type=F32
        )
        carried = (carried[:, :HEAD_DIM] + carried[:, HEAD_DIM:]) * (jnp.exp(down) * scale)
        student_ref[span, :] = (inner + carried + skip * values.astype(F32)).astype(BF16)
        if index == 0:
            state = jnp.exp(across[:, stretch - 1 :]) * state + first_ref[head]
    if len(rest) > 2:
        place = slice(head * HEAD_DIM, (head + 1) * HEAD_DIM)
        for kind, (held, out) in enumerate(((teacher_ref, teacher_out), (student_ref, student_out))):
            copies.append(
                pltpu.make_async_copy(held, out.at[:, place], sems.at[len(before) + kind])
            )
            copies[-1].start()
        for copy in copies:
            copy.wait()


def head_call(order, head, piece, shared, total, before):
    tok = piece[0].shape[0]
    args = list(piece) + list(shared)
    kernel = functools.partial(head_kernel, STRETCH, head)
    if before is None:
        return call(kernel, order, args, [((tok, HEAD_DIM), BF16)] * 2, 10**9, grant=GRANTS[2])
    args += before
    held = pltpu.VMEM((tok, HEAD_DIM), BF16)
    return call(
        kernel, order, args, [((tok, total), BF16)] * 2, 10**9, out_specs=[ANY] * 2, grant=GRANTS[2],
        scratch_shapes=[held, held, pltpu.SemaphoreType.DMA((len(before) + 2,))],
    )


def pair_body(*args):
    return pair_steps(*args)


def pair_steps(layer_input, attn_weight, rate_weight, rate_bias, decay_rate, skip_gain):
    tok, _ = layer_input.shape
    heads = rate_bias.shape[0]
    group = HEADS // KV_HEADS
    ids = skip_gain[:1]
    count = lax.axis_size("grp")
    swap_high = [(g, g ^ 2) for g in range(count)]
    swap_low = [(g, g ^ 1) for g in range(count)]
    over_high = lambda a: lax.ppermute(a, "grp", swap_high)
    over_low = lambda a: lax.ppermute(a, "grp", swap_low)
    over_seq = lambda a: lax.ppermute(a, "seq", [(0, 1), (1, 0)])

    other = over_seq(layer_input)
    weights_all = jnp.transpose(attn_weight, (1, 0, 2))
    shapes = [((EXTRA, tok), F32), ((tok, HEAD_DIM), F32), ((tok, HEAD_DIM), F32)]

    def pair_places(h, l):
        return [(1 - h, group), (1 - h, group + 1), (h, group), (h, group + 1)]

    def high_places(j):
        return lambda h, l: [
            (1 - h, (1 - l) * heads + j), (1 - h, l * heads + j),
            (h, (1 - l) * heads + j), (h, l * heads + j),
        ]

    def low_places(j):
        return lambda h, l: [
            (1 - h, (1 - l) * heads + j), (h, (1 - l) * heads + j),
            (1 - h, l * heads + j), (h, l * heads + j),
        ]

    ahead = [(ids, weights_all)]

    def queued(make):
        ready, _ = lax.optimization_barrier((ids, ahead[0]))
        outs = make(ready)
        ahead[0] = outs[0]
        return outs

    def prepare():
        return queued(
            lambda ready: call(prepare_kernel, ready, [layer_input, rate_weight.T], shapes, 10**9)
        )

    raw, cosine, sine = prepare()
    other, weights_all, raw = lax.optimization_barrier((other, weights_all, raw))
    plan = [(None, weights_all, pair_places, over_high, over_low)]
    for pair in range(heads // 2):
        plan.append((2 * pair + 1, weights_all, low_places(2 * pair + 1), over_low, over_high))
        plan.append((2 * pair, weights_all, high_places(2 * pair), over_high, over_low))
    crossed, parts, arrived, pieces, kept = {}, {}, {}, {}, {}

    def cross(at):
        _, weights, places, _, _ = plan[at]
        out = queued(lambda ready: project(ready, other, weights, places))[0]
        crossed[at] = over_seq(out)

    def mine(at):
        j, weights, places, first, _ = plan[at]
        send, kept[at] = queued(
            lambda ready: project_add(
                ready, layer_input, weights, places, crossed[at],
                raw if j is None else None,
            )
        )
        parts[at] = first(send)

    def middle(at):
        j, _, _, _, second = plan[at]
        keep, u = kept[at], parts[at]
        if j is None:
            shapes = [((tok + EXTRA, 2 * HEAD_DIM), BF16)]
            send = queued(lambda ready: call(pair_middle_kernel, ready, [raw, keep, u], shapes, 10**7))[0]
        else:
            shapes = [((tok, LANES), BF16)]
            send = queued(lambda ready: call(middle_kernel, ready, [keep, u], shapes, 10**7))[0]
        arrived[at] = second(send)
        if j is not None:
            pieces[j] = (keep, u, arrived[at])

    def context():
        args = [
            raw, kept[0], parts[0], arrived[0], cosine, sine, rate_bias[None, :], decay_rate[None, :],
        ]
        spans = tok // STRETCH
        shapes = [
            ((tok + heads // 2 * HEAD_DIM, 2 * HEAD_DIM), BF16), ((tok, HEAD_DIM), BF16),
            ((heads * spans, STRETCH), F32), ((STRETCH, LANES), F32), ((heads * spans, STRETCH), F32),
            ((heads, HEAD_DIM, HEAD_DIM), F32),
        ]
        carry, *rest = queued(
            lambda ready: call(
                functools.partial(context_kernel, STRETCH), ready, args, shapes, 10**9,
                grant=GRANTS[2],
            )
        )
        came = over_seq(carry)
        bterm, across, down, step, first_state = rest
        return (
            cosine, sine, carry, bterm, came, across, down, step, first_state, skip_gain[None, :],
        )

    def tail(j, shared, before):
        return queued(
            lambda ready: head_call(ready, j, pieces[j], shared, heads * HEAD_DIM, before)
        )

    cross(0)
    cross(1)
    cross(2)
    mine(0)
    mine(1)
    mine(2)
    cross(4)
    cross(3)
    middle(0)
    mine(4)
    mine(3)
    middle(1)
    middle(2)
    shared = context()
    middle(4)
    done = {1: tail(1, shared, None)}
    middle(3)
    for j in (0, 3):
        done[j] = tail(j, shared, None)
    outs = tail(2, shared, [part for j in sorted(done) for part in done[j]])
    return outs[0], outs[1]


def solution(mesh):
    placed = (
        P("seq", "grp"),
        P(("grp", "seq"), "mdl", None),
        P("grp", "mdl"),
        P(("mdl", "grp")),
        P(("mdl", "grp")),
        P(("mdl", "grp")),
    )
    chips = mesh.shape["grp"] * mesh.shape["mdl"]
    paired = (
        mesh.shape["seq"] == 2
        and mesh.shape["grp"] == 4
        and KV_HEADS == 2 * mesh.shape["mdl"]
        and HEADS // chips == 4
    )
    return jax.shard_map(
        pair_body if paired else body,
        mesh=mesh,
        in_specs=placed,
        out_specs=(P("seq", ("mdl", "grp")), P("seq", ("mdl", "grp"))),
        check_vma=False,
    )
```

```python
import functools
import math

import jax
import jax.numpy as jnp
from jax import lax
from jax.experimental import pallas as pl
from jax.experimental.pallas import tpu as pltpu
from jax.sharding import PartitionSpec as P


HEADS = 64
KV_HEADS = 8
HEAD_DIM = 128
STRETCH = 256


ROPE_BASE = 500000.0
FAR_BELOW = -1e30


def rope_angles(positions):
    half = HEAD_DIM // 2
    freq = ROPE_BASE ** (-2.0 * jnp.arange(half, dtype=jnp.float32) / HEAD_DIM)
    angle = positions.astype(jnp.float32)[:, None] * freq[None, :]
    return (jnp.cos(angle), jnp.sin(angle))


def rotate(vectors, cosine, sine):
    half = vectors.shape[-1] // 2
    first = vectors[..., :half]
    second = vectors[..., half:]
    cosine = cosine[:, None, :]
    sine = sine[:, None, :]
    return jnp.concatenate(
        [first * cosine - second * sine, second * cosine + first * sine], axis=-1
    )


def state_product(cterm, state):
    high = state.astype(jnp.bfloat16)
    low = (state - high.astype(jnp.float32)).astype(jnp.bfloat16)
    upper = jnp.einsum("thn,hnp->thp", cterm, high, preferred_element_type=jnp.float32)
    return upper + jnp.einsum("thn,hnp->thp", cterm, low, preferred_element_type=jnp.float32)


def key_absorber(queries, own_first, scale, carry, piece):
    top, total, accum = carry
    keys, values = piece
    scores = jnp.einsum("thd,nd->thn", queries, keys, preferred_element_type=jnp.float32) * scale
    query_pos = own_first + jnp.arange(queries.shape[0], dtype=jnp.int32)
    key_pos = jnp.arange(keys.shape[0], dtype=jnp.int32)
    causal = (key_pos[None, :] <= query_pos[:, None])[:, None, :]
    masked = jnp.where(causal, scores, FAR_BELOW)
    new_top = jnp.maximum(top, jnp.max(masked, axis=2))
    weights = jnp.where(causal, jnp.exp(masked - new_top[:, :, None]), 0.0)
    total = jnp.sum(weights, axis=2)
    accum = jnp.einsum(
        "thn,nd->thd", weights.astype(jnp.bfloat16), values, preferred_element_type=jnp.float32
    )
    return (new_top, total, accum)


def body(layer_input, attn_weight, rate_weight, rate_bias, decay_rate, skip_gain):
    tok = layer_input.shape[0]
    kv_local = attn_weight.shape[1]
    heads_local = rate_bias.shape[0]
    group = HEADS // KV_HEADS
    scale = HEAD_DIM ** (-0.5)
    merged = jnp.einsum(
        "td,dkc->tkc",
        layer_input,
        lax.all_gather(attn_weight, "seq", axis=0, tiled=True),
        preferred_element_type=jnp.float32,
    )
    rate_part = jnp.dot(layer_input, rate_weight, preferred_element_type=jnp.float32)
    grp_index = lax.axis_index("grp")
    summed, rate_whole = (
        lax.psum(merged.astype(jnp.bfloat16), "grp").astype(jnp.float32),
        lax.psum(rate_part.astype(jnp.bfloat16), "grp").astype(jnp.float32),
    )
    query_whole = summed[:, :, : group * HEAD_DIM].reshape(tok, kv_local * group * HEAD_DIM)
    query_flat = lax.dynamic_slice_in_dim(
        query_whole, grp_index * heads_local * HEAD_DIM, heads_local * HEAD_DIM, 1
    )
    raw = lax.dynamic_slice_in_dim(rate_whole, grp_index * heads_local, heads_local, 1)
    pairs = summed[:, :, group * HEAD_DIM :]
    kv_index = grp_index * heads_local // group
    pair = lax.dynamic_index_in_dim(pairs, kv_index, 1, keepdims=False)
    keys = pair[:, :HEAD_DIM]
    values = pair[:, HEAD_DIM:].astype(jnp.bfloat16)
    query = query_flat.reshape(tok, heads_local, HEAD_DIM)
    own_first = lax.axis_index("seq") * tok
    cosine, sine = rope_angles(own_first + jnp.arange(tok, dtype=jnp.int32))
    rot_query = rotate(query, cosine, sine).astype(jnp.bfloat16)
    rot_keys = rotate(keys[:, None, :], cosine, sine)[:, 0].astype(jnp.bfloat16)
    start_carry = (
        jnp.full((tok, heads_local), FAR_BELOW, jnp.float32),
        jnp.zeros((tok, heads_local), jnp.float32),
        jnp.zeros((tok, heads_local, HEAD_DIM), jnp.float32),
    )
    _, total, accum = key_absorber(
        rot_query,
        own_first,
        scale,
        start_carry,
        (
            lax.all_gather(rot_keys, "seq", axis=0, tiled=True),
            lax.all_gather(values, "seq", axis=0, tiled=True),
        ),
    )
    teacher = (accum / total[:, :, None]).astype(jnp.bfloat16).reshape(tok, heads_local * HEAD_DIM)
    step = jax.nn.softplus(raw + rate_bias[None, :])
    log_decay = -decay_rate[None, :] * step
    c_all = query.astype(jnp.bfloat16)
    b_all = keys.astype(jnp.bfloat16)
    causal = (
        jnp.arange(STRETCH, dtype=jnp.int32)[:, None]
        >= jnp.arange(STRETCH, dtype=jnp.int32)[None, :]
    )[None]
    state = jnp.zeros((heads_local, HEAD_DIM, HEAD_DIM), jnp.float32)
    before = jnp.zeros((heads_local,), jnp.float32)
    partials = []
    offsets = []
    for index in range(tok // STRETCH):
        first = index * STRETCH
        cpart = c_all[first : first + STRETCH]
        bpart = b_all[first : first + STRETCH]
        xpart = values[first : first + STRETCH]
        decay = log_decay[first : first + STRETCH]
        rate = step[first : first + STRETCH]
        cum = jnp.cumsum(decay, axis=0)
        gram = jnp.einsum("thn,sn->hts", cpart, bpart, preferred_element_type=jnp.float32) * scale
        diff = cum.T[:, :, None] - cum.T[:, None, :]
        mix = jnp.where(
            causal, jnp.exp(jnp.where(causal, diff, -10000.0)) * rate.T[:, None, :] * gram, 0.0
        ).astype(jnp.bfloat16)
        intra = jnp.einsum("hts,sp->thp", mix, xpart, preferred_element_type=jnp.float32)
        carried = state_product(cpart, state) * scale * jnp.exp(cum)[:, :, None]
        weighted = (
            (jnp.exp(cum[-1][None, :] - cum) * rate)[:, :, None]
            * bpart.astype(jnp.float32)[:, None, :]
        ).astype(jnp.bfloat16)
        contribution = jnp.einsum(
            "shn,sp->hnp", weighted, xpart, preferred_element_type=jnp.float32
        )
        state = jnp.exp(cum[-1])[:, None, None] * state + contribution
        partials.append(intra + carried)
        offsets.append(cum + before[None, :])
        before = before + cum[-1]
    totals, states = (
        lax.all_gather(before[None, :].astype(jnp.bfloat16), "seq", axis=0, tiled=True).astype(
            jnp.float32
        ),
        lax.all_gather(state[None].astype(jnp.bfloat16), "seq", axis=0, tiled=True).astype(
            jnp.float32
        ),
    )
    position = lax.axis_index("seq")
    order = jnp.arange(totals.shape[0], dtype=jnp.int32)
    between = ((order[:, None] < order[None, :]) & (order[None, :] < position)).astype(jnp.float32)
    span = jnp.dot(between, totals, precision=lax.Precision.HIGHEST)
    reach_back = jnp.where(order[:, None] < position, jnp.exp(span), 0.0)
    incoming = jnp.einsum("dh,dhnp->hnp", reach_back, states, precision=lax.Precision.HIGHEST)
    inside = jnp.concatenate(partials, axis=0)
    reach = jnp.exp(jnp.concatenate(offsets, axis=0))
    arriving = state_product(c_all, incoming) * scale * reach[:, :, None]
    skipped = skip_gain[None, :, None] * values.astype(jnp.float32)[:, None, :]
    student = (
        (inside + arriving + skipped).astype(jnp.bfloat16).reshape(tok, heads_local * HEAD_DIM)
    )
    return (teacher, student)


LANES = 128
EXTRA = 16
GRANTS = tuple(mib * 1024 * 1024 for mib in (6, 12, 16, 24))
F32 = jnp.float32
BF16 = jnp.bfloat16
LAST = (((1,), (1,)), ((), ()))


def cost(flops, moved):
    return pl.CostEstimate(flops=flops, bytes_accessed=moved, transcendentals=0)


def place_of():
    grp = lax.axis_index("grp")
    return grp // 2, grp % 2, lax.axis_index("seq")


def gathered(w_ref, blocks):
    return jnp.concatenate(
        [w_ref[kv, :, pl.ds(pl.multiple_of(col * LANES, LANES), LANES)] for kv, col in blocks], axis=1
    )


def own_columns(x_ref, rows):
    first = pl.multiple_of(lax.axis_index("seq") * rows, LANES)
    return x_ref[:, pl.ds(first, rows)]


def project_kernel(places, order, x_ref, w_ref, out_ref):
    high, low, _ = place_of()
    weights = gathered(w_ref, places(high, low))
    out_ref[...] = jnp.dot(
        own_columns(x_ref, w_ref.shape[1]), weights, preferred_element_type=F32
    ).astype(BF16)


def project_add_kernel(places, order, x_ref, w_ref, r_ref, send_ref, keep_ref):
    high, low, _ = place_of()
    blocks = places(high, low)
    tok, half = keep_ref.shape
    tokens = own_columns(x_ref, w_ref.shape[1])
    first = jnp.dot(tokens, gathered(w_ref, blocks[:2]), preferred_element_type=F32)
    send_ref[:tok, :] = (first + r_ref[:, :half].astype(F32)).astype(BF16)
    second = jnp.dot(tokens, gathered(w_ref, blocks[2:]), preferred_element_type=F32)
    keep_ref[...] = second + r_ref[:, half:].astype(F32)


def folded(rates):
    parts = rates.shape[1] // LANES
    return jnp.concatenate([rates[:, i * LANES : (i + 1) * LANES] for i in range(parts)], axis=0)


def unfolded(rows, count):
    parts = rows.shape[0] // count
    return jnp.concatenate([rows[i * count : (i + 1) * count] for i in range(parts)], axis=1)


def project_pair_kernel(places, order, raw_ref, x_ref, w_ref, r_ref, keys_ref, values_ref, keep_ref):
    high, low, _ = place_of()
    blocks = places(high, low)
    tok, half = keep_ref.shape
    tokens = own_columns(x_ref, w_ref.shape[1])
    first = jnp.dot(tokens, gathered(w_ref, blocks[:2]), preferred_element_type=F32)
    first = (first + r_ref[:, :half].astype(F32)).astype(BF16)
    keys_ref[:tok, :] = first[:, :LANES]
    values_ref[...] = first[:, LANES:]
    second = jnp.dot(tokens, gathered(w_ref, blocks[2:]), preferred_element_type=F32)
    keep_ref[...] = second + r_ref[:, half:].astype(F32)
    away = EXTRA // 2
    rates = jnp.where(high == 0, raw_ref[away:, :], raw_ref[:away, :])
    keys_ref[tok:, :] = folded(rates).astype(BF16)


def own_rates(raw_ref, u_ref):
    tok = raw_ref.shape[1]
    own = EXTRA // 2
    rates = jnp.where(place_of()[0] == 0, raw_ref[:own, :], raw_ref[own:, :])
    return rates + unfolded(u_ref[tok:, :].astype(F32), own)


def keys_middle_kernel(order, raw_ref, keep_ref, u_ref, send_ref):
    tok = keep_ref.shape[0]
    send_ref[:tok, :] = (keep_ref[:, :LANES] + u_ref[:tok, :].astype(F32)).astype(BF16)
    send_ref[tok:, :] = folded(own_rates(raw_ref, u_ref)).astype(BF16)


def values_middle_kernel(order, keep_ref, u_ref, send_ref):
    send_ref[...] = (keep_ref[:, LANES:] + u_ref[...].astype(F32)).astype(BF16)


def middle_kernel(order, keep_ref, u_ref, send_ref):
    send_ref[...] = (keep_ref[:, :LANES] + u_ref[:, :LANES].astype(F32)).astype(BF16)


def prepare_kernel(order, x_ref, rates_ref, raw_ref, cos_ref, sin_ref):
    raw_ref[...] = lax.dot_general(
        rates_ref[...], x_ref[...], LAST, preferred_element_type=F32
    )
    tok, wide = cos_ref.shape
    half = wide // 2
    fine = EXTRA
    lane = lax.broadcasted_iota(jnp.int32, (1, wide), 1)
    slot = jnp.where(lane < half, lane, lane - half).astype(F32)
    freq = jnp.exp(slot * (-2.0 / wide * math.log(ROPE_BASE)))
    start = lax.axis_index("seq") * tok
    coarse = lax.broadcasted_iota(jnp.int32, (tok // fine, wide), 0) * fine + start
    coarse = coarse.astype(F32) * freq
    small = lax.broadcasted_iota(jnp.int32, (fine, wide), 0).astype(F32) * freq
    cos_big, sin_big = jnp.cos(coarse), jnp.sin(coarse)
    cos_small, sin_small = jnp.cos(small), jnp.sin(small)
    sign = jnp.where(lane < half, -1.0, 1.0)
    for at in range(tok // fine):
        c, d = cos_big[at : at + 1, :], sin_big[at : at + 1, :]
        span = slice(at * fine, (at + 1) * fine)
        cos_ref[span, :] = c * cos_small - d * sin_small
        sin_ref[span, :] = (d * cos_small + c * sin_small) * sign


VMEM = pl.BlockSpec(memory_space=pltpu.VMEM)
SMEM = pl.BlockSpec(memory_space=pltpu.SMEM)
ANY = pl.BlockSpec(memory_space=pl.ANY)


def call(kernel, order, args, shapes, flops, in_specs=None, **rest):
    return pl.pallas_call(
        kernel,
        in_specs=[ANY] + (in_specs or [VMEM] * len(args)),
        out_specs=rest.pop("out_specs", [VMEM] * len(shapes)),
        out_shape=[jax.ShapeDtypeStruct(s, d) for s, d in shapes],
        compiler_params=pltpu.CompilerParams(vmem_limit_bytes=rest.pop("grant", GRANTS[1])),
        cost_estimate=cost(flops, 3 * 10**6),
        **rest,
    )(order, *args)


def project(order, x, weights, places):
    tok, rows = x.shape[0], weights.shape[1]
    wide = 4 * LANES
    return call(
        functools.partial(project_kernel, places), order, [x, weights],
        [((tok, wide), BF16)], 2 * tok * rows * wide,
    )


def project_add(order, x, weights, places, received, raw):
    tok, rows = x.shape[0], weights.shape[1]
    wide = 4 * LANES
    args, kernel = [x, weights, received], project_add_kernel
    kept = ((tok, wide // 2), F32)
    if raw is None:
        shapes = [((tok, wide // 2), BF16), kept]
    else:
        args, kernel = [raw] + args, project_pair_kernel
        tall = tok + EXTRA // 2 * tok // LANES
        shapes = [((tall, LANES), BF16), ((tok, LANES), BF16), kept]
    return call(functools.partial(kernel, places), order, args, shapes, 2 * tok * rows * wide)


def turn(vectors, cosine, sine):
    return vectors * cosine + pltpu.roll(vectors, HEAD_DIM // 2, 1) * sine


def split_sum(rows, mask):
    high = rows.astype(BF16)
    rest = rows - high.astype(F32)
    middle = rest.astype(BF16)
    low = (rest - middle.astype(F32)).astype(BF16)
    count = rows.shape[0]
    parts = jnp.concatenate([high.astype(F32), middle.astype(F32), low.astype(F32)], axis=0)
    sums = lax.dot_general(parts.astype(BF16), mask, LAST, preferred_element_type=F32)
    return sums[:count] + (sums[count : 2 * count] + sums[2 * count :])


def upright(row):
    count = row.shape[1]
    down = lax.broadcasted_iota(jnp.int32, (count, count), 0)
    along = lax.broadcasted_iota(jnp.int32, (count, count), 1)
    return jnp.sum(jnp.where(down == along, row, 0.0), axis=1, keepdims=True)


def context_kernel(
    stretch, order, raw_ref, keep_ref, u_ref, u_values_ref, z_ref, z_values_ref, cos_ref, sin_ref,
    bias_ref, rate_ref,
    carry_ref, bterm_ref, across_ref, down_ref, step_ref, first_ref,
):
    tok = keep_ref.shape[0]
    heads = bias_ref.shape[1]
    spans = tok // stretch
    keys = keep_ref[:, :LANES] + u_ref[:tok, :].astype(F32) + z_ref[:tok, :].astype(F32)
    values = keep_ref[:, LANES:] + u_values_ref[...].astype(F32) + z_values_ref[...].astype(F32)
    values = values.astype(BF16)
    bterm = keys.astype(BF16)
    carry_ref[:tok, :HEAD_DIM] = turn(keys, cos_ref[...], sin_ref[...]).astype(BF16)
    carry_ref[:tok, HEAD_DIM:] = values
    bterm_ref[...] = bterm
    both = own_rates(raw_ref, u_ref) + unfolded(z_ref[tok:, :].astype(F32), EXTRA // 2)
    raw = jnp.where(place_of()[1] == 0, both[:heads], both[heads:])
    bias, rate = upright(bias_ref[...]), upright(rate_ref[...])
    step = jax.nn.softplus(raw + bias)
    decay = -rate * step
    rows = lax.broadcasted_iota(jnp.int32, (stretch, stretch), 0)
    cols = lax.broadcasted_iota(jnp.int32, (stretch, stretch), 1)
    below = (cols <= rows).astype(F32).astype(BF16)
    fold = lambda a: jnp.concatenate([a[:, i * stretch : (i + 1) * stretch] for i in range(spans)], axis=0)
    across = split_sum(fold(decay), below)
    steps = fold(step)
    tails = jnp.exp(across[:, stretch - 1 :] - across) * steps
    across_ref[...] = across
    step_ref[...] = steps
    count = heads * spans
    filler = jnp.zeros((LANES - 2 * count, stretch), F32)
    down = jnp.transpose(jnp.concatenate([across, tails, filler], axis=0))
    down_ref[...] = down
    states = [None] * heads
    for index in range(spans):
        span = slice(index * stretch, (index + 1) * stretch)
        part = bterm[span].astype(F32)
        weighted = jnp.concatenate(
            [
                (part * down[:, count + index * heads + h : count + index * heads + h + 1]).astype(BF16)
                for h in range(heads)
            ],
            axis=1,
        )
        fresh = lax.dot_general(
            weighted, values[span], (((0,), (0,)), ((), ())), preferred_element_type=F32
        )
        for h in range(heads):
            new = fresh[h * HEAD_DIM : (h + 1) * HEAD_DIM]
            if index > 0:
                at = index * heads + h
                new = new + jnp.exp(across[at : at + 1, stretch - 1 :]) * states[h]
            else:
                first_ref[h] = new
            states[h] = new
    for h in range(heads):
        row, col = tok + (h // 2) * HEAD_DIM, (h % 2) * HEAD_DIM
        carry_ref[row : row + HEAD_DIM, col : col + HEAD_DIM] = states[h].astype(BF16)


def head_kernel(
    stretch, head, order, keep_ref, u_ref, z_ref, cos_ref, sin_ref, carry_ref, bterm_ref, came_ref,
    across_ref, down_ref, step_ref, first_ref, skip_ref, *rest,
):
    if len(rest) == 2:
        teacher_ref, student_ref = rest
    else:
        teacher_out, student_out, teacher_ref, student_ref, sems = rest[-5:]
        before, copies = rest[:-5], []
        for at, held in enumerate(before):
            number, kind = at // 2, at % 2
            number = number + (number >= head)
            out = (teacher_out, student_out)[kind]
            place = slice(number * HEAD_DIM, (number + 1) * HEAD_DIM)
            copies.append(pltpu.make_async_copy(held, out.at[:, place], sems.at[at]))
            copies[-1].start()
    tok = bterm_ref.shape[0]
    heads = first_ref.shape[0]
    scale = HEAD_DIM ** (-0.5)
    power = scale * 1.4426950408889634
    later = (lax.axis_index("seq") > 0).astype(F32)
    blocked = (1.0 - later) * FAR_BELOW
    rows = lax.broadcasted_iota(jnp.int32, (stretch, stretch), 0)
    cols = lax.broadcasted_iota(jnp.int32, (stretch, stretch), 1)
    causal = cols <= rows
    ones = jnp.ones((tok, HEAD_DIM), BF16)
    own_keys = carry_ref[:tok, :HEAD_DIM]
    prev_keys = came_ref[:tok, :HEAD_DIM]
    own_values = jnp.concatenate([carry_ref[:tok, HEAD_DIM:], ones], axis=1)
    prev_values = jnp.concatenate([came_ref[:tok, HEAD_DIM:], ones], axis=1)
    query = keep_ref[:, LANES:] + u_ref[:, LANES:].astype(F32) + z_ref[...].astype(F32)
    turned = turn(query, cos_ref[...], sin_ref[...]).astype(BF16)
    cterm = query.astype(BF16)
    row, col = tok + (head // 2) * HEAD_DIM, (head % 2) * HEAD_DIM
    state = came_ref[row : row + HEAD_DIM, col : col + HEAD_DIM].astype(F32) * later
    skip = skip_ref[:, head : head + 1]
    for index in range(tok // stretch):
        span = slice(index * stretch, (index + 1) * stretch)
        reach = (index + 1) * stretch
        queries = turned[span]
        far = lax.dot_general(queries, prev_keys, LAST, preferred_element_type=F32) + blocked
        near = lax.dot_general(queries, own_keys[:reach], LAST, preferred_element_type=F32)
        diagonal = jnp.where(causal, near[:, index * stretch :], FAR_BELOW)
        if index > 0:
            near = jnp.concatenate([near[:, : index * stretch], diagonal], axis=1)
        else:
            near = diagonal
        top = jnp.maximum(
            jnp.max(far, axis=1, keepdims=True), jnp.max(near, axis=1, keepdims=True)
        )
        far = jnp.exp2((far - top) * power).astype(BF16)
        near = jnp.exp2((near - top) * power).astype(BF16)
        mixed = jnp.dot(far, prev_values, preferred_element_type=F32) + jnp.dot(
            near, own_values[:reach], preferred_element_type=F32
        )
        teacher_ref[span, :] = (mixed[:, :HEAD_DIM] / mixed[:, HEAD_DIM:]).astype(BF16)
        values = carry_ref[span, HEAD_DIM:]
        which = index * heads + head
        down = down_ref[:, which : which + 1]
        across = across_ref[which : which + 1, :]
        gram = lax.dot_general(
            cterm[span], bterm_ref[span, :], LAST, preferred_element_type=F32
        ) * (step_ref[which : which + 1, :] * scale)
        mix = jnp.where(causal, jnp.exp(jnp.where(causal, down - across, -1e4)) * gram, 0.0)
        inner = jnp.dot(mix.astype(BF16), values, preferred_element_type=F32)
        high = state.astype(BF16)
        low = (state - high.astype(F32)).astype(BF16)
        carried = jnp.dot(
            cterm[span], jnp.concatenate([high, low], axis=1), preferred_element_type=F32
        )
        carried = (carried[:, :HEAD_DIM] + carried[:, HEAD_DIM:]) * (jnp.exp(down) * scale)
        student_ref[span, :] = (inner + carried + skip * values.astype(F32)).astype(BF16)
        if index == 0:
            state = jnp.exp(across[:, stretch - 1 :]) * state + first_ref[head]
    if len(rest) > 2:
        place = slice(head * HEAD_DIM, (head + 1) * HEAD_DIM)
        for kind, (held, out) in enumerate(((teacher_ref, teacher_out), (student_ref, student_out))):
            copies.append(
                pltpu.make_async_copy(held, out.at[:, place], sems.at[len(before) + kind])
            )
            copies[-1].start()
        for copy in copies:
            copy.wait()


def head_call(order, head, piece, shared, total, before):
    tok = piece[0].shape[0]
    args = list(piece) + list(shared)
    kernel = functools.partial(head_kernel, STRETCH, head)
    if before is None:
        return call(kernel, order, args, [((tok, HEAD_DIM), BF16)] * 2, 10**9, grant=GRANTS[2])
    args += before
    held = pltpu.VMEM((tok, HEAD_DIM), BF16)
    return call(
        kernel, order, args, [((tok, total), BF16)] * 2, 10**9, out_specs=[ANY] * 2, grant=GRANTS[2],
        scratch_shapes=[held, held, pltpu.SemaphoreType.DMA((len(before) + 2,))],
    )


def pair_body(*args):
    return pair_steps(*args)


def pair_steps(layer_input, attn_weight, rate_weight, rate_bias, decay_rate, skip_gain):
    tok, _ = layer_input.shape
    heads = rate_bias.shape[0]
    group = HEADS // KV_HEADS
    ids = skip_gain[:1]
    count = lax.axis_size("grp")
    swap_high = [(g, g ^ 2) for g in range(count)]
    swap_low = [(g, g ^ 1) for g in range(count)]
    over_high = lambda a: lax.ppermute(a, "grp", swap_high)
    over_low = lambda a: lax.ppermute(a, "grp", swap_low)
    over_seq = lambda a: lax.ppermute(a, "seq", [(0, 1), (1, 0)])

    other = over_seq(layer_input)
    weights_all = jnp.transpose(attn_weight, (1, 0, 2))
    shapes = [((EXTRA, tok), F32), ((tok, HEAD_DIM), F32), ((tok, HEAD_DIM), F32)]

    def pair_places(h, l):
        return [(1 - h, group), (1 - h, group + 1), (h, group), (h, group + 1)]

    def high_places(j):
        return lambda h, l: [
            (1 - h, (1 - l) * heads + j), (1 - h, l * heads + j),
            (h, (1 - l) * heads + j), (h, l * heads + j),
        ]

    def low_places(j):
        return lambda h, l: [
            (1 - h, (1 - l) * heads + j), (h, (1 - l) * heads + j),
            (1 - h, l * heads + j), (h, l * heads + j),
        ]

    ahead = [(ids, weights_all)]

    def queued(make):
        ready, _ = lax.optimization_barrier((ids, ahead[0]))
        outs = make(ready)
        ahead[0] = outs[0]
        return outs

    def prepare():
        return queued(
            lambda ready: call(prepare_kernel, ready, [layer_input, rate_weight.T], shapes, 10**9)
        )

    raw, cosine, sine = prepare()
    other, weights_all, raw = lax.optimization_barrier((other, weights_all, raw))
    plan = [(None, weights_all, pair_places, over_high, over_low)]
    for pair in range(heads // 2):
        plan.append((2 * pair + 1, weights_all, low_places(2 * pair + 1), over_low, over_high))
        plan.append((2 * pair, weights_all, high_places(2 * pair), over_high, over_low))
    crossed, parts, arrived, pieces, kept = {}, {}, {}, {}, {}

    def cross(at):
        _, weights, places, _, _ = plan[at]
        out = queued(lambda ready: project(ready, other, weights, places))[0]
        crossed[at] = over_seq(out)

    def mine(at):
        j, weights, places, first, _ = plan[at]
        *sends, kept[at] = queued(
            lambda ready: project_add(
                ready, layer_input, weights, places, crossed[at], raw if j is None else None
            )
        )
        if j is None:
            for name, send in zip("kv", sends):
                parts[name] = first(send)
        else:
            parts[at] = first(sends[0])

    def middle(at):
        j, _, _, _, second = plan[0 if at in ("k", "v") else at]
        keep, u = kept[0 if at in ("k", "v") else at], parts[at]
        args, shapes, kernel = [keep, u], [((tok, LANES), BF16)], middle_kernel
        if at == "k":
            args, shapes, kernel = [raw, keep, u], [(u.shape, BF16)], keys_middle_kernel
        if at == "v":
            kernel = values_middle_kernel
        send = queued(lambda ready: call(kernel, ready, args, shapes, 10**7))[0]
        arrived[at] = second(send)
        if j is not None:
            pieces[j] = (keep, u, arrived[at])

    def context():
        args = [
            raw, kept[0], parts["k"], parts["v"], arrived["k"], arrived["v"], cosine, sine, rate_bias[None, :], decay_rate[None, :],
        ]
        spans = tok // STRETCH
        shapes = [
            ((tok + heads // 2 * HEAD_DIM, 2 * HEAD_DIM), BF16), ((tok, HEAD_DIM), BF16),
            ((heads * spans, STRETCH), F32), ((STRETCH, LANES), F32), ((heads * spans, STRETCH), F32),
            ((heads, HEAD_DIM, HEAD_DIM), F32),
        ]
        carry, *rest = queued(
            lambda ready: call(
                functools.partial(context_kernel, STRETCH), ready, args, shapes, 10**9,
                grant=GRANTS[2],
            )
        )
        came = over_seq(carry)
        bterm, across, down, step, first_state = rest
        return (
            cosine, sine, carry, bterm, came, across, down, step, first_state, skip_gain[None, :],
        )

    def tail(j, shared, before):
        return queued(
            lambda ready: head_call(ready, j, pieces[j], shared, heads * HEAD_DIM, before)
        )

    cross(0)
    cross(1)
    cross(2)
    mine(0)
    mine(1)
    mine(2)
    cross(3)
    middle("k")
    cross(4)
    middle("v")
    mine(3)
    middle(1)
    mine(4)
    middle(2)
    shared = context()
    done = {1: tail(1, shared, None)}
    middle(3)
    middle(4)
    for j in (0, 3):
        done[j] = tail(j, shared, None)
    outs = tail(2, shared, [part for j in sorted(done) for part in done[j]])
    return outs[0], outs[1]


def solution(mesh):
    placed = (
        P("seq", "grp"),
        P(("grp", "seq"), "mdl", None),
        P("grp", "mdl"),
        P(("mdl", "grp")),
        P(("mdl", "grp")),
        P(("mdl", "grp")),
    )
    chips = mesh.shape["grp"] * mesh.shape["mdl"]
    paired = (
        mesh.shape["seq"] == 2
        and mesh.shape["grp"] == 4
        and KV_HEADS == 2 * mesh.shape["mdl"]
        and HEADS // chips == 4
    )
    return jax.shard_map(
        pair_body if paired else body,
        mesh=mesh,
        in_specs=placed,
        out_specs=(P("seq", ("mdl", "grp")), P("seq", ("mdl", "grp"))),
        check_vma=False,
    )
```

```python
import functools
import math

import jax
import jax.numpy as jnp
from jax import lax
from jax.experimental import pallas as pl
from jax.experimental.pallas import tpu as pltpu
from jax.sharding import PartitionSpec as P


HEADS = 64
KV_HEADS = 8
HEAD_DIM = 128
STRETCH = 256


ROPE_BASE = 500000.0
FAR_BELOW = -1e30


def rope_angles(positions):
    half = HEAD_DIM // 2
    freq = ROPE_BASE ** (-2.0 * jnp.arange(half, dtype=jnp.float32) / HEAD_DIM)
    angle = positions.astype(jnp.float32)[:, None] * freq[None, :]
    return (jnp.cos(angle), jnp.sin(angle))


def rotate(vectors, cosine, sine):
    half = vectors.shape[-1] // 2
    first = vectors[..., :half]
    second = vectors[..., half:]
    cosine = cosine[:, None, :]
    sine = sine[:, None, :]
    return jnp.concatenate(
        [first * cosine - second * sine, second * cosine + first * sine], axis=-1
    )


def state_product(cterm, state):
    high = state.astype(jnp.bfloat16)
    low = (state - high.astype(jnp.float32)).astype(jnp.bfloat16)
    upper = jnp.einsum("thn,hnp->thp", cterm, high, preferred_element_type=jnp.float32)
    return upper + jnp.einsum("thn,hnp->thp", cterm, low, preferred_element_type=jnp.float32)


def key_absorber(queries, own_first, scale, carry, piece):
    top, total, accum = carry
    keys, values = piece
    scores = jnp.einsum("thd,nd->thn", queries, keys, preferred_element_type=jnp.float32) * scale
    query_pos = own_first + jnp.arange(queries.shape[0], dtype=jnp.int32)
    key_pos = jnp.arange(keys.shape[0], dtype=jnp.int32)
    causal = (key_pos[None, :] <= query_pos[:, None])[:, None, :]
    masked = jnp.where(causal, scores, FAR_BELOW)
    new_top = jnp.maximum(top, jnp.max(masked, axis=2))
    weights = jnp.where(causal, jnp.exp(masked - new_top[:, :, None]), 0.0)
    total = jnp.sum(weights, axis=2)
    accum = jnp.einsum(
        "thn,nd->thd", weights.astype(jnp.bfloat16), values, preferred_element_type=jnp.float32
    )
    return (new_top, total, accum)


def body(layer_input, attn_weight, rate_weight, rate_bias, decay_rate, skip_gain):
    tok = layer_input.shape[0]
    kv_local = attn_weight.shape[1]
    heads_local = rate_bias.shape[0]
    group = HEADS // KV_HEADS
    scale = HEAD_DIM ** (-0.5)
    merged = jnp.einsum(
        "td,dkc->tkc",
        layer_input,
        lax.all_gather(attn_weight, "seq", axis=0, tiled=True),
        preferred_element_type=jnp.float32,
    )
    rate_part = jnp.dot(layer_input, rate_weight, preferred_element_type=jnp.float32)
    grp_index = lax.axis_index("grp")
    summed, rate_whole = (
        lax.psum(merged.astype(jnp.bfloat16), "grp").astype(jnp.float32),
        lax.psum(rate_part.astype(jnp.bfloat16), "grp").astype(jnp.float32),
    )
    query_whole = summed[:, :, : group * HEAD_DIM].reshape(tok, kv_local * group * HEAD_DIM)
    query_flat = lax.dynamic_slice_in_dim(
        query_whole, grp_index * heads_local * HEAD_DIM, heads_local * HEAD_DIM, 1
    )
    raw = lax.dynamic_slice_in_dim(rate_whole, grp_index * heads_local, heads_local, 1)
    pairs = summed[:, :, group * HEAD_DIM :]
    kv_index = grp_index * heads_local // group
    pair = lax.dynamic_index_in_dim(pairs, kv_index, 1, keepdims=False)
    keys = pair[:, :HEAD_DIM]
    values = pair[:, HEAD_DIM:].astype(jnp.bfloat16)
    query = query_flat.reshape(tok, heads_local, HEAD_DIM)
    own_first = lax.axis_index("seq") * tok
    cosine, sine = rope_angles(own_first + jnp.arange(tok, dtype=jnp.int32))
    rot_query = rotate(query, cosine, sine).astype(jnp.bfloat16)
    rot_keys = rotate(keys[:, None, :], cosine, sine)[:, 0].astype(jnp.bfloat16)
    start_carry = (
        jnp.full((tok, heads_local), FAR_BELOW, jnp.float32),
        jnp.zeros((tok, heads_local), jnp.float32),
        jnp.zeros((tok, heads_local, HEAD_DIM), jnp.float32),
    )
    _, total, accum = key_absorber(
        rot_query,
        own_first,
        scale,
        start_carry,
        (
            lax.all_gather(rot_keys, "seq", axis=0, tiled=True),
            lax.all_gather(values, "seq", axis=0, tiled=True),
        ),
    )
    teacher = (accum / total[:, :, None]).astype(jnp.bfloat16).reshape(tok, heads_local * HEAD_DIM)
    step = jax.nn.softplus(raw + rate_bias[None, :])
    log_decay = -decay_rate[None, :] * step
    c_all = query.astype(jnp.bfloat16)
    b_all = keys.astype(jnp.bfloat16)
    causal = (
        jnp.arange(STRETCH, dtype=jnp.int32)[:, None]
        >= jnp.arange(STRETCH, dtype=jnp.int32)[None, :]
    )[None]
    state = jnp.zeros((heads_local, HEAD_DIM, HEAD_DIM), jnp.float32)
    before = jnp.zeros((heads_local,), jnp.float32)
    partials = []
    offsets = []
    for index in range(tok // STRETCH):
        first = index * STRETCH
        cpart = c_all[first : first + STRETCH]
        bpart = b_all[first : first + STRETCH]
        xpart = values[first : first + STRETCH]
        decay = log_decay[first : first + STRETCH]
        rate = step[first : first + STRETCH]
        cum = jnp.cumsum(decay, axis=0)
        gram = jnp.einsum("thn,sn->hts", cpart, bpart, preferred_element_type=jnp.float32) * scale
        diff = cum.T[:, :, None] - cum.T[:, None, :]
        mix = jnp.where(
            causal, jnp.exp(jnp.where(causal, diff, -10000.0)) * rate.T[:, None, :] * gram, 0.0
        ).astype(jnp.bfloat16)
        intra = jnp.einsum("hts,sp->thp", mix, xpart, preferred_element_type=jnp.float32)
        carried = state_product(cpart, state) * scale * jnp.exp(cum)[:, :, None]
        weighted = (
            (jnp.exp(cum[-1][None, :] - cum) * rate)[:, :, None]
            * bpart.astype(jnp.float32)[:, None, :]
        ).astype(jnp.bfloat16)
        contribution = jnp.einsum(
            "shn,sp->hnp", weighted, xpart, preferred_element_type=jnp.float32
        )
        state = jnp.exp(cum[-1])[:, None, None] * state + contribution
        partials.append(intra + carried)
        offsets.append(cum + before[None, :])
        before = before + cum[-1]
    totals, states = (
        lax.all_gather(before[None, :].astype(jnp.bfloat16), "seq", axis=0, tiled=True).astype(
            jnp.float32
        ),
        lax.all_gather(state[None].astype(jnp.bfloat16), "seq", axis=0, tiled=True).astype(
            jnp.float32
        ),
    )
    position = lax.axis_index("seq")
    order = jnp.arange(totals.shape[0], dtype=jnp.int32)
    between = ((order[:, None] < order[None, :]) & (order[None, :] < position)).astype(jnp.float32)
    span = jnp.dot(between, totals, precision=lax.Precision.HIGHEST)
    reach_back = jnp.where(order[:, None] < position, jnp.exp(span), 0.0)
    incoming = jnp.einsum("dh,dhnp->hnp", reach_back, states, precision=lax.Precision.HIGHEST)
    inside = jnp.concatenate(partials, axis=0)
    reach = jnp.exp(jnp.concatenate(offsets, axis=0))
    arriving = state_product(c_all, incoming) * scale * reach[:, :, None]
    skipped = skip_gain[None, :, None] * values.astype(jnp.float32)[:, None, :]
    student = (
        (inside + arriving + skipped).astype(jnp.bfloat16).reshape(tok, heads_local * HEAD_DIM)
    )
    return (teacher, student)


LANES = 128
EXTRA = 16
GRANTS = tuple(mib * 1024 * 1024 for mib in (6, 12, 16, 24))
F32 = jnp.float32
BF16 = jnp.bfloat16
LAST = (((1,), (1,)), ((), ()))


def cost(flops, moved):
    return pl.CostEstimate(flops=flops, bytes_accessed=moved, transcendentals=0)


def place_of():
    grp = lax.axis_index("grp")
    return grp // 2, grp % 2, lax.axis_index("seq")


def gathered(w_ref, blocks):
    return jnp.concatenate(
        [w_ref[kv, :, pl.ds(pl.multiple_of(col * LANES, LANES), LANES)] for kv, col in blocks], axis=1
    )


def own_columns(x_ref, rows):
    first = pl.multiple_of(lax.axis_index("seq") * rows, LANES)
    return x_ref[:, pl.ds(first, rows)]


def project_kernel(places, order, x_ref, w_ref, out_ref):
    high, low, _ = place_of()
    weights = gathered(w_ref, places(high, low))
    out_ref[...] = jnp.dot(
        own_columns(x_ref, w_ref.shape[1]), weights, preferred_element_type=F32
    ).astype(BF16)


def project_add_kernel(places, order, x_ref, w_ref, r_ref, send_ref, keep_ref):
    high, low, _ = place_of()
    blocks = places(high, low)
    tok, half = keep_ref.shape
    tokens = own_columns(x_ref, w_ref.shape[1])
    first = jnp.dot(tokens, gathered(w_ref, blocks[:2]), preferred_element_type=F32)
    send_ref[:tok, :] = (first + r_ref[:, :half].astype(F32)).astype(BF16)
    second = jnp.dot(tokens, gathered(w_ref, blocks[2:]), preferred_element_type=F32)
    keep_ref[...] = second + r_ref[:, half:].astype(F32)


def folded(rates):
    parts = rates.shape[1] // LANES
    return jnp.concatenate([rates[:, i * LANES : (i + 1) * LANES] for i in range(parts)], axis=0)


def unfolded(rows, count):
    parts = rows.shape[0] // count
    return jnp.concatenate([rows[i * count : (i + 1) * count] for i in range(parts)], axis=1)


def project_pair_kernel(places, order, raw_ref, x_ref, w_ref, r_ref, keys_ref, values_ref, keep_ref):
    high, low, _ = place_of()
    blocks = places(high, low)
    tok, half = keep_ref.shape
    tokens = own_columns(x_ref, w_ref.shape[1])
    first = jnp.dot(tokens, gathered(w_ref, blocks[:2]), preferred_element_type=F32)
    first = (first + r_ref[:, :half].astype(F32)).astype(BF16)
    keys_ref[:tok, :] = first[:, :LANES]
    values_ref[...] = first[:, LANES:]
    second = jnp.dot(tokens, gathered(w_ref, blocks[2:]), preferred_element_type=F32)
    keep_ref[...] = second + r_ref[:, half:].astype(F32)
    away = EXTRA // 2
    rates = jnp.where(high == 0, raw_ref[away:, :], raw_ref[:away, :])
    keys_ref[tok:, :] = folded(rates).astype(BF16)


def own_rates(raw_ref, u_ref):
    tok = raw_ref.shape[1]
    own = EXTRA // 2
    rates = jnp.where(place_of()[0] == 0, raw_ref[:own, :], raw_ref[own:, :])
    return rates + unfolded(u_ref[tok:, :].astype(F32), own)


def keys_middle_kernel(order, raw_ref, keep_ref, u_ref, send_ref):
    tok = keep_ref.shape[0]
    send_ref[:tok, :] = (keep_ref[:, :LANES] + u_ref[:tok, :].astype(F32)).astype(BF16)
    send_ref[tok:, :] = folded(own_rates(raw_ref, u_ref)).astype(BF16)


def values_middle_kernel(order, keep_ref, u_ref, send_ref):
    send_ref[...] = (keep_ref[:, LANES:] + u_ref[...].astype(F32)).astype(BF16)


def middle_kernel(order, keep_ref, u_ref, send_ref):
    send_ref[...] = (keep_ref[:, :LANES] + u_ref[:, :LANES].astype(F32)).astype(BF16)


def prepare_kernel(order, x_ref, rates_ref, raw_ref, cos_ref, sin_ref):
    raw_ref[...] = lax.dot_general(
        rates_ref[...], x_ref[...], LAST, preferred_element_type=F32
    )
    tok, wide = cos_ref.shape
    half = wide // 2
    fine = EXTRA
    lane = lax.broadcasted_iota(jnp.int32, (1, wide), 1)
    slot = jnp.where(lane < half, lane, lane - half).astype(F32)
    freq = jnp.exp(slot * (-2.0 / wide * math.log(ROPE_BASE)))
    start = lax.axis_index("seq") * tok
    coarse = lax.broadcasted_iota(jnp.int32, (tok // fine, wide), 0) * fine + start
    coarse = coarse.astype(F32) * freq
    small = lax.broadcasted_iota(jnp.int32, (fine, wide), 0).astype(F32) * freq
    cos_big, sin_big = jnp.cos(coarse), jnp.sin(coarse)
    cos_small, sin_small = jnp.cos(small), jnp.sin(small)
    sign = jnp.where(lane < half, -1.0, 1.0)
    for at in range(tok // fine):
        c, d = cos_big[at : at + 1, :], sin_big[at : at + 1, :]
        span = slice(at * fine, (at + 1) * fine)
        cos_ref[span, :] = c * cos_small - d * sin_small
        sin_ref[span, :] = (d * cos_small + c * sin_small) * sign


VMEM = pl.BlockSpec(memory_space=pltpu.VMEM)
SMEM = pl.BlockSpec(memory_space=pltpu.SMEM)
ANY = pl.BlockSpec(memory_space=pl.ANY)


def call(kernel, order, args, shapes, flops, in_specs=None, **rest):
    return pl.pallas_call(
        kernel,
        in_specs=[ANY] + (in_specs or [VMEM] * len(args)),
        out_specs=rest.pop("out_specs", [VMEM] * len(shapes)),
        out_shape=[jax.ShapeDtypeStruct(s, d) for s, d in shapes],
        compiler_params=pltpu.CompilerParams(vmem_limit_bytes=rest.pop("grant", GRANTS[1])),
        cost_estimate=cost(flops, 3 * 10**6),
        **rest,
    )(order, *args)


def project(order, x, weights, places):
    tok, rows = x.shape[0], weights.shape[1]
    wide = 4 * LANES
    return call(
        functools.partial(project_kernel, places), order, [x, weights],
        [((tok, wide), BF16)], 2 * tok * rows * wide,
    )


def project_add(order, x, weights, places, received, raw):
    tok, rows = x.shape[0], weights.shape[1]
    wide = 4 * LANES
    args, kernel = [x, weights, received], project_add_kernel
    kept = ((tok, wide // 2), F32)
    if raw is None:
        shapes = [((tok, wide // 2), BF16), kept]
    else:
        args, kernel = [raw] + args, project_pair_kernel
        tall = tok + EXTRA // 2 * tok // LANES
        shapes = [((tall, LANES), BF16), ((tok, LANES), BF16), kept]
    return call(functools.partial(kernel, places), order, args, shapes, 2 * tok * rows * wide)


def turn(vectors, cosine, sine):
    return vectors * cosine + pltpu.roll(vectors, HEAD_DIM // 2, 1) * sine


def split_sum(rows, mask):
    high = rows.astype(BF16)
    rest = rows - high.astype(F32)
    middle = rest.astype(BF16)
    low = (rest - middle.astype(F32)).astype(BF16)
    count = rows.shape[0]
    parts = jnp.concatenate([high.astype(F32), middle.astype(F32), low.astype(F32)], axis=0)
    sums = lax.dot_general(parts.astype(BF16), mask, LAST, preferred_element_type=F32)
    return sums[:count] + (sums[count : 2 * count] + sums[2 * count :])


def upright(row):
    count = row.shape[1]
    down = lax.broadcasted_iota(jnp.int32, (count, count), 0)
    along = lax.broadcasted_iota(jnp.int32, (count, count), 1)
    return jnp.sum(jnp.where(down == along, row, 0.0), axis=1, keepdims=True)


def context_kernel(
    stretch, order, raw_ref, keep_ref, u_ref, u_values_ref, z_ref, z_values_ref, cos_ref, sin_ref,
    bias_ref, rate_ref,
    carry_ref, bterm_ref, across_ref, down_ref, step_ref, first_ref,
):
    tok = keep_ref.shape[0]
    heads = bias_ref.shape[1]
    spans = tok // stretch
    keys = keep_ref[:, :LANES] + u_ref[:tok, :].astype(F32) + z_ref[:tok, :].astype(F32)
    values = keep_ref[:, LANES:] + u_values_ref[...].astype(F32) + z_values_ref[...].astype(F32)
    values = values.astype(BF16)
    bterm = keys.astype(BF16)
    carry_ref[:tok, :HEAD_DIM] = turn(keys, cos_ref[...], sin_ref[...]).astype(BF16)
    carry_ref[:tok, HEAD_DIM:] = values
    bterm_ref[...] = bterm
    both = own_rates(raw_ref, u_ref) + unfolded(z_ref[tok:, :].astype(F32), EXTRA // 2)
    raw = jnp.where(place_of()[1] == 0, both[:heads], both[heads:])
    bias, rate = upright(bias_ref[...]), upright(rate_ref[...])
    step = jax.nn.softplus(raw + bias)
    decay = -rate * step
    rows = lax.broadcasted_iota(jnp.int32, (stretch, stretch), 0)
    cols = lax.broadcasted_iota(jnp.int32, (stretch, stretch), 1)
    below = (cols <= rows).astype(F32).astype(BF16)
    fold = lambda a: jnp.concatenate([a[:, i * stretch : (i + 1) * stretch] for i in range(spans)], axis=0)
    across = split_sum(fold(decay), below)
    steps = fold(step)
    tails = jnp.exp(across[:, stretch - 1 :] - across) * steps
    across_ref[...] = across
    step_ref[...] = steps
    count = heads * spans
    filler = jnp.zeros((LANES - 2 * count, stretch), F32)
    down = jnp.transpose(jnp.concatenate([across, tails, filler], axis=0))
    down_ref[...] = down
    states = [None] * heads
    for index in range(spans):
        span = slice(index * stretch, (index + 1) * stretch)
        part = bterm[span].astype(F32)
        weighted = jnp.concatenate(
            [
                (part * down[:, count + index * heads + h : count + index * heads + h + 1]).astype(BF16)
                for h in range(heads)
            ],
            axis=1,
        )
        fresh = lax.dot_general(
            weighted, values[span], (((0,), (0,)), ((), ())), preferred_element_type=F32
        )
        for h in range(heads):
            new = fresh[h * HEAD_DIM : (h + 1) * HEAD_DIM]
            if index > 0:
                at = index * heads + h
                new = new + jnp.exp(across[at : at + 1, stretch - 1 :]) * states[h]
            else:
                first_ref[h] = new
            states[h] = new
    for h in range(heads):
        row, col = tok + (h // 2) * HEAD_DIM, (h % 2) * HEAD_DIM
        carry_ref[row : row + HEAD_DIM, col : col + HEAD_DIM] = states[h].astype(BF16)


def head_kernel(
    stretch, head, order, keep_ref, u_ref, z_ref, cos_ref, sin_ref, carry_ref, bterm_ref, came_ref,
    across_ref, down_ref, step_ref, first_ref, skip_ref, *rest,
):
    if len(rest) == 2:
        teacher_ref, student_ref = rest
    else:
        teacher_out, student_out, teacher_ref, student_ref, sems = rest[-5:]
        before, copies = rest[:-5], []
        for at, held in enumerate(before):
            number, kind = at // 2, at % 2
            number = number + (number >= head)
            out = (teacher_out, student_out)[kind]
            place = slice(number * HEAD_DIM, (number + 1) * HEAD_DIM)
            copies.append(pltpu.make_async_copy(held, out.at[:, place], sems.at[at]))
            copies[-1].start()
    tok = bterm_ref.shape[0]
    heads = first_ref.shape[0]
    scale = HEAD_DIM ** (-0.5)
    power = scale * 1.4426950408889634
    later = (lax.axis_index("seq") > 0).astype(F32)
    blocked = (1.0 - later) * FAR_BELOW
    rows = lax.broadcasted_iota(jnp.int32, (stretch, stretch), 0)
    cols = lax.broadcasted_iota(jnp.int32, (stretch, stretch), 1)
    causal = cols <= rows
    ones = jnp.ones((tok, HEAD_DIM), BF16)
    own_keys = carry_ref[:tok, :HEAD_DIM]
    prev_keys = came_ref[:tok, :HEAD_DIM]
    own_values = jnp.concatenate([carry_ref[:tok, HEAD_DIM:], ones], axis=1)
    prev_values = jnp.concatenate([came_ref[:tok, HEAD_DIM:], ones], axis=1)
    query = keep_ref[:, LANES:] + u_ref[:, LANES:].astype(F32) + z_ref[...].astype(F32)
    turned = turn(query, cos_ref[...], sin_ref[...]).astype(BF16)
    cterm = query.astype(BF16)
    row, col = tok + (head // 2) * HEAD_DIM, (head % 2) * HEAD_DIM
    state = came_ref[row : row + HEAD_DIM, col : col + HEAD_DIM].astype(F32) * later
    skip = skip_ref[:, head : head + 1]
    for index in range(tok // stretch):
        span = slice(index * stretch, (index + 1) * stretch)
        reach = (index + 1) * stretch
        queries = turned[span]
        far = lax.dot_general(queries, prev_keys, LAST, preferred_element_type=F32) + blocked
        near = lax.dot_general(queries, own_keys[:reach], LAST, preferred_element_type=F32)
        diagonal = jnp.where(causal, near[:, index * stretch :], FAR_BELOW)
        if index > 0:
            near = jnp.concatenate([near[:, : index * stretch], diagonal], axis=1)
        else:
            near = diagonal
        top = jnp.maximum(
            jnp.max(far, axis=1, keepdims=True), jnp.max(near, axis=1, keepdims=True)
        )
        far = jnp.exp2((far - top) * power).astype(BF16)
        near = jnp.exp2((near - top) * power).astype(BF16)
        mixed = jnp.dot(far, prev_values, preferred_element_type=F32) + jnp.dot(
            near, own_values[:reach], preferred_element_type=F32
        )
        teacher_ref[span, :] = (mixed[:, :HEAD_DIM] / mixed[:, HEAD_DIM:]).astype(BF16)
        values = carry_ref[span, HEAD_DIM:]
        which = index * heads + head
        down = down_ref[:, which : which + 1]
        across = across_ref[which : which + 1, :]
        gram = lax.dot_general(
            cterm[span], bterm_ref[span, :], LAST, preferred_element_type=F32
        ) * (step_ref[which : which + 1, :] * scale)
        mix = jnp.where(causal, jnp.exp(jnp.where(causal, down - across, -1e4)) * gram, 0.0)
        inner = jnp.dot(mix.astype(BF16), values, preferred_element_type=F32)
        high = state.astype(BF16)
        low = (state - high.astype(F32)).astype(BF16)
        carried = jnp.dot(
            cterm[span], jnp.concatenate([high, low], axis=1), preferred_element_type=F32
        )
        carried = (carried[:, :HEAD_DIM] + carried[:, HEAD_DIM:]) * (jnp.exp(down) * scale)
        student_ref[span, :] = (inner + carried + skip * values.astype(F32)).astype(BF16)
        if index == 0:
            state = jnp.exp(across[:, stretch - 1 :]) * state + first_ref[head]
    if len(rest) > 2:
        place = slice(head * HEAD_DIM, (head + 1) * HEAD_DIM)
        for kind, (held, out) in enumerate(((teacher_ref, teacher_out), (student_ref, student_out))):
            copies.append(
                pltpu.make_async_copy(held, out.at[:, place], sems.at[len(before) + kind])
            )
            copies[-1].start()
        for copy in copies:
            copy.wait()


def head_call(order, head, piece, shared, total, before):
    tok = piece[0].shape[0]
    args = list(piece) + list(shared)
    kernel = functools.partial(head_kernel, STRETCH, head)
    if before is None:
        return call(kernel, order, args, [((tok, HEAD_DIM), BF16)] * 2, 10**9, grant=GRANTS[2])
    args += before
    held = pltpu.VMEM((tok, HEAD_DIM), BF16)
    return call(
        kernel, order, args, [((tok, total), BF16)] * 2, 10**9, out_specs=[ANY] * 2, grant=GRANTS[2],
        scratch_shapes=[held, held, pltpu.SemaphoreType.DMA((len(before) + 2,))],
    )


def pair_body(*args):
    return pair_steps(*args)


def pair_steps(layer_input, attn_weight, rate_weight, rate_bias, decay_rate, skip_gain):
    tok, _ = layer_input.shape
    heads = rate_bias.shape[0]
    group = HEADS // KV_HEADS
    ids = skip_gain[:1]
    count = lax.axis_size("grp")
    swap_high = [(g, g ^ 2) for g in range(count)]
    swap_low = [(g, g ^ 1) for g in range(count)]
    over_high = lambda a: lax.ppermute(a, "grp", swap_high)
    over_low = lambda a: lax.ppermute(a, "grp", swap_low)
    over_seq = lambda a: lax.ppermute(a, "seq", [(0, 1), (1, 0)])

    other = over_seq(layer_input)
    weights_all = jnp.transpose(attn_weight, (1, 0, 2))
    shapes = [((EXTRA, tok), F32), ((tok, HEAD_DIM), F32), ((tok, HEAD_DIM), F32)]

    def pair_places(h, l):
        return [(1 - h, group), (1 - h, group + 1), (h, group), (h, group + 1)]

    def high_places(j):
        return lambda h, l: [
            (1 - h, (1 - l) * heads + j), (1 - h, l * heads + j),
            (h, (1 - l) * heads + j), (h, l * heads + j),
        ]

    def low_places(j):
        return lambda h, l: [
            (1 - h, (1 - l) * heads + j), (h, (1 - l) * heads + j),
            (1 - h, l * heads + j), (h, l * heads + j),
        ]

    ahead = [(ids, weights_all)]

    def queued(make):
        ready, _ = lax.optimization_barrier((ids, ahead[0]))
        outs = make(ready)
        ahead[0] = outs[0]
        return outs

    def prepare():
        return queued(
            lambda ready: call(prepare_kernel, ready, [layer_input, rate_weight.T], shapes, 10**9)
        )

    raw, cosine, sine = prepare()
    other, weights_all, raw = lax.optimization_barrier((other, weights_all, raw))
    plan = [(None, weights_all, pair_places, over_high, over_low)]
    for pair in range(heads // 2):
        plan.append((2 * pair + 1, weights_all, low_places(2 * pair + 1), over_low, over_high))
        plan.append((2 * pair, weights_all, high_places(2 * pair), over_high, over_low))
    crossed, parts, arrived, pieces, kept = {}, {}, {}, {}, {}

    def cross(at):
        _, weights, places, _, _ = plan[at]
        out = queued(lambda ready: project(ready, other, weights, places))[0]
        crossed[at] = over_seq(out)

    def mine(at):
        j, weights, places, first, _ = plan[at]
        *sends, kept[at] = queued(
            lambda ready: project_add(
                ready, layer_input, weights, places, crossed[at], raw if j is None else None
            )
        )
        if j is None:
            for name, send in zip("kv", sends):
                parts[name] = first(send)
        else:
            parts[at] = first(sends[0])

    def middle(at):
        j, _, _, _, second = plan[0 if at in ("k", "v") else at]
        keep, u = kept[0 if at in ("k", "v") else at], parts[at]
        args, shapes, kernel = [keep, u], [((tok, LANES), BF16)], middle_kernel
        if at == "k":
            args, shapes, kernel = [raw, keep, u], [(u.shape, BF16)], keys_middle_kernel
        if at == "v":
            kernel = values_middle_kernel
        send = queued(lambda ready: call(kernel, ready, args, shapes, 10**7))[0]
        arrived[at] = second(send)
        if j is not None:
            pieces[j] = (keep, u, arrived[at])

    def context():
        args = [
            raw, kept[0], parts["k"], parts["v"], arrived["k"], arrived["v"], cosine, sine, rate_bias[None, :], decay_rate[None, :],
        ]
        spans = tok // STRETCH
        shapes = [
            ((tok + heads // 2 * HEAD_DIM, 2 * HEAD_DIM), BF16), ((tok, HEAD_DIM), BF16),
            ((heads * spans, STRETCH), F32), ((STRETCH, LANES), F32), ((heads * spans, STRETCH), F32),
            ((heads, HEAD_DIM, HEAD_DIM), F32),
        ]
        carry, *rest = queued(
            lambda ready: call(
                functools.partial(context_kernel, STRETCH), ready, args, shapes, 10**9,
                grant=GRANTS[2],
            )
        )
        came = over_seq(carry)
        bterm, across, down, step, first_state = rest
        return (
            cosine, sine, carry, bterm, came, across, down, step, first_state, skip_gain[None, :],
        )

    def tail(j, shared, before):
        return queued(
            lambda ready: head_call(ready, j, pieces[j], shared, heads * HEAD_DIM, before)
        )

    cross(0)
    cross(1)
    cross(2)
    mine(0)
    mine(1)
    mine(2)
    cross(3)
    middle("k")
    cross(4)
    middle("v")
    mine(3)
    mine(4)
    middle(1)
    middle(2)
    shared = context()
    middle(4)
    middle(3)
    done = {j: tail(j, shared, None) for j in (0, 1, 2)}
    outs = tail(3, shared, [part for j in sorted(done) for part in done[j]])
    return outs[0], outs[1]


def solution(mesh):
    placed = (
        P("seq", "grp"),
        P(("grp", "seq"), "mdl", None),
        P("grp", "mdl"),
        P(("mdl", "grp")),
        P(("mdl", "grp")),
        P(("mdl", "grp")),
    )
    chips = mesh.shape["grp"] * mesh.shape["mdl"]
    paired = (
        mesh.shape["seq"] == 2
        and mesh.shape["grp"] == 4
        and KV_HEADS == 2 * mesh.shape["mdl"]
        and HEADS // chips == 4
    )
    return jax.shard_map(
        pair_body if paired else body,
        mesh=mesh,
        in_specs=placed,
        out_specs=(P("seq", ("mdl", "grp")), P("seq", ("mdl", "grp"))),
        check_vma=False,
    )
```
